16 devices in a mesh: etp: 4 (over z, y), ep: 4 (over x, core).
Axes of the slice: x: 2, y: 2, z: 2, core: 2. Of those that a mesh axis runs over, the one named last changes fastest.
Arguments:
- hidden: bfloat16 [65536, 256], P(('ep', 'etp'))
- w_router: float32 [256, 64], replicated
- expert_ids: int32 [65536, 2], P(('ep', 'etp'))
- d_out: bfloat16 [65536, 256], P(('ep', 'etp'))
- w_gate: bfloat16 [64, 256, 1024], P('ep', None, 'etp')
- w_up: bfloat16 [64, 256, 1024], P('ep', None, 'etp')
- w_down: bfloat16 [64, 1024, 256], P('ep', 'etp')
Outputs:
- output 1: bfloat16 [65536, 256], P(('ep', 'etp'))
- output 2: bfloat16 [65536, 256], P(('ep', 'etp'))
- output 3: float32 [256, 64], replicated
- output 4: float32 [], replicated
- output 5: float32 [64, 256, 1024], P('ep', None, 'etp')
- output 6: float32 [64, 256, 1024], P('ep', None, 'etp')
- output 7: float32 [64, 1024, 256], P('ep', 'etp')
All inputs are finite; a program needn't handle non-finite values.
Results may differ from the reference program's by a relative error of at most 0.00894483.
Values are sent between devices in bfloat16 or wider.
A program may use at most 1 GiB of HBM per device.

```python
import jax
import jax.numpy as jnp
from jax import lax

EXPERTS = 64
D_MODEL = 256
D_FF = 1024
TOKENS = 65536
N_DEVICES = 16

CAPACITY = (5 * TOKENS + 2 * EXPERTS - 1) // (2 * EXPERTS)
BLOCK_TOKENS = TOKENS // N_DEVICES


def draw_choices(draw_key):
    quarter = BLOCK_TOKENS // (2 * EXPERTS)
    perm_key, block_key = jax.random.split(draw_key)
    expert_order = jax.random.permutation(perm_key, EXPERTS)
    hot_shift = jnp.zeros((EXPERTS,), jnp.int32).at[:4].set(jnp.array([2, 2, -2, -2], jnp.int32) * quarter)

    def one_block(one_key):
        k_noise, k_rows, k_flip = jax.random.split(one_key, 3)
        count_noise = jax.random.randint(k_noise, (EXPERTS,), 0, quarter + 1)
        count_noise = count_noise.at[0].set(quarter).at[1].set(0)
        count_perm = 4 * quarter + count_noise - jnp.roll(count_noise, -1) + hot_shift
        counts = jnp.zeros((EXPERTS,), jnp.int32).at[expert_order].set(count_perm)
        ends = jnp.cumsum(counts)
        id_seq = jnp.sum(jnp.arange(2 * BLOCK_TOKENS)[:, None] >= ends[None, :], axis=1).astype(jnp.int32)
        id_pairs = jnp.stack([id_seq[:BLOCK_TOKENS], id_seq[BLOCK_TOKENS:]], axis=1)
        id_pairs = id_pairs[jax.random.permutation(k_rows, BLOCK_TOKENS)]
        flip_mask = jax.random.randint(k_flip, (BLOCK_TOKENS, 1), 0, 2) == 1
        return jnp.where(flip_mask, id_pairs[:, ::-1], id_pairs)

    blocks = jax.vmap(one_block)(jax.random.split(block_key, N_DEVICES))
    return blocks.reshape(TOKENS, 2)


def setup_inputs(seed: int = 0) -> dict:
    root_key = jax.random.key(seed)
    k_hid, k_route, k_ids, k_dout, k_gate, k_up, k_down = jax.random.split(root_key, 7)
    hidden = jax.random.normal(k_hid, (TOKENS, D_MODEL), jnp.float32).astype(jnp.bfloat16)
    w_router = jax.random.normal(k_route, (D_MODEL, EXPERTS), jnp.float32) * (0.5 * D_MODEL ** -0.5)
    expert_ids = draw_choices(k_ids)
    d_out = jax.random.normal(k_dout, (TOKENS, D_MODEL), jnp.float32).astype(jnp.bfloat16)
    w_gate = (jax.random.normal(k_gate, (EXPERTS, D_MODEL, D_FF), jnp.float32) * D_MODEL ** -0.5).astype(jnp.bfloat16)
    w_up = (jax.random.normal(k_up, (EXPERTS, D_MODEL, D_FF), jnp.float32) * D_MODEL ** -0.5).astype(jnp.bfloat16)
    w_down = (jax.random.normal(k_down, (EXPERTS, D_FF, D_MODEL), jnp.float32) * D_FF ** -0.5).astype(jnp.bfloat16)
    return {"hidden": hidden, "w_router": w_router, "expert_ids": expert_ids, "d_out": d_out, "w_gate": w_gate, "w_up": w_up, "w_down": w_down}


def route_terms(logits, expert_ids):
    prob_vals = jax.nn.softmax(logits, axis=-1)
    picked = jnp.take_along_axis(prob_vals, expert_ids, axis=1)
    return picked / jnp.sum(picked, axis=1, keepdims=True), jnp.sum(prob_vals, axis=0)


def expert_pass(operands):
    x_buf, dy_buf, gate_w, up_w, down_w = operands
    act_a = jnp.dot(x_buf, gate_w, preferred_element_type=jnp.float32)
    act_b = jnp.dot(x_buf, up_w, preferred_element_type=jnp.float32)
    sig_a = jax.nn.sigmoid(act_a)
    silu_a = act_a * sig_a
    inner_act = (silu_a * act_b).astype(jnp.bfloat16)
    y_buf = jnp.dot(inner_act, down_w, preferred_element_type=jnp.float32).astype(jnp.bfloat16)
    d_inner = jnp.dot(dy_buf, down_w.T, preferred_element_type=jnp.float32)
    d_act_a = (d_inner * act_b * sig_a * (1.0 + act_a * (1.0 - sig_a))).astype(jnp.bfloat16)
    d_act_b = (d_inner * silu_a).astype(jnp.bfloat16)
    dx_buf = (jnp.dot(d_act_a, gate_w.T, preferred_element_type=jnp.float32) + jnp.dot(d_act_b, up_w.T, preferred_element_type=jnp.float32)).astype(jnp.bfloat16)
    g_gate = jnp.dot(x_buf.T, d_act_a, preferred_element_type=jnp.float32)
    g_up = jnp.dot(x_buf.T, d_act_b, preferred_element_type=jnp.float32)
    g_down = jnp.dot(inner_act.T, dy_buf, preferred_element_type=jnp.float32)
    return y_buf, dx_buf, g_gate, g_up, g_down


def reference(hidden, w_router, expert_ids, d_out, w_gate, w_up, w_down):
    hidden_f = hidden.astype(jnp.float32)
    logits = jnp.dot(hidden_f, w_router, preferred_element_type=jnp.float32)
    (gate_vals, prob_sum), route_vjp = jax.vjp(lambda logit_in: route_terms(logit_in, expert_ids), logits)
    n_assign = 2 * TOKENS
    flat_ids = expert_ids.reshape(-1)
    assign = jnp.arange(n_assign, dtype=jnp.int32)
    counts = jnp.bincount(flat_ids, length=EXPERTS)
    sort_order = jnp.argsort(flat_ids * n_assign + assign)
    sort_rank = jnp.zeros((n_assign,), jnp.int32).at[sort_order].set(assign)
    starts = jnp.cumsum(counts) - counts
    slot_pos = sort_rank - starts[flat_ids]
    dest_rows = jnp.where(slot_pos < CAPACITY, flat_ids * CAPACITY + slot_pos, EXPERTS * CAPACITY)
    source = jnp.full((EXPERTS * CAPACITY,), n_assign, jnp.int32).at[dest_rows].set(assign, mode="drop")
    x_buf = jnp.take(hidden, source // 2, axis=0, mode="fill", fill_value=0).reshape(EXPERTS, CAPACITY, D_MODEL)
    d_mix = 2.0 * d_out.astype(jnp.float32)
    dy_assign = (gate_vals[:, :, None] * d_mix[:, None, :]).astype(jnp.bfloat16).reshape(n_assign, D_MODEL)
    dy_buf = jnp.take(dy_assign, source, axis=0, mode="fill", fill_value=0).reshape(EXPERTS, CAPACITY, D_MODEL)
    y_buf, dx_buf, g_gate, g_up, g_down = lax.map(expert_pass, (x_buf, dy_buf, w_gate, w_up, w_down))
    y_pair = jnp.take(y_buf.reshape(EXPERTS * CAPACITY, D_MODEL), dest_rows, axis=0, mode="fill", fill_value=0).reshape(TOKENS, 2, D_MODEL).astype(jnp.float32)
    dx_pair = jnp.take(dx_buf.reshape(EXPERTS * CAPACITY, D_MODEL), dest_rows, axis=0, mode="fill", fill_value=0).reshape(TOKENS, 2, D_MODEL).astype(jnp.float32)
    output = (hidden_f + 2.0 * jnp.sum(gate_vals[:, :, None] * y_pair, axis=1)).astype(jnp.bfloat16)
    d_gates = jnp.sum(d_mix[:, None, :] * y_pair, axis=2)
    route_frac = counts.astype(jnp.float32) / n_assign
    aux_loss = 0.01 * EXPERTS * jnp.sum(route_frac * prob_sum) / TOKENS
    (d_logits,) = route_vjp((d_gates, (0.01 * EXPERTS / TOKENS) * route_frac))
    d_router = jnp.dot(hidden_f.T, d_logits, preferred_element_type=jnp.float32)
    d_hidden = (d_out.astype(jnp.float32) + jnp.sum(dx_pair, axis=1) + jnp.dot(d_logits, w_router.T, preferred_element_type=jnp.float32)).astype(jnp.bfloat16)
    return output, d_hidden, d_router, aux_loss, g_gate, g_up, g_down
```

```python
import functools
import jax
import jax.numpy as jnp
from jax import lax
from jax.experimental import pallas as pl
from jax.experimental.pallas import tpu as pltpu
from jax.sharding import PartitionSpec as P

AUX_COEF = 0.01
OUT_SCALE = 2.0
F32 = jnp.float32
BF16 = jnp.bfloat16
HI = lax.Precision.HIGHEST
MESH = pl.DeviceIdType.MESH
NT = (((1,), (1,)), ((), ()))
TN = (((0,), (0,)), ((), ()))


def dot(a, b, dims=(((1,), (0,)), ((), ())), precision=None):
    return lax.dot_general(a, b, dims, precision=precision, preferred_element_type=F32)


def flip(index, mask, bits):
    total = 0
    for bit in range(bits):
        total = total + ((index // 2**bit + mask // 2**bit) % 2) * 2**bit
    return total


def route_kernel(per_expert, hidden_ref, wr_ref, ids_ref, pos_ref, gate_ref, prob_ref, stat_ref):
    n_experts = wr_ref.shape[0]
    rows = hidden_ref.shape[0]
    block = min(512, rows)
    iota_e = lax.broadcasted_iota(jnp.int32, (n_experts, block), 0)
    upper = (lax.broadcasted_iota(jnp.int32, (block, block), 0) < lax.broadcasted_iota(jnp.int32, (block, block), 1)).astype(BF16)
    ones = jnp.ones((8, block), BF16)
    ones_f = jnp.ones((8, block), F32)
    wr = wr_ref[...]
    wr_hi = wr.astype(BF16)
    rest = wr - wr_hi.astype(F32)
    wr_mid = rest.astype(BF16)
    wr_lo = (rest - wr_mid.astype(F32)).astype(BF16)
    carry = jnp.zeros((n_experts, 1), F32)
    counts = jnp.zeros((8, n_experts), F32)
    probs = jnp.zeros((8, n_experts), F32)
    for i in range(rows // block):
        cols = pl.ds(i * block, block)
        h = hidden_ref[cols, :]
        z = dot(wr_lo, h, NT) + dot(wr_mid, h, NT) + dot(wr_hi, h, NT)
        e = jnp.exp(z - jnp.max(z, axis=0, keepdims=True))
        p = e / jnp.sum(e, axis=0, keepdims=True)
        prob_ref[:, cols] = p
        id0 = ids_ref[0:1, cols]
        id1 = ids_ref[1:2, cols]
        hit0 = iota_e == id0
        hit1 = iota_e == id1
        p0 = jnp.sum(jnp.where(hit0, p, 0.0), axis=0, keepdims=True)
        p1 = jnp.sum(jnp.where(hit1, p, 0.0), axis=0, keepdims=True)
        den = p0 + p1
        gate_ref[0:1, cols] = p0 / den
        gate_ref[1:2, cols] = p1 / den
        hits = jnp.where(hit0 | hit1, 1.0, 0.0).astype(F32)
        hits_b = hits.astype(BF16)
        rank = dot(hits_b, upper) + carry
        r0 = jnp.sum(jnp.where(hit0, rank, 0.0), axis=0, keepdims=True)
        r1 = jnp.sum(jnp.where(hit1, rank, 0.0), axis=0, keepdims=True)
        pos_ref[0:1, cols] = id0 * per_expert + r0.astype(jnp.int32)
        pos_ref[1:2, cols] = id1 * per_expert + r1.astype(jnp.int32)
        carry = carry + jnp.sum(hits, axis=1, keepdims=True)
        counts = counts + dot(ones, hits_b, NT)
        probs = probs + dot(ones_f, p, NT, HI)
    stat_ref[:, 0:n_experts] = counts
    stat_ref[:, n_experts:2 * n_experts] = probs


def scatter_kernel(steps, pos_ref, gate_ref, hidden_ref, dout_ref, send_ref, xf_ref, mf_ref, slots_ref):
    step = pl.program_id(0)
    block, d = hidden_ref.shape
    tile = send_ref.shape[0]

    @pl.when(step < steps)
    def _():
        xf_ref[...] = hidden_ref[...].astype(F32)
        mf_ref[...] = OUT_SCALE * dout_ref[...].astype(F32)

        def one(i, _):
            n = step * block + i
            x = xf_ref[pl.ds(i, 1), :]
            m = mf_ref[pl.ds(i, 1), :]
            for k in range(2):
                q = pos_ref[k, n]
                slots_ref[pl.ds(q, 1), 0:d] = x
                slots_ref[pl.ds(q, 1), d:2 * d] = gate_ref[k, n] * m
            return 0

        lax.fori_loop(0, block, one, 0, unroll=8)

    @pl.when(step >= steps)
    def _():
        start = pl.multiple_of((step - steps) * tile, tile)
        send_ref[...] = slots_ref[pl.ds(start, tile), :].astype(BF16)


def expert_kernel(
    ep, etp, capacity, pair,
    send_ref, stat_ref, w1_ref, w3_ref, w2_ref,
    back_ref, g1_ref, g3_ref, g2_ref, tab_out_ref,
    x_ref, w13_ref, w2f_ref, ga13_ref, ga2_ref, ga2t_ref, xm_ref, u_ref, dab_ref, tab_ref,
    stat_send, stat_recv, w_send, w13_recv, w2_recv, x_send, x_recv, back_send, back_recv, g_send, g_recv,
):
    n_dev = ep * etp
    n_slots = x_ref.shape[0]
    rows = x_ref.shape[2]
    d = w1_ref.shape[1]
    part = w1_ref.shape[2]
    ff = w2f_ref.shape[1]
    bits = n_dev.bit_length() - 1
    etp_bits = etp.bit_length() - 1
    me_o = lax.axis_index("ep")
    me_t = lax.axis_index("etp")
    me = me_o * etp + me_t

    def where_is(peer):
        return {"ep": peer // etp, "etp": peer % etp}

    def remote(src, dst, send, recv, peer):
        pltpu.make_async_remote_copy(src_ref=src, dst_ref=dst, send_sem=send, recv_sem=recv, device_id=where_is(peer), device_id_type=MESH).start()

    def wait_bytes(ref, sem):
        pltpu.make_async_copy(ref, ref, sem).wait()

    barrier = pltpu.get_barrier_semaphore()

    def hello(i, _):
        pl.semaphore_signal(barrier, inc=1, device_id=where_is((me + i) % n_dev), device_id_type=MESH)
        return 0

    lax.fori_loop(1, n_dev, hello, 0)
    pl.semaphore_wait(barrier, n_dev - 1)

    def order(i):
        return flip(me, (i * 11) % n_dev, bits)

    def send_stats(i, _):
        remote(stat_ref, tab_ref.at[me], stat_send, stat_recv, order(i))
        return 0

    lax.fori_loop(1, n_dev, send_stats, 0)
    tab_ref[me] = stat_ref[...]

    def lanes(offset, t):
        return pl.ds(pl.multiple_of(offset + t * part, part), part)

    def send_slot(j, _):
        mine = me_t * n_slots + j
        pltpu.make_async_copy(w1_ref.at[mine], w13_ref.at[j, :, lanes(0, me_t)], w13_recv.at[j]).start()
        pltpu.make_async_copy(w3_ref.at[mine], w13_ref.at[j, :, lanes(ff, me_t)], w13_recv.at[j]).start()
        pltpu.make_async_copy(w2_ref.at[mine], w2f_ref.at[j, lanes(0, me_t), :], w2_recv.at[j]).start()

        def weights(i, _):
            t = flip(me_t, i, etp_bits)
            peer = me_o * etp + t
            theirs = t * n_slots + j
            remote(w1_ref.at[theirs], w13_ref.at[j, :, lanes(0, me_t)], w_send, w13_recv.at[j], peer)
            remote(w3_ref.at[theirs], w13_ref.at[j, :, lanes(ff, me_t)], w_send, w13_recv.at[j], peer)
            remote(w2_ref.at[theirs], w2f_ref.at[j, lanes(0, me_t), :], w_send, w2_recv.at[j], peer)
            return 0

        lax.fori_loop(1, etp, weights, 0)
        pltpu.make_async_copy(send_ref.at[me * n_slots + j], x_ref.at[j, me], x_recv.at[j]).start()

        def tokens(i, _):
            peer = order(i)
            remote(send_ref.at[peer * n_slots + j], x_ref.at[j, me], x_send, x_recv.at[j], peer)
            return 0

        lax.fori_loop(1, n_dev, tokens, 0)
        return 0

    lax.fori_loop(0, n_slots, send_slot, 0)

    wait_bytes(tab_ref.at[0:n_dev - 1], stat_recv)
    tab_out_ref[...] = tab_ref[...]
    table = tab_ref[:, 0, :]
    shape = table.shape
    below = (lax.broadcasted_iota(jnp.int32, (n_dev, n_dev), 1) < lax.broadcasted_iota(jnp.int32, (n_dev, n_dev), 0)).astype(F32)
    keep = jnp.minimum(table, capacity - dot(below, table, precision=HI))
    src_iota = lax.broadcasted_iota(jnp.int32, shape, 0)
    lane_iota = lax.broadcasted_iota(jnp.int32, shape, 1)
    row_iota = lax.broadcasted_iota(jnp.int32, (rows, 2 * d), 0).astype(F32)
    n_blocks = n_dev // pair
    block_bits = n_blocks.bit_length() - 1

    def give_back(j, src):
        @pl.when(src == me)
        def _():
            pltpu.make_async_copy(x_ref.at[j, me], back_ref.at[me * n_slots + j], back_recv).start()

        @pl.when(src != me)
        def _():
            remote(x_ref.at[j, src], back_ref.at[me * n_slots + j], back_send, back_recv, src)

    def do_slot(j, _):
        wait_bytes(w13_ref.at[j], w13_recv.at[j])
        wait_bytes(w2f_ref.at[j], w2_recv.at[j])
        wait_bytes(x_ref.at[j], x_recv.at[j])
        ga13_ref[j] = jnp.zeros((d, 2 * ff), F32)
        ga2t_ref[...] = jnp.zeros((d, ff), F32)

        def first_of(b):
            return flip(me // pair, b, block_bits) * pair

        def do_block(b, _):
            first = first_of(b)
            for s in range(pair):
                limit = jnp.sum(jnp.where((src_iota == first + s) & (lane_iota == me * n_slots + j), keep, 0.0), keepdims=True)
                full = x_ref[j, first + s].astype(F32)
                xm_ref[s * rows:(s + 1) * rows, :] = jnp.where(row_iota < limit, full, 0.0).astype(BF16)
            x = xm_ref[:, 0:d]
            c = xm_ref[:, d:2 * d]
            for q in range(ff // part):
                here = slice(q * part, (q + 1) * part)
                there = slice(ff + q * part, ff + (q + 1) * part)
                a = dot(x, w13_ref[j, :, here])
                v = dot(x, w13_ref[j, :, there])
                du = dot(c, w2f_ref[j, here, :], NT)
                sig = jax.nn.sigmoid(a)
                silu = a * sig
                u_ref[:, here] = (silu * v).astype(BF16)
                dab_ref[:, here] = (du * v * sig * (1.0 + a * (1.0 - sig))).astype(BF16)
                dab_ref[:, there] = (du * silu).astype(BF16)
            y = dot(u_ref[...], w2f_ref[j]).astype(BF16)
            dx = dot(dab_ref[...], w13_ref[j], NT).astype(BF16)
            for s in range(pair):
                x_ref[j, first + s, :, 0:d] = y[s * rows:(s + 1) * rows]
                x_ref[j, first + s, :, d:2 * d] = dx[s * rows:(s + 1) * rows]
            ga13_ref[j] += dot(x, dab_ref[...], TN)
            ga2t_ref[...] += dot(c, u_ref[...], TN)

            @pl.when(b > 0)
            def _():
                for s in range(pair):
                    give_back(j, first_of(b - 1) + s)

            return 0

        lax.fori_loop(0, n_blocks, do_block, 0)
        ga2_ref[j] = ga2t_ref[...].T
        for s in range(pair):
            give_back(j, first_of(n_blocks - 1) + s)

        mine = me_t * n_slots + j
        pltpu.make_async_copy(ga13_ref.at[j, :, lanes(0, me_t)], g1_ref.at[mine], g_recv.at[0]).start()
        pltpu.make_async_copy(ga13_ref.at[j, :, lanes(ff, me_t)], g3_ref.at[mine], g_recv.at[1]).start()
        pltpu.make_async_copy(ga2_ref.at[j, lanes(0, me_t), :], g2_ref.at[mine], g_recv.at[2]).start()

        def grads(i, _):
            t = flip(me_t, i, etp_bits)
            peer = me_o * etp + t
            remote(ga13_ref.at[j, :, lanes(0, t)], g1_ref.at[mine], g_send, g_recv.at[0], peer)
            remote(ga13_ref.at[j, :, lanes(ff, t)], g3_ref.at[mine], g_send, g_recv.at[1], peer)
            remote(ga2_ref.at[j, lanes(0, t), :], g2_ref.at[mine], g_send, g_recv.at[2], peer)
            return 0

        lax.fori_loop(1, etp, grads, 0)
        return 0

    lax.fori_loop(0, n_slots, do_slot, 0)

    others = (n_dev - 1) * n_slots
    wait_bytes(tab_ref.at[0:n_dev - 1], stat_send)
    for _ in range(3):
        wait_bytes(w1_ref.at[0:(etp - 1) * n_slots], w_send)
    wait_bytes(send_ref.at[0:others], x_send)
    wait_bytes(send_ref.at[0:others], back_send)
    for _ in range(3):
        wait_bytes(g1_ref.at[0:(etp - 1) * n_slots], g_send)
    wait_bytes(back_ref, back_recv)
    wait_bytes(g1_ref, g_recv.at[0])
    wait_bytes(g3_ref, g_recv.at[1])
    wait_bytes(g2_ref, g_recv.at[2])


def combine_kernel(
    n_tokens, chunk,
    pos_ref, gates_ref, back_ref, tab_ref, wr_ref, hidden_ref, dout_ref, ids_ref, gate_ref, prob_ref,
    out_ref, dh_ref, dwr_ref, aux_ref,
    rows_ref, stage_ref, y_ref, mix_ref, sem,
):
    step = pl.program_id(0)
    block, d = hidden_ref.shape
    n_experts = wr_ref.shape[0]
    n_chunks = rows_ref.shape[0] // chunk

    totals = jnp.sum(tab_ref[:, 0:1, :], axis=0)
    frac = totals[:, 0:n_experts] / (2 * n_tokens)

    def fetch(i, slot):
        start = pl.multiple_of(i * chunk, chunk)
        return pltpu.make_async_copy(back_ref.at[pl.ds(start, chunk), :], stage_ref.at[slot], sem.at[slot])

    @pl.when(step == 0)
    def _():
        fetch(0, 0).start()

        def body(i, _):
            slot = i % 2

            @pl.when(i + 1 < n_chunks)
            def _():
                fetch(i + 1, 1 - slot).start()

            fetch(i, slot).wait()
            rows_ref[pl.ds(pl.multiple_of(i * chunk, chunk), chunk), :] = stage_ref[slot].astype(F32)
            return 0

        lax.fori_loop(0, n_chunks, body, 0)
        dwr_ref[...] = jnp.zeros_like(dwr_ref)
        mean_prob = totals[:, n_experts:2 * n_experts] / n_tokens
        aux_ref[0, 0] = AUX_COEF * n_experts * jnp.sum(frac * mean_prob)

    def one(i, _):
        n = step * block + i
        r0 = rows_ref[pl.ds(pos_ref[0, n], 1), :]
        r1 = rows_ref[pl.ds(pos_ref[1, n], 1), :]
        y0, y1 = r0[:, 0:d], r1[:, 0:d]
        y_ref[pl.ds(i, 1), 0:d] = y0
        y_ref[pl.ds(i, 1), d:2 * d] = y1
        mix_ref[pl.ds(i, 1), 0:d] = gates_ref[0, n] * y0 + gates_ref[1, n] * y1
        mix_ref[pl.ds(i, 1), d:2 * d] = r0[:, d:2 * d] + r1[:, d:2 * d]
        return 0

    lax.fori_loop(0, block, one, 0, unroll=8)

    h = hidden_ref[...].astype(F32)
    dy = dout_ref[...].astype(F32)
    m = OUT_SCALE * dy
    out_ref[...] = (h + OUT_SCALE * mix_ref[:, 0:d]).astype(BF16)

    ones = jnp.ones((8, d), F32)
    dg0 = dot(ones, m * y_ref[:, 0:d], NT, HI)[0:1]
    dg1 = dot(ones, m * y_ref[:, d:2 * d], NT, HI)[0:1]
    p = prob_ref[...]
    iota_e = lax.broadcasted_iota(jnp.int32, p.shape, 0)
    hit0 = iota_e == ids_ref[0:1, :]
    hit1 = iota_e == ids_ref[1:2, :]
    den = jnp.sum(jnp.where(hit0 | hit1, p, 0.0), axis=0, keepdims=True)
    mean = gate_ref[0:1, :] * dg0 + gate_ref[1:2, :] * dg1
    eye = lax.broadcasted_iota(jnp.int32, (n_experts, n_experts), 0) == lax.broadcasted_iota(jnp.int32, (n_experts, n_experts), 1)
    ct = (AUX_COEF * n_experts / n_tokens) * jnp.sum(jnp.where(eye, frac, 0.0), axis=1, keepdims=True)
    dp = jnp.where(hit0, (dg0 - mean) / den, 0.0) + jnp.where(hit1, (dg1 - mean) / den, 0.0) + ct
    dz = p * (dp - jnp.sum(p * dp, axis=0, keepdims=True))
    dwr_ref[...] += dot(dz, h, precision=HI)
    dh_ref[...] = (dy + mix_ref[:, d:2 * d] + dot(dz, wr_ref[...], TN, HI)).astype(BF16)


def sum_kernel(ep, etp, part_ref, out_ref, box_ref, mine_ref, all_ref, send1, recv1, send2, recv2):
    n_dev = ep * etp
    across = part_ref.shape[1] // 128
    me = lax.axis_index("ep") * etp + lax.axis_index("etp")

    def where_is(peer):
        return {"ep": peer // etp, "etp": peer % etp}

    def tile(ref, i):
        return ref.at[pl.ds(pl.multiple_of((i // across) * 8, 8), 8), pl.ds(pl.multiple_of((i % across) * 128, 128), 128)]

    def wait_bytes(ref, sem):
        pltpu.make_async_copy(ref, ref, sem).wait()

    barrier = pltpu.get_barrier_semaphore()

    def hello(i, _):
        pl.semaphore_signal(barrier, inc=1, device_id=where_is((me + i) % n_dev), device_id_type=MESH)
        return 0

    lax.fori_loop(1, n_dev, hello, 0)
    pl.semaphore_wait(barrier, n_dev - 1)

    def first(i, _):
        peer = (me + i) % n_dev
        pltpu.make_async_remote_copy(tile(part_ref, peer), box_ref.at[me], send1, recv1, device_id=where_is(peer), device_id_type=MESH).start()
        return 0

    lax.fori_loop(1, n_dev, first, 0)
    pltpu.make_async_copy(tile(part_ref, me), box_ref.at[me], recv1).start()
    wait_bytes(box_ref, recv1)
    mine_ref[...] = jnp.sum(box_ref[...], axis=0)

    def second(i, _):
        peer = (me + i) % n_dev
        pltpu.make_async_remote_copy(mine_ref, all_ref.at[me], send2, recv2, device_id=where_is(peer), device_id_type=MESH).start()
        return 0

    lax.fori_loop(1, n_dev, second, 0)
    all_ref[me] = mine_ref[...]
    wait_bytes(all_ref.at[0:n_dev - 1], recv2)
    for i in range(n_dev):
        out_ref[(i // across) * 8:(i // across) * 8 + 8, (i % across) * 128:(i % across) * 128 + 128] = all_ref[i]
    wait_bytes(box_ref.at[0:n_dev - 1], send1)
    wait_bytes(all_ref.at[0:n_dev - 1], send2)


def solution(mesh):
    ep_size = mesh.shape["ep"]
    etp_size = mesh.shape["etp"]
    n_dev = ep_size * etp_size
    all_axes = ("ep", "etp")
    tok_spec = P(all_axes, None)
    gate_spec = P("ep", None, "etp")
    down_spec = P("ep", "etp", None)

    def layer(hidden, w_router, expert_ids, d_out, w_gate, w_up, w_down):
        rows, d = hidden.shape
        n_experts = w_router.shape[1]
        n_tokens = rows * n_dev
        capacity = (5 * n_tokens + 2 * n_experts - 1) // (2 * n_experts)
        per_expert = 7 * rows // (2 * n_experts)
        n_slots = n_experts // n_dev
        local_experts, _, part = w_gate.shape
        ff = part * etp_size
        all_slots = n_experts * per_expert
        ids_t = expert_ids.T
        wr_t = w_router.T

        vmem = pl.BlockSpec(memory_space=pltpu.VMEM)
        smem = pl.BlockSpec(memory_space=pltpu.SMEM)
        anywhere = pl.BlockSpec(memory_space=pl.ANY)
        big = 60 * 1024 * 1024

        pos, gates, probs, stats = pl.pallas_call(
            functools.partial(route_kernel, per_expert),
            out_shape=(
                jax.ShapeDtypeStruct((2, rows), jnp.int32),
                jax.ShapeDtypeStruct((2, rows), F32),
                jax.ShapeDtypeStruct((n_experts, rows), F32),
                jax.ShapeDtypeStruct((8, 2 * n_experts), F32),
            ),
            in_specs=[vmem] * 3,
            out_specs=(vmem,) * 4,
            name="route",
        )(hidden, wr_t, ids_t)

        block = min(512, rows)
        steps = rows // block
        tile = n_slots * per_expert
        tiles = all_slots // tile
        send = pl.pallas_call(
            functools.partial(scatter_kernel, steps),
            out_shape=jax.ShapeDtypeStruct((all_slots, 2 * d), BF16),
            grid=(steps + tiles,),
            in_specs=[
                smem, smem,
                pl.BlockSpec((block, d), lambda i: (jnp.minimum(i, steps - 1), 0)),
                pl.BlockSpec((block, d), lambda i: (jnp.minimum(i, steps - 1), 0)),
            ],
            out_specs=pl.BlockSpec((tile, 2 * d), lambda i: (jnp.maximum(i - steps, 0), 0)),
            scratch_shapes=[pltpu.VMEM((block, d), F32), pltpu.VMEM((block, d), F32), pltpu.VMEM((all_slots, 2 * d), F32)],
            compiler_params=pltpu.CompilerParams(vmem_limit_bytes=big),
            name="scatter",
        )(pos, gates, hidden, d_out)
        send = send.reshape(n_experts, per_expert, 2 * d)

        pair = 2
        dma = pltpu.SemaphoreType.DMA
        grad = jax.ShapeDtypeStruct((local_experts, d, part), F32)
        back, g_gate, g_up, g_down, table = pl.pallas_call(
            functools.partial(expert_kernel, ep_size, etp_size, float(capacity), pair),
            out_shape=(
                jax.ShapeDtypeStruct((n_experts, per_expert, 2 * d), BF16),
                grad, grad,
                jax.ShapeDtypeStruct((local_experts, part, d), F32),
                jax.ShapeDtypeStruct((n_dev, 8, 2 * n_experts), F32),
            ),
            in_specs=[anywhere, vmem, anywhere, anywhere, anywhere],
            out_specs=(anywhere,) * 4 + (vmem,),
            scratch_shapes=[
                pltpu.VMEM((n_slots, n_dev, per_expert, 2 * d), BF16),
                pltpu.VMEM((n_slots, d, 2 * ff), BF16),
                pltpu.VMEM((n_slots, ff, d), BF16),
                pltpu.VMEM((n_slots, d, 2 * ff), F32),
                pltpu.VMEM((n_slots, ff, d), F32),
                pltpu.VMEM((d, ff), F32),
                pltpu.VMEM((pair * per_expert, 2 * d), BF16),
                pltpu.VMEM((pair * per_expert, ff), BF16),
                pltpu.VMEM((pair * per_expert, 2 * ff), BF16),
                pltpu.VMEM((n_dev, 8, 2 * n_experts), F32),
                dma, dma, dma, dma((n_slots,)), dma((n_slots,)), dma, dma((n_slots,)), dma, dma, dma, dma((3,)),
            ],
            compiler_params=pltpu.CompilerParams(collective_id=0, has_side_effects=True, vmem_limit_bytes=big),
            name="experts",
        )(send, stats, w_gate, w_up, w_down)

        cols = lambda n: pl.BlockSpec((n, block), lambda i: (0, i))
        tok = pl.BlockSpec((block, d), lambda i: (i, 0))
        output, d_hidden, dwr_part, aux_loss = pl.pallas_call(
            functools.partial(combine_kernel, n_tokens, tile),
            out_shape=(
                jax.ShapeDtypeStruct((rows, d), BF16),
                jax.ShapeDtypeStruct((rows, d), BF16),
                jax.ShapeDtypeStruct((n_experts, d), F32),
                jax.ShapeDtypeStruct((1, 1), F32),
            ),
            grid=(steps,),
            in_specs=[smem, smem, anywhere, vmem, vmem, tok, tok, cols(2), cols(2), cols(n_experts)],
            out_specs=(tok, tok, pl.BlockSpec((n_experts, d), lambda i: (0, 0)), smem),
            scratch_shapes=[
                pltpu.VMEM((all_slots, 2 * d), F32),
                pltpu.VMEM((2, tile, 2 * d), BF16),
                pltpu.VMEM((block, 2 * d), F32),
                pltpu.VMEM((block, 2 * d), F32),
                dma((2,)),
            ],
            compiler_params=pltpu.CompilerParams(vmem_limit_bytes=big),
            name="combine",
        )(pos, gates, back.reshape(all_slots, 2 * d), table, wr_t, hidden, d_out, ids_t, gates, probs)

        dwr = pl.pallas_call(
            functools.partial(sum_kernel, ep_size, etp_size),
            out_shape=jax.ShapeDtypeStruct((n_experts, d), F32),
            in_specs=[vmem],
            out_specs=vmem,
            scratch_shapes=[
                pltpu.VMEM((n_dev, 8, 128), F32), pltpu.VMEM((8, 128), F32), pltpu.VMEM((n_dev, 8, 128), F32),
                dma, dma, dma, dma,
            ],
            compiler_params=pltpu.CompilerParams(collective_id=1, has_side_effects=True),
            name="sum_router",
        )(dwr_part)
        return output, d_hidden, dwr.T, aux_loss.reshape(()), g_gate, g_up, g_down

    return jax.shard_map(layer, mesh=mesh, in_specs=(tok_spec, P(), tok_spec, tok_spec, gate_spec, gate_spec, down_spec), out_specs=(tok_spec, tok_spec, P(), P(), gate_spec, gate_spec, down_spec), check_vma=False)
```

```python
import functools
import jax
import jax.numpy as jnp
from jax import lax
from jax.experimental import pallas as pl
from jax.experimental.pallas import tpu as pltpu
from jax.sharding import PartitionSpec as P

AUX_COEF = 0.01
OUT_SCALE = 2.0
F32 = jnp.float32
BF16 = jnp.bfloat16
HI = lax.Precision.HIGHEST
MESH = pl.DeviceIdType.MESH
NT = (((1,), (1,)), ((), ()))
TN = (((0,), (0,)), ((), ()))


def dot(a, b, dims=(((1,), (0,)), ((), ())), precision=None):
    return lax.dot_general(a, b, dims, precision=precision, preferred_element_type=F32)


def flip(index, mask, bits):
    total = 0
    for bit in range(bits):
        total = total + ((index // 2**bit + mask // 2**bit) % 2) * 2**bit
    return total


def route_kernel(per_expert, hidden_ref, wr_ref, ids_ref, pos_ref, gate_ref, prob_ref, stat_ref):
    n_experts = wr_ref.shape[0]
    rows = hidden_ref.shape[0]
    block = min(512, rows)
    iota_e = lax.broadcasted_iota(jnp.int32, (n_experts, block), 0)
    upper = (lax.broadcasted_iota(jnp.int32, (block, block), 0) < lax.broadcasted_iota(jnp.int32, (block, block), 1)).astype(BF16)
    ones = jnp.ones((8, block), BF16)
    ones_f = jnp.ones((8, block), F32)
    wr = wr_ref[...]
    wr_hi = wr.astype(BF16)
    rest = wr - wr_hi.astype(F32)
    wr_mid = rest.astype(BF16)
    wr_lo = (rest - wr_mid.astype(F32)).astype(BF16)
    carry = jnp.zeros((n_experts, 1), F32)
    counts = jnp.zeros((8, n_experts), F32)
    probs = jnp.zeros((8, n_experts), F32)
    for i in range(rows // block):
        cols = pl.ds(i * block, block)
        h = hidden_ref[cols, :]
        z = dot(wr_lo, h, NT) + dot(wr_mid, h, NT) + dot(wr_hi, h, NT)
        e = jnp.exp(z - jnp.max(z, axis=0, keepdims=True))
        p = e / jnp.sum(e, axis=0, keepdims=True)
        prob_ref[:, cols] = p
        id0 = ids_ref[0:1, cols]
        id1 = ids_ref[1:2, cols]
        hit0 = iota_e == id0
        hit1 = iota_e == id1
        p0 = jnp.sum(jnp.where(hit0, p, 0.0), axis=0, keepdims=True)
        p1 = jnp.sum(jnp.where(hit1, p, 0.0), axis=0, keepdims=True)
        den = p0 + p1
        gate_ref[0:1, cols] = p0 / den
        gate_ref[1:2, cols] = p1 / den
        hits = jnp.where(hit0 | hit1, 1.0, 0.0).astype(F32)
        hits_b = hits.astype(BF16)
        rank = dot(hits_b, upper) + carry
        r0 = jnp.sum(jnp.where(hit0, rank, 0.0), axis=0, keepdims=True)
        r1 = jnp.sum(jnp.where(hit1, rank, 0.0), axis=0, keepdims=True)
        pos_ref[0:1, cols] = id0 * per_expert + r0.astype(jnp.int32)
        pos_ref[1:2, cols] = id1 * per_expert + r1.astype(jnp.int32)
        carry = carry + jnp.sum(hits, axis=1, keepdims=True)
        counts = counts + dot(ones, hits_b, NT)
        probs = probs + dot(ones_f, p, NT, HI)
    stat_ref[:, 0:n_experts] = counts
    stat_ref[:, n_experts:2 * n_experts] = probs


def scatter_kernel(steps, pos_ref, gate_ref, hidden_ref, dout_ref, send_ref, xf_ref, mf_ref, slots_ref):
    step = pl.program_id(0)
    block, d = hidden_ref.shape
    tile = send_ref.shape[0]

    @pl.when(step < steps)
    def _():
        xf_ref[...] = hidden_ref[...].astype(F32)
        mf_ref[...] = OUT_SCALE * dout_ref[...].astype(F32)

        def one(i, _):
            n = step * block + i
            x = xf_ref[pl.ds(i, 1), :]
            m = mf_ref[pl.ds(i, 1), :]
            for k in range(2):
                q = pos_ref[k, n]
                slots_ref[pl.ds(q, 1), 0:d] = x
                slots_ref[pl.ds(q, 1), d:2 * d] = gate_ref[k, n] * m
            return 0

        lax.fori_loop(0, block, one, 0, unroll=8)

    @pl.when(step >= steps)
    def _():
        start = pl.multiple_of((step - steps) * tile, tile)
        send_ref[...] = slots_ref[pl.ds(start, tile), :].astype(BF16)


def expert_kernel(
    ep, etp, capacity, pair,
    send_ref, stat_ref, *refs,
):
    weights, refs = refs[:etp], refs[etp:]
    back_ref, refs = refs[0], refs[1:]
    grads, refs = refs[:etp], refs[etp:]
    tab_out_ref, x_ref, w13_ref, w2f_ref, ga13_ref, ga2_ref, ga2t_ref, xm_ref, u_ref, dab_ref, tab_ref = refs[:11]
    stat_send, stat_recv, w13_recv, w2_recv, x_send, x_recv, back_send, back_recv, g_done = refs[11:]
    n_dev = ep * etp
    n_slots = x_ref.shape[0]
    rows = x_ref.shape[2]
    d = w2f_ref.shape[2]
    ff = w2f_ref.shape[1]
    part = ff // etp
    bits = n_dev.bit_length() - 1
    etp_bits = etp.bit_length() - 1
    me_o = lax.axis_index("ep")
    me_t = lax.axis_index("etp")
    me = me_o * etp + me_t

    def where_is(peer):
        return {"ep": peer // etp, "etp": peer % etp}

    def remote(src, dst, send, recv, peer):
        pltpu.make_async_remote_copy(src_ref=src, dst_ref=dst, send_sem=send, recv_sem=recv, device_id=where_is(peer), device_id_type=MESH).start()

    def wait_bytes(ref, sem):
        pltpu.make_async_copy(ref, ref, sem).wait()

    barrier = pltpu.get_barrier_semaphore()

    def hello(i, _):
        pl.semaphore_signal(barrier, inc=1, device_id=where_is((me + i) % n_dev), device_id_type=MESH)
        return 0

    lax.fori_loop(1, n_dev, hello, 0)
    pl.semaphore_wait(barrier, n_dev - 1)

    def order(i):
        return flip(me, (i * 11) % n_dev, bits)

    def send_stats(i, _):
        remote(stat_ref, tab_ref.at[me], stat_send, stat_recv, order(i))
        return 0

    lax.fori_loop(1, n_dev, send_stats, 0)
    tab_ref[me] = stat_ref[...]

    def lanes(offset, t):
        return pl.ds(pl.multiple_of(offset + t * part, part), part)

    for b in range(etp):
        t = flip(me_t, b, etp_bits)
        pltpu.make_async_copy(weights[b].at[0:n_slots], w13_ref.at[:, :, lanes(0, t)], w13_recv).start()
        pltpu.make_async_copy(weights[b].at[n_slots:2 * n_slots], w13_ref.at[:, :, lanes(ff, t)], w13_recv).start()
        pltpu.make_async_copy(weights[b].at[2 * n_slots:3 * n_slots], w2f_ref.at[:, lanes(0, t), :], w2_recv).start()

    def send_slot(j, _):
        pltpu.make_async_copy(send_ref.at[me * n_slots + j], x_ref.at[j, me], x_recv.at[j]).start()

        def tokens(i, _):
            peer = order(i)
            remote(send_ref.at[peer * n_slots + j], x_ref.at[j, me], x_send, x_recv.at[j], peer)
            return 0

        lax.fori_loop(1, n_dev, tokens, 0)
        return 0

    lax.fori_loop(0, n_slots, send_slot, 0)

    wait_bytes(w13_ref, w13_recv)
    wait_bytes(w2f_ref, w2_recv)

    wait_bytes(tab_ref.at[0:n_dev - 1], stat_recv)
    tab_out_ref[...] = tab_ref[...]
    table = tab_ref[:, 0, :]
    shape = table.shape
    below = (lax.broadcasted_iota(jnp.int32, (n_dev, n_dev), 1) < lax.broadcasted_iota(jnp.int32, (n_dev, n_dev), 0)).astype(F32)
    keep = jnp.minimum(table, capacity - dot(below, table, precision=HI))
    src_iota = lax.broadcasted_iota(jnp.int32, shape, 0)
    lane_iota = lax.broadcasted_iota(jnp.int32, shape, 1)
    row_iota = lax.broadcasted_iota(jnp.int32, (rows, 2 * d), 0).astype(F32)
    n_blocks = n_dev // pair
    block_bits = n_blocks.bit_length() - 1

    def give_back(j, src):
        @pl.when(src == me)
        def _():
            pltpu.make_async_copy(x_ref.at[j, me], back_ref.at[me * n_slots + j], back_recv).start()

        @pl.when(src != me)
        def _():
            remote(x_ref.at[j, src], back_ref.at[me * n_slots + j], back_send, back_recv, src)

    def do_slot(j, _):
        wait_bytes(x_ref.at[j], x_recv.at[j])
        ga13_ref[j] = jnp.zeros((d, 2 * ff), F32)
        ga2t_ref[...] = jnp.zeros((d, ff), F32)

        def first_of(b):
            return flip(me // pair, b, block_bits) * pair

        def do_block(b, _):
            first = first_of(b)
            for s in range(pair):
                limit = jnp.sum(jnp.where((src_iota == first + s) & (lane_iota == me * n_slots + j), keep, 0.0), keepdims=True)
                full = x_ref[j, first + s].astype(F32)
                xm_ref[s * rows:(s + 1) * rows, :] = jnp.where(row_iota < limit, full, 0.0).astype(BF16)
            x = xm_ref[:, 0:d]
            c = xm_ref[:, d:2 * d]
            for q in range(ff // part):
                here = slice(q * part, (q + 1) * part)
                there = slice(ff + q * part, ff + (q + 1) * part)
                a = dot(x, w13_ref[j, :, here])
                v = dot(x, w13_ref[j, :, there])
                du = dot(c, w2f_ref[j, here, :], NT)
                sig = jax.nn.sigmoid(a)
                silu = a * sig
                u_ref[:, here] = (silu * v).astype(BF16)
                dab_ref[:, here] = (du * v * sig * (1.0 + a * (1.0 - sig))).astype(BF16)
                dab_ref[:, there] = (du * silu).astype(BF16)
            y = dot(u_ref[...], w2f_ref[j]).astype(BF16)
            dx = dot(dab_ref[...], w13_ref[j], NT).astype(BF16)
            for s in range(pair):
                x_ref[j, first + s, :, 0:d] = y[s * rows:(s + 1) * rows]
                x_ref[j, first + s, :, d:2 * d] = dx[s * rows:(s + 1) * rows]
            ga13_ref[j] += dot(x, dab_ref[...], TN)
            ga2t_ref[...] += dot(c, u_ref[...], TN)

            @pl.when(b > 0)
            def _():
                for s in range(pair):
                    give_back(j, first_of(b - 1) + s)

            return 0

        lax.fori_loop(0, n_blocks, do_block, 0)
        ga2_ref[j] = ga2t_ref[...].T
        for s in range(pair):
            give_back(j, first_of(n_blocks - 1) + s)

        for b in range(etp):
            t = flip(me_t, b, etp_bits)
            pltpu.make_async_copy(ga13_ref.at[j, :, lanes(0, t)], grads[b].at[j], g_done).start()
            pltpu.make_async_copy(ga13_ref.at[j, :, lanes(ff, t)], grads[b].at[n_slots + j], g_done).start()
            pltpu.make_async_copy(ga2_ref.at[j, lanes(0, t), :], grads[b].at[2 * n_slots + j], g_done).start()
        return 0

    lax.fori_loop(0, n_slots, do_slot, 0)

    others = (n_dev - 1) * n_slots
    wait_bytes(tab_ref.at[0:n_dev - 1], stat_send)
    wait_bytes(send_ref.at[0:others], x_send)
    wait_bytes(send_ref.at[0:others], back_send)
    wait_bytes(back_ref, back_recv)
    for b in range(etp):
        wait_bytes(grads[b], g_done)


def combine_kernel(
    n_tokens, chunk,
    pos_ref, gates_ref, back_ref, tab_ref, wr_ref, hidden_ref, dout_ref, ids_ref, gate_ref, prob_ref,
    out_ref, dh_ref, dwr_ref, aux_ref,
    rows_ref, stage_ref, y_ref, mix_ref, sem,
):
    step = pl.program_id(0)
    block, d = hidden_ref.shape
    n_experts = wr_ref.shape[0]
    n_chunks = rows_ref.shape[0] // chunk

    totals = jnp.sum(tab_ref[:, 0:1, :], axis=0)
    frac = totals[:, 0:n_experts] / (2 * n_tokens)

    def fetch(i, slot):
        start = pl.multiple_of(i * chunk, chunk)
        return pltpu.make_async_copy(back_ref.at[pl.ds(start, chunk), :], stage_ref.at[slot], sem.at[slot])

    @pl.when(step == 0)
    def _():
        fetch(0, 0).start()

        def body(i, _):
            slot = i % 2

            @pl.when(i + 1 < n_chunks)
            def _():
                fetch(i + 1, 1 - slot).start()

            fetch(i, slot).wait()
            rows_ref[pl.ds(pl.multiple_of(i * chunk, chunk), chunk), :] = stage_ref[slot].astype(F32)
            return 0

        lax.fori_loop(0, n_chunks, body, 0)
        dwr_ref[...] = jnp.zeros_like(dwr_ref)
        mean_prob = totals[:, n_experts:2 * n_experts] / n_tokens
        aux_ref[0, 0] = AUX_COEF * n_experts * jnp.sum(frac * mean_prob)

    def one(i, _):
        n = step * block + i
        r0 = rows_ref[pl.ds(pos_ref[0, n], 1), :]
        r1 = rows_ref[pl.ds(pos_ref[1, n], 1), :]
        y0, y1 = r0[:, 0:d], r1[:, 0:d]
        y_ref[pl.ds(i, 1), 0:d] = y0
        y_ref[pl.ds(i, 1), d:2 * d] = y1
        mix_ref[pl.ds(i, 1), 0:d] = gates_ref[0, n] * y0 + gates_ref[1, n] * y1
        mix_ref[pl.ds(i, 1), d:2 * d] = r0[:, d:2 * d] + r1[:, d:2 * d]
        return 0

    lax.fori_loop(0, block, one, 0, unroll=8)

    h = hidden_ref[...].astype(F32)
    dy = dout_ref[...].astype(F32)
    m = OUT_SCALE * dy
    out_ref[...] = (h + OUT_SCALE * mix_ref[:, 0:d]).astype(BF16)

    ones = jnp.ones((8, d), F32)
    dg0 = dot(ones, m * y_ref[:, 0:d], NT, HI)[0:1]
    dg1 = dot(ones, m * y_ref[:, d:2 * d], NT, HI)[0:1]
    p = prob_ref[...]
    iota_e = lax.broadcasted_iota(jnp.int32, p.shape, 0)
    hit0 = iota_e == ids_ref[0:1, :]
    hit1 = iota_e == ids_ref[1:2, :]
    den = jnp.sum(jnp.where(hit0 | hit1, p, 0.0), axis=0, keepdims=True)
    mean = gate_ref[0:1, :] * dg0 + gate_ref[1:2, :] * dg1
    eye = lax.broadcasted_iota(jnp.int32, (n_experts, n_experts), 0) == lax.broadcasted_iota(jnp.int32, (n_experts, n_experts), 1)
    ct = (AUX_COEF * n_experts / n_tokens) * jnp.sum(jnp.where(eye, frac, 0.0), axis=1, keepdims=True)
    dp = jnp.where(hit0, (dg0 - mean) / den, 0.0) + jnp.where(hit1, (dg1 - mean) / den, 0.0) + ct
    dz = p * (dp - jnp.sum(p * dp, axis=0, keepdims=True))
    dwr_ref[...] += dot(dz, h, precision=HI)
    dh_ref[...] = (dy + mix_ref[:, d:2 * d] + dot(dz, wr_ref[...], TN, HI)).astype(BF16)


def sum_kernel(ep, etp, part_ref, out_ref, box_ref, mine_ref, all_ref, send1, recv1, send2, recv2):
    n_dev = ep * etp
    across = part_ref.shape[1] // 128
    me = lax.axis_index("ep") * etp + lax.axis_index("etp")

    def where_is(peer):
        return {"ep": peer // etp, "etp": peer % etp}

    def tile(ref, i):
        return ref.at[pl.ds(pl.multiple_of((i // across) * 8, 8), 8), pl.ds(pl.multiple_of((i % across) * 128, 128), 128)]

    def wait_bytes(ref, sem):
        pltpu.make_async_copy(ref, ref, sem).wait()

    barrier = pltpu.get_barrier_semaphore()

    def hello(i, _):
        pl.semaphore_signal(barrier, inc=1, device_id=where_is((me + i) % n_dev), device_id_type=MESH)
        return 0

    lax.fori_loop(1, n_dev, hello, 0)
    pl.semaphore_wait(barrier, n_dev - 1)

    def first(i, _):
        peer = (me + i) % n_dev
        pltpu.make_async_remote_copy(tile(part_ref, peer), box_ref.at[me], send1, recv1, device_id=where_is(peer), device_id_type=MESH).start()
        return 0

    lax.fori_loop(1, n_dev, first, 0)
    pltpu.make_async_copy(tile(part_ref, me), box_ref.at[me], recv1).start()
    wait_bytes(box_ref, recv1)
    mine_ref[...] = jnp.sum(box_ref[...], axis=0)

    def second(i, _):
        peer = (me + i) % n_dev
        pltpu.make_async_remote_copy(mine_ref, all_ref.at[me], send2, recv2, device_id=where_is(peer), device_id_type=MESH).start()
        return 0

    lax.fori_loop(1, n_dev, second, 0)
    all_ref[me] = mine_ref[...]
    wait_bytes(all_ref.at[0:n_dev - 1], recv2)
    for i in range(n_dev):
        out_ref[(i // across) * 8:(i // across) * 8 + 8, (i % across) * 128:(i % across) * 128 + 128] = all_ref[i]
    wait_bytes(box_ref.at[0:n_dev - 1], send1)
    wait_bytes(all_ref.at[0:n_dev - 1], send2)


def assemble_kernel(etp, *refs):
    parts, outs = refs[:etp], refs[etp:etp + 3]
    stage_ref, in_sem, out_sem = refs[etp + 3:]
    n_slots = stage_ref.shape[1]
    me_t = lax.axis_index("etp")

    def load(b, w):
        i = b * 3 + w
        return pltpu.make_async_copy(parts[b].at[w * n_slots:(w + 1) * n_slots], stage_ref.at[i], in_sem.at[i])

    def store(b, w):
        t = flip(me_t, b, etp.bit_length() - 1)
        i = b * 3 + w
        return pltpu.make_async_copy(stage_ref.at[i], outs[w].at[pl.ds(t * n_slots, n_slots)], out_sem.at[i])

    every = [(b, w) for b in range(etp) for w in range(3)]
    for b, w in every:
        load(b, w).start()
    for b, w in every:
        load(b, w).wait()
        store(b, w).start()
    for b, w in every:
        store(b, w).wait()


def solution(mesh):
    ep_size = mesh.shape["ep"]
    etp_size = mesh.shape["etp"]
    n_dev = ep_size * etp_size
    all_axes = ("ep", "etp")
    tok_spec = P(all_axes, None)
    gate_spec = P("ep", None, "etp")
    down_spec = P("ep", "etp", None)

    def layer(hidden, w_router, expert_ids, d_out, w_gate, w_up, w_down):
        rows, d = hidden.shape
        n_experts = w_router.shape[1]
        n_tokens = rows * n_dev
        capacity = (5 * n_tokens + 2 * n_experts - 1) // (2 * n_experts)
        per_expert = 7 * rows // (2 * n_experts)
        n_slots = n_experts // n_dev
        local_experts, _, part = w_gate.shape
        ff = part * etp_size
        all_slots = n_experts * per_expert
        me_t = lax.axis_index("etp")
        others = [[(t, t ^ b) for t in range(etp_size)] for b in range(etp_size)]

        def parts_for(t):
            return jnp.concatenate([lax.dynamic_slice_in_dim(w, t * n_slots, n_slots) for w in (w_gate, w_up, w_down)])

        weights = [parts_for(me_t)] + [lax.ppermute(parts_for(me_t ^ b), "etp", others[b]) for b in range(1, etp_size)]
        ids_t = expert_ids.T
        wr_t = w_router.T

        vmem = pl.BlockSpec(memory_space=pltpu.VMEM)
        smem = pl.BlockSpec(memory_space=pltpu.SMEM)
        anywhere = pl.BlockSpec(memory_space=pl.ANY)
        big = 60 * 1024 * 1024

        pos, gates, probs, stats = pl.pallas_call(
            functools.partial(route_kernel, per_expert),
            out_shape=(
                jax.ShapeDtypeStruct((2, rows), jnp.int32),
                jax.ShapeDtypeStruct((2, rows), F32),
                jax.ShapeDtypeStruct((n_experts, rows), F32),
                jax.ShapeDtypeStruct((8, 2 * n_experts), F32),
            ),
            in_specs=[vmem] * 3,
            out_specs=(vmem,) * 4,
            cost_estimate=pl.CostEstimate(flops=5_000_000_000, bytes_accessed=4_000_000, transcendentals=0),
            name="route",
        )(hidden, wr_t, ids_t)

        block = min(512, rows)
        steps = rows // block
        tile = n_slots * per_expert
        tiles = all_slots // tile
        send = pl.pallas_call(
            functools.partial(scatter_kernel, steps),
            out_shape=jax.ShapeDtypeStruct((all_slots, 2 * d), BF16),
            grid=(steps + tiles,),
            in_specs=[
                smem, smem,
                pl.BlockSpec((block, d), lambda i: (jnp.minimum(i, steps - 1), 0)),
                pl.BlockSpec((block, d), lambda i: (jnp.minimum(i, steps - 1), 0)),
            ],
            out_specs=pl.BlockSpec((tile, 2 * d), lambda i: (jnp.maximum(i - steps, 0), 0)),
            scratch_shapes=[pltpu.VMEM((block, d), F32), pltpu.VMEM((block, d), F32), pltpu.VMEM((all_slots, 2 * d), F32)],
            compiler_params=pltpu.CompilerParams(vmem_limit_bytes=big),
            cost_estimate=pl.CostEstimate(flops=50_000_000_000, bytes_accessed=20_000_000, transcendentals=0),
            name="scatter",
        )(pos, gates, hidden, d_out)
        send = send.reshape(n_experts, per_expert, 2 * d)

        pair = 2
        dma = pltpu.SemaphoreType.DMA
        assert part == d
        grad = jax.ShapeDtypeStruct((3 * n_slots, d, part), F32)
        back, *rest = pl.pallas_call(
            functools.partial(expert_kernel, ep_size, etp_size, float(capacity), pair),
            out_shape=(
                jax.ShapeDtypeStruct((n_experts, per_expert, 2 * d), BF16),
                *(grad,) * etp_size,
                jax.ShapeDtypeStruct((n_dev, 8, 2 * n_experts), F32),
            ),
            in_specs=[anywhere, vmem] + [anywhere] * etp_size,
            out_specs=(anywhere,) * (1 + etp_size) + (vmem,),
            scratch_shapes=[
                pltpu.VMEM((n_slots, n_dev, per_expert, 2 * d), BF16),
                pltpu.VMEM((n_slots, d, 2 * ff), BF16),
                pltpu.VMEM((n_slots, ff, d), BF16),
                pltpu.VMEM((n_slots, d, 2 * ff), F32),
                pltpu.VMEM((n_slots, ff, d), F32),
                pltpu.VMEM((d, ff), F32),
                pltpu.VMEM((pair * per_expert, 2 * d), BF16),
                pltpu.VMEM((pair * per_expert, ff), BF16),
                pltpu.VMEM((pair * per_expert, 2 * ff), BF16),
                pltpu.VMEM((n_dev, 8, 2 * n_experts), F32),
                dma, dma, dma, dma, dma, dma((n_slots,)), dma, dma, dma,
            ],
            compiler_params=pltpu.CompilerParams(collective_id=0, has_side_effects=True, vmem_limit_bytes=big),
            cost_estimate=pl.CostEstimate(flops=300_000_000_000, bytes_accessed=60_000_000, transcendentals=0),
            name="experts",
        )(send, stats, *weights)
        table = rest[-1]
        grads = [rest[0]] + [lax.ppermute(rest[b], "etp", others[b]) for b in range(1, etp_size)]

        cols = lambda n: pl.BlockSpec((n, block), lambda i: (0, i))
        tok = pl.BlockSpec((block, d), lambda i: (i, 0))
        output, d_hidden, dwr_part, aux_loss = pl.pallas_call(
            functools.partial(combine_kernel, n_tokens, tile),
            out_shape=(
                jax.ShapeDtypeStruct((rows, d), BF16),
                jax.ShapeDtypeStruct((rows, d), BF16),
                jax.ShapeDtypeStruct((n_experts, d), F32),
                jax.ShapeDtypeStruct((1, 1), F32),
            ),
            grid=(steps,),
            in_specs=[smem, smem, anywhere, vmem, vmem, tok, tok, cols(2), cols(2), cols(n_experts)],
            out_specs=(tok, tok, pl.BlockSpec((n_experts, d), lambda i: (0, 0)), smem),
            scratch_shapes=[
                pltpu.VMEM((all_slots, 2 * d), F32),
                pltpu.VMEM((2, tile, 2 * d), BF16),
                pltpu.VMEM((block, 2 * d), F32),
                pltpu.VMEM((block, 2 * d), F32),
                dma((2,)),
            ],
            compiler_params=pltpu.CompilerParams(vmem_limit_bytes=big),
            cost_estimate=pl.CostEstimate(flops=60_000_000_000, bytes_accessed=30_000_000, transcendentals=0),
            name="combine",
        )(pos, gates, back.reshape(all_slots, 2 * d), table, wr_t, hidden, d_out, ids_t, gates, probs)

        dwr = pl.pallas_call(
            functools.partial(sum_kernel, ep_size, etp_size),
            out_shape=jax.ShapeDtypeStruct((n_experts, d), F32),
            in_specs=[vmem],
            out_specs=vmem,
            scratch_shapes=[
                pltpu.VMEM((n_dev, 8, 128), F32), pltpu.VMEM((8, 128), F32), pltpu.VMEM((n_dev, 8, 128), F32),
                dma, dma, dma, dma,
            ],
            compiler_params=pltpu.CompilerParams(collective_id=1, has_side_effects=True),
            cost_estimate=pl.CostEstimate(flops=10_000_000_000, bytes_accessed=100_000, transcendentals=0),
            name="sum_router",
        )(dwr_part)
        g_gate, g_up, g_down = pl.pallas_call(
            functools.partial(assemble_kernel, etp_size),
            out_shape=(jax.ShapeDtypeStruct((local_experts, d, part), F32),) * 3,
            in_specs=[anywhere] * etp_size,
            out_specs=(anywhere,) * 3,
            scratch_shapes=[pltpu.VMEM((3 * etp_size, n_slots, d, part), F32), dma((3 * etp_size,)), dma((3 * etp_size,))],
            compiler_params=pltpu.CompilerParams(vmem_limit_bytes=big),
            name="assemble",
        )(*grads)
        return output, d_hidden, dwr.T, aux_loss.reshape(()), g_gate, g_up, g_down

    return jax.shard_map(layer, mesh=mesh, in_specs=(tok_spec, P(), tok_spec, tok_spec, gate_spec, gate_spec, down_spec), out_specs=(tok_spec, tok_spec, P(), P(), gate_spec, gate_spec, down_spec), check_vma=False)
```

```python
import functools
import jax
import jax.numpy as jnp
from jax import lax
from jax.experimental import pallas as pl
from jax.experimental.pallas import tpu as pltpu
from jax.sharding import PartitionSpec as P

AUX_COEF = 0.01
OUT_SCALE = 2.0
GROUP = 128
F32 = jnp.float32
BF16 = jnp.bfloat16
HI = lax.Precision.HIGHEST
MESH = pl.DeviceIdType.MESH
NT = (((1,), (1,)), ((), ()))
TN = (((0,), (0,)), ((), ()))


def dot(a, b, dims=(((1,), (0,)), ((), ())), precision=None):
    return lax.dot_general(a, b, dims, precision=precision, preferred_element_type=F32)


def flip(index, mask, bits):
    total = 0
    for bit in range(bits):
        total = total + ((index // 2**bit + mask // 2**bit) % 2) * 2**bit
    return total


def route_kernel(per_expert, hidden_ref, wr_ref, ids_ref, pos_ref, gate_ref, prob_ref, stat_ref):
    n_experts = wr_ref.shape[0]
    rows = hidden_ref.shape[0]
    block = min(512, rows)
    iota_e = lax.broadcasted_iota(jnp.int32, (n_experts, block), 0)
    upper = (lax.broadcasted_iota(jnp.int32, (block, block), 0) < lax.broadcasted_iota(jnp.int32, (block, block), 1)).astype(BF16)
    ones = jnp.ones((8, block), BF16)
    ones_f = jnp.ones((8, block), F32)
    wr = wr_ref[...]
    wr_hi = wr.astype(BF16)
    rest = wr - wr_hi.astype(F32)
    wr_mid = rest.astype(BF16)
    wr_lo = (rest - wr_mid.astype(F32)).astype(BF16)
    gate_ref[...] = jnp.zeros_like(gate_ref)
    carry = jnp.zeros((n_experts, 1), F32)
    counts = jnp.zeros((8, n_experts), F32)
    probs = jnp.zeros((8, n_experts), F32)
    for i in range(rows // block):
        cols = pl.ds(i * block, block)
        h = hidden_ref[cols, :]
        z = dot(wr_lo, h, NT) + dot(wr_mid, h, NT) + dot(wr_hi, h, NT)
        e = jnp.exp(z - jnp.max(z, axis=0, keepdims=True))
        p = e / jnp.sum(e, axis=0, keepdims=True)
        prob_ref[:, cols] = p
        id0 = ids_ref[0:1, cols]
        id1 = ids_ref[1:2, cols]
        hit0 = iota_e == id0
        hit1 = iota_e == id1
        p0 = jnp.sum(jnp.where(hit0, p, 0.0), axis=0, keepdims=True)
        p1 = jnp.sum(jnp.where(hit1, p, 0.0), axis=0, keepdims=True)
        den = p0 + p1
        gate_ref[0:1, cols] = p0 / den
        gate_ref[1:2, cols] = p1 / den
        hits = jnp.where(hit0 | hit1, 1.0, 0.0).astype(F32)
        hits_b = hits.astype(BF16)
        rank = dot(hits_b, upper) + carry
        r0 = jnp.sum(jnp.where(hit0, rank, 0.0), axis=0, keepdims=True)
        r1 = jnp.sum(jnp.where(hit1, rank, 0.0), axis=0, keepdims=True)
        pos_ref[0:1, cols] = id0 * per_expert + r0.astype(jnp.int32)
        pos_ref[1:2, cols] = id1 * per_expert + r1.astype(jnp.int32)
        carry = carry + jnp.sum(hits, axis=1, keepdims=True)
        counts = counts + dot(ones, hits_b, NT)
        probs = probs + dot(ones_f, p, NT, HI)
    stat_ref[:, 0:n_experts] = counts
    stat_ref[:, n_experts:2 * n_experts] = probs


def scatter_kernel(steps, pos_ref, gate_ref, hidden_ref, dout_ref, send_ref, first_ref, second_ref, slots_ref):
    step = pl.program_id(0)
    block, d = hidden_ref.shape
    tile = send_ref.shape[0]

    @pl.when(step < steps)
    def _():
        x = hidden_ref[...].astype(F32)
        m = OUT_SCALE * dout_ref[...].astype(F32)
        g = gate_ref[...].T
        x = x.reshape(block // 8, 8, d)
        first_ref[:, :, 0:d] = x
        first_ref[:, :, d:2 * d] = (g[:, 0:1] * m).reshape(block // 8, 8, d)
        second_ref[:, :, 0:d] = x
        second_ref[:, :, d:2 * d] = (g[:, 1:2] * m).reshape(block // 8, 8, d)

        def group(c, _):
            for i in range(GROUP):
                for k, ref in enumerate((first_ref, second_ref)):
                    q = pos_ref[step * (block // GROUP) + c, k, i]
                    slots_ref[pl.ds(q, 1), :] = ref[c * (GROUP // 8) + i // 8, i % 8:i % 8 + 1, :]
            return 0

        lax.fori_loop(0, block // GROUP, group, 0)

    @pl.when(step >= steps)
    def _():
        start = pl.multiple_of((step - steps) * tile, tile)
        send_ref[...] = slots_ref[pl.ds(start, tile), :].astype(BF16)


def expert_kernel(
    ep, etp, capacity, pair, early,
    send_ref, stat_ref, *refs,
):
    weights, refs = refs[:etp], refs[etp:]
    back_ref, refs = refs[0], refs[1:]
    sooner, later, refs = refs[:etp], refs[etp:2 * etp], refs[2 * etp:]
    tab_out_ref, x_ref, w13_ref, w2f_ref, ga13_ref, ga2_ref, ga2t_ref, xm_ref, u_ref, dab_ref, tab_ref = refs[:11]
    stat_send, stat_recv, w13_recv, w2_recv, x_send, x_recv, back_send, back_recv, g_done, g_send, g_recv = refs[11:]
    n_dev = ep * etp
    n_slots = x_ref.shape[0]
    rows = x_ref.shape[2]
    d = w2f_ref.shape[2]
    ff = w2f_ref.shape[1]
    part = ff // etp
    bits = n_dev.bit_length() - 1
    etp_bits = etp.bit_length() - 1
    me_o = lax.axis_index("ep")
    me_t = lax.axis_index("etp")
    me = me_o * etp + me_t

    def where_is(peer):
        return {"ep": peer // etp, "etp": peer % etp}

    def remote(src, dst, send, recv, peer):
        pltpu.make_async_remote_copy(src_ref=src, dst_ref=dst, send_sem=send, recv_sem=recv, device_id=where_is(peer), device_id_type=MESH).start()

    def wait_bytes(ref, sem):
        pltpu.make_async_copy(ref, ref, sem).wait()

    barrier = pltpu.get_barrier_semaphore()

    def hello(i, _):
        pl.semaphore_signal(barrier, inc=1, device_id=where_is((me + i) % n_dev), device_id_type=MESH)
        return 0

    lax.fori_loop(1, n_dev, hello, 0)
    pl.semaphore_wait(barrier, n_dev - 1)

    def order(i):
        return flip(me, (i * 11) % n_dev, bits)

    def send_stats(i, _):
        remote(stat_ref, tab_ref.at[me], stat_send, stat_recv, order(i))
        return 0

    lax.fori_loop(1, n_dev, send_stats, 0)
    tab_ref[me] = stat_ref[...]

    def lanes(offset, t):
        return pl.ds(pl.multiple_of(offset + t * part, part), part)

    for b in range(etp):
        t = flip(me_t, b, etp_bits)
        pltpu.make_async_copy(weights[b].at[0:n_slots], w13_ref.at[:, :, lanes(0, t)], w13_recv).start()
        pltpu.make_async_copy(weights[b].at[n_slots:2 * n_slots], w13_ref.at[:, :, lanes(ff, t)], w13_recv).start()
        pltpu.make_async_copy(weights[b].at[2 * n_slots:3 * n_slots], w2f_ref.at[:, lanes(0, t), :], w2_recv).start()

    def send_slot(j, _):
        pltpu.make_async_copy(send_ref.at[me * n_slots + j], x_ref.at[j, me], x_recv.at[j]).start()

        def tokens(i, _):
            peer = order(i)
            remote(send_ref.at[peer * n_slots + j], x_ref.at[j, me], x_send, x_recv.at[j], peer)
            return 0

        lax.fori_loop(1, n_dev, tokens, 0)
        return 0

    lax.fori_loop(0, n_slots, send_slot, 0)

    wait_bytes(w13_ref, w13_recv)
    wait_bytes(w2f_ref, w2_recv)

    wait_bytes(tab_ref.at[0:n_dev - 1], stat_recv)
    tab_out_ref[...] = tab_ref[...]
    table = tab_ref[:, 0, :]
    shape = table.shape
    below = (lax.broadcasted_iota(jnp.int32, (n_dev, n_dev), 1) < lax.broadcasted_iota(jnp.int32, (n_dev, n_dev), 0)).astype(F32)
    keep = jnp.minimum(table, capacity - dot(below, table, precision=HI))
    src_iota = lax.broadcasted_iota(jnp.int32, shape, 0)
    lane_iota = lax.broadcasted_iota(jnp.int32, shape, 1)
    row_iota = lax.broadcasted_iota(jnp.int32, (rows, 2 * d), 0).astype(F32)
    n_blocks = n_dev // pair
    block_bits = n_blocks.bit_length() - 1

    def give_back(j, src):
        @pl.when(src == me)
        def _():
            pltpu.make_async_copy(x_ref.at[j, me], back_ref.at[me * n_slots + j], back_recv).start()

        @pl.when(src != me)
        def _():
            remote(x_ref.at[j, src], back_ref.at[me * n_slots + j], back_send, back_recv, src)

    def do_slot(j, _):
        wait_bytes(x_ref.at[j], x_recv.at[j])
        ga13_ref[j] = jnp.zeros((d, 2 * ff), F32)
        ga2t_ref[...] = jnp.zeros((d, ff), F32)

        def first_of(b):
            return flip(me // pair, b, block_bits) * pair

        def do_block(b, _):
            first = first_of(b)
            for s in range(pair):
                limit = jnp.sum(jnp.where((src_iota == first + s) & (lane_iota == me * n_slots + j), keep, 0.0), keepdims=True)
                full = x_ref[j, first + s].astype(F32)
                xm_ref[s * rows:(s + 1) * rows, :] = jnp.where(row_iota < limit, full, 0.0).astype(BF16)
            x = xm_ref[:, 0:d]
            c = xm_ref[:, d:2 * d]
            for q in range(ff // part):
                here = slice(q * part, (q + 1) * part)
                there = slice(ff + q * part, ff + (q + 1) * part)
                a = dot(x, w13_ref[j, :, here])
                v = dot(x, w13_ref[j, :, there])
                du = dot(c, w2f_ref[j, here, :], NT)
                sig = jax.nn.sigmoid(a)
                silu = a * sig
                u_ref[:, here] = (silu * v).astype(BF16)
                dab_ref[:, here] = (du * v * sig * (1.0 + a * (1.0 - sig))).astype(BF16)
                dab_ref[:, there] = (du * silu).astype(BF16)
            y = dot(u_ref[...], w2f_ref[j]).astype(BF16)
            dx = dot(dab_ref[...], w13_ref[j], NT).astype(BF16)
            for s in range(pair):
                x_ref[j, first + s, :, 0:d] = y[s * rows:(s + 1) * rows]
                x_ref[j, first + s, :, d:2 * d] = dx[s * rows:(s + 1) * rows]
            ga13_ref[j] += dot(x, dab_ref[...], TN)
            ga2t_ref[...] += dot(c, u_ref[...], TN)

            @pl.when(b > 0)
            def _():
                for s in range(pair):
                    give_back(j, first_of(b - 1) + s)

            return 0

        lax.fori_loop(0, n_blocks, do_block, 0)
        ga2_ref[j] = ga2t_ref[...].T
        for s in range(pair):
            give_back(j, first_of(n_blocks - 1) + s)

        late = n_slots - early

        @pl.when(j < early)
        def _():
            for b in range(etp):
                t = flip(me_t, b, etp_bits)
                for w, ref in enumerate((ga13_ref.at[j, :, lanes(0, t)], ga13_ref.at[j, :, lanes(ff, t)], ga2_ref.at[j, lanes(0, t), :])):
                    if b == 0:
                        pltpu.make_async_copy(ref, sooner[b].at[w * early + j], g_done).start()
                    else:
                        remote(ref, sooner[b].at[w * early + j], g_send, g_recv.at[b - 1], me_o * etp + t)

        @pl.when(j >= early)
        def _():
            for b in range(etp):
                t = flip(me_t, b, etp_bits)
                for w, ref in enumerate((ga13_ref.at[j, :, lanes(0, t)], ga13_ref.at[j, :, lanes(ff, t)], ga2_ref.at[j, lanes(0, t), :])):
                    pltpu.make_async_copy(ref, later[b].at[w * late + j - early], g_done).start()

        return 0

    lax.fori_loop(0, n_slots, do_slot, 0)

    others = (n_dev - 1) * n_slots
    wait_bytes(tab_ref.at[0:n_dev - 1], stat_send)
    wait_bytes(send_ref.at[0:others], x_send)
    wait_bytes(send_ref.at[0:others], back_send)
    wait_bytes(back_ref, back_recv)
    wait_bytes(sooner[0], g_done)
    for b in range(etp):
        wait_bytes(later[b], g_done)
    for b in range(1, etp):
        wait_bytes(sooner[b], g_send)
        wait_bytes(sooner[b], g_recv.at[b - 1])


def combine_kernel(
    n_tokens, chunk,
    pos_ref, back_ref, tab_ref, wr_ref, hidden_ref, dout_ref, ids_ref, gate_ref, prob_ref,
    out_ref, dh_ref, dwr_ref, aux_ref,
    rows_ref, stage_ref, first_ref, second_ref, sem,
):
    step = pl.program_id(0)
    block, d = hidden_ref.shape
    n_experts = wr_ref.shape[0]
    n_chunks = rows_ref.shape[0] // chunk

    totals = jnp.sum(tab_ref[:, 0:1, :], axis=0)
    frac = totals[:, 0:n_experts] / (2 * n_tokens)

    def fetch(i, slot):
        start = pl.multiple_of(i * chunk, chunk)
        return pltpu.make_async_copy(back_ref.at[pl.ds(start, chunk), :], stage_ref.at[slot], sem.at[slot])

    @pl.when(step == 0)
    def _():
        fetch(0, 0).start()

        def body(i, _):
            slot = i % 2

            @pl.when(i + 1 < n_chunks)
            def _():
                fetch(i + 1, 1 - slot).start()

            fetch(i, slot).wait()
            rows_ref[pl.ds(pl.multiple_of(i * chunk, chunk), chunk), :] = stage_ref[slot].astype(F32)
            return 0

        lax.fori_loop(0, n_chunks, body, 0)
        dwr_ref[...] = jnp.zeros_like(dwr_ref)
        mean_prob = totals[:, n_experts:2 * n_experts] / n_tokens
        aux_ref[0, 0] = AUX_COEF * n_experts * jnp.sum(frac * mean_prob)

    def group(c, _):
        for i in range(GROUP):
            for k, ref in enumerate((first_ref, second_ref)):
                q = pos_ref[step * (block // GROUP) + c, k, i]
                ref[c * (GROUP // 8) + i // 8, i % 8:i % 8 + 1, :] = rows_ref[pl.ds(q, 1), :]
        return 0

    lax.fori_loop(0, block // GROUP, group, 0)

    h = hidden_ref[...].astype(F32)
    dy = dout_ref[...].astype(F32)
    m = OUT_SCALE * dy
    y0 = first_ref[:, :, 0:d].reshape(block, d)
    y1 = second_ref[:, :, 0:d].reshape(block, d)
    dx = (first_ref[:, :, d:2 * d] + second_ref[:, :, d:2 * d]).reshape(block, d)
    g = gate_ref[...].T
    out_ref[...] = (h + OUT_SCALE * (g[:, 0:1] * y0 + g[:, 1:2] * y1)).astype(BF16)

    ones = jnp.ones((8, d), F32)
    dg0 = dot(ones, m * y0, NT, HI)[0:1]
    dg1 = dot(ones, m * y1, NT, HI)[0:1]
    p = prob_ref[...]
    iota_e = lax.broadcasted_iota(jnp.int32, p.shape, 0)
    hit0 = iota_e == ids_ref[0:1, :]
    hit1 = iota_e == ids_ref[1:2, :]
    den = jnp.sum(jnp.where(hit0 | hit1, p, 0.0), axis=0, keepdims=True)
    mean = gate_ref[0:1, :] * dg0 + gate_ref[1:2, :] * dg1
    eye = lax.broadcasted_iota(jnp.int32, (n_experts, n_experts), 0) == lax.broadcasted_iota(jnp.int32, (n_experts, n_experts), 1)
    ct = (AUX_COEF * n_experts / n_tokens) * jnp.sum(jnp.where(eye, frac, 0.0), axis=1, keepdims=True)
    dp = jnp.where(hit0, (dg0 - mean) / den, 0.0) + jnp.where(hit1, (dg1 - mean) / den, 0.0) + ct
    dz = p * (dp - jnp.sum(p * dp, axis=0, keepdims=True))
    dwr_ref[...] += dot(dz, h, precision=HI)
    dh_ref[...] = (dy + dx + dot(dz, wr_ref[...], TN, HI)).astype(BF16)


def sum_kernel(ep, etp, part_ref, out_ref, box_ref, mine_ref, all_ref, send1, recv1, send2, recv2):
    n_dev = ep * etp
    across = part_ref.shape[1] // 128
    me = lax.axis_index("ep") * etp + lax.axis_index("etp")

    def where_is(peer):
        return {"ep": peer // etp, "etp": peer % etp}

    def tile(ref, i):
        return ref.at[pl.ds(pl.multiple_of((i // across) * 8, 8), 8), pl.ds(pl.multiple_of((i % across) * 128, 128), 128)]

    def wait_bytes(ref, sem):
        pltpu.make_async_copy(ref, ref, sem).wait()

    barrier = pltpu.get_barrier_semaphore()

    def hello(i, _):
        pl.semaphore_signal(barrier, inc=1, device_id=where_is((me + i) % n_dev), device_id_type=MESH)
        return 0

    lax.fori_loop(1, n_dev, hello, 0)
    pl.semaphore_wait(barrier, n_dev - 1)

    def first(i, _):
        peer = (me + i) % n_dev
        pltpu.make_async_remote_copy(tile(part_ref, peer), box_ref.at[me], send1, recv1, device_id=where_is(peer), device_id_type=MESH).start()
        return 0

    lax.fori_loop(1, n_dev, first, 0)
    pltpu.make_async_copy(tile(part_ref, me), box_ref.at[me], recv1).start()
    wait_bytes(box_ref, recv1)
    mine_ref[...] = jnp.sum(box_ref[...], axis=0)

    def second(i, _):
        peer = (me + i) % n_dev
        pltpu.make_async_remote_copy(mine_ref, all_ref.at[me], send2, recv2, device_id=where_is(peer), device_id_type=MESH).start()
        return 0

    lax.fori_loop(1, n_dev, second, 0)
    all_ref[me] = mine_ref[...]
    wait_bytes(all_ref.at[0:n_dev - 1], recv2)
    for i in range(n_dev):
        out_ref[(i // across) * 8:(i // across) * 8 + 8, (i % across) * 128:(i % across) * 128 + 128] = all_ref[i]
    wait_bytes(box_ref.at[0:n_dev - 1], send1)
    wait_bytes(all_ref.at[0:n_dev - 1], send2)


def assemble_kernel(etp, early, *refs):
    parts, outs = refs[:2 * etp], refs[2 * etp:2 * etp + 3]
    stage_ref, in_sem, out_sem = refs[2 * etp + 3:]
    n_slots = outs[0].shape[0] // etp
    me_t = lax.axis_index("etp")
    every = [(b, w, half) for half in range(2) for b in range(etp) for w in range(3)]

    def copies(i):
        b, w, half = every[i]
        t = flip(me_t, b, etp.bit_length() - 1)
        size = (early, n_slots - early)[half]
        mine = stage_ref.at[i, 0:size]
        load = pltpu.make_async_copy(parts[half * etp + b].at[w * size:(w + 1) * size], mine, in_sem.at[i])
        store = pltpu.make_async_copy(mine, outs[w].at[pl.ds(t * n_slots + half * early, size)], out_sem.at[i])
        return load, store

    for i in range(len(every)):
        copies(i)[0].start()
    for i in range(len(every)):
        load, store = copies(i)
        load.wait()
        store.start()
    for i in range(len(every)):
        copies(i)[1].wait()


def solution(mesh):
    ep_size = mesh.shape["ep"]
    etp_size = mesh.shape["etp"]
    n_dev = ep_size * etp_size
    all_axes = ("ep", "etp")
    tok_spec = P(all_axes, None)
    gate_spec = P("ep", None, "etp")
    down_spec = P("ep", "etp", None)

    def layer(hidden, w_router, expert_ids, d_out, w_gate, w_up, w_down):
        rows, d = hidden.shape
        n_experts = w_router.shape[1]
        n_tokens = rows * n_dev
        capacity = (5 * n_tokens + 2 * n_experts - 1) // (2 * n_experts)
        per_expert = 7 * rows // (2 * n_experts)
        n_slots = n_experts // n_dev
        local_experts, _, part = w_gate.shape
        ff = part * etp_size
        all_slots = n_experts * per_expert
        me_t = lax.axis_index("etp")
        others = [[(t, t ^ b) for t in range(etp_size)] for b in range(etp_size)]

        def parts_for(t):
            return jnp.concatenate([lax.dynamic_slice_in_dim(w, t * n_slots, n_slots) for w in (w_gate, w_up, w_down)])

        weights = [parts_for(me_t)] + [lax.ppermute(parts_for(me_t ^ b), "etp", others[b]) for b in range(1, etp_size)]
        ids_t = expert_ids.T
        wr_t = w_router.T

        vmem = pl.BlockSpec(memory_space=pltpu.VMEM)
        smem = pl.BlockSpec(memory_space=pltpu.SMEM)
        anywhere = pl.BlockSpec(memory_space=pl.ANY)
        big = 60 * 1024 * 1024

        pos, gates, probs, stats = pl.pallas_call(
            functools.partial(route_kernel, per_expert),
            out_shape=(
                jax.ShapeDtypeStruct((2, rows), jnp.int32),
                jax.ShapeDtypeStruct((8, rows), F32),
                jax.ShapeDtypeStruct((n_experts, rows), F32),
                jax.ShapeDtypeStruct((8, 2 * n_experts), F32),
            ),
            in_specs=[vmem] * 3,
            out_specs=(vmem,) * 4,
            cost_estimate=pl.CostEstimate(flops=5_000_000_000, bytes_accessed=4_000_000, transcendentals=0),
            name="route",
        )(hidden, wr_t, ids_t)

        block = min(512, rows)
        steps = rows // block
        pos = pos.reshape(2, rows // GROUP, GROUP).transpose(1, 0, 2)
        tile = n_slots * per_expert
        tiles = all_slots // tile
        send = pl.pallas_call(
            functools.partial(scatter_kernel, steps),
            out_shape=jax.ShapeDtypeStruct((all_slots, 2 * d), BF16),
            grid=(steps + tiles,),
            in_specs=[
                smem,
                pl.BlockSpec((8, block), lambda i: (0, jnp.minimum(i, steps - 1))),
                pl.BlockSpec((block, d), lambda i: (jnp.minimum(i, steps - 1), 0)),
                pl.BlockSpec((block, d), lambda i: (jnp.minimum(i, steps - 1), 0)),
            ],
            out_specs=pl.BlockSpec((tile, 2 * d), lambda i: (jnp.maximum(i - steps, 0), 0)),
            scratch_shapes=[pltpu.VMEM((block // 8, 8, 2 * d), F32)] * 2 + [pltpu.VMEM((all_slots, 2 * d), F32)],
            compiler_params=pltpu.CompilerParams(vmem_limit_bytes=big),
            cost_estimate=pl.CostEstimate(flops=50_000_000_000, bytes_accessed=20_000_000, transcendentals=0),
            name="scatter",
        )(pos, gates, hidden, d_out)
        send = send.reshape(n_experts, per_expert, 2 * d)

        pair = 2
        dma = pltpu.SemaphoreType.DMA
        assert part == d
        early = n_slots // 2
        sooner = jax.ShapeDtypeStruct((3 * early, d, part), F32)
        later = jax.ShapeDtypeStruct((3 * (n_slots - early), d, part), F32)
        back, *rest = pl.pallas_call(
            functools.partial(expert_kernel, ep_size, etp_size, float(capacity), pair, early),
            out_shape=(
                jax.ShapeDtypeStruct((n_experts, per_expert, 2 * d), BF16),
                *(sooner,) * etp_size,
                *(later,) * etp_size,
                jax.ShapeDtypeStruct((n_dev, 8, 2 * n_experts), F32),
            ),
            in_specs=[anywhere, vmem] + [anywhere] * etp_size,
            out_specs=(anywhere,) * (1 + 2 * etp_size) + (vmem,),
            scratch_shapes=[
                pltpu.VMEM((n_slots, n_dev, per_expert, 2 * d), BF16),
                pltpu.VMEM((n_slots, d, 2 * ff), BF16),
                pltpu.VMEM((n_slots, ff, d), BF16),
                pltpu.VMEM((n_slots, d, 2 * ff), F32),
                pltpu.VMEM((n_slots, ff, d), F32),
                pltpu.VMEM((d, ff), F32),
                pltpu.VMEM((pair * per_expert, 2 * d), BF16),
                pltpu.VMEM((pair * per_expert, ff), BF16),
                pltpu.VMEM((pair * per_expert, 2 * ff), BF16),
                pltpu.VMEM((n_dev, 8, 2 * n_experts), F32),
                dma, dma, dma, dma, dma, dma((n_slots,)), dma, dma, dma, dma, dma((etp_size - 1,)),
            ],
            compiler_params=pltpu.CompilerParams(collective_id=0, has_side_effects=True, vmem_limit_bytes=big),
            cost_estimate=pl.CostEstimate(flops=300_000_000_000, bytes_accessed=60_000_000, transcendentals=0),
            name="experts",
        )(send, stats, *weights)
        table = rest[-1]
        sooner, later = rest[:etp_size], rest[etp_size:2 * etp_size]
        grads = [*sooner, later[0]] + [lax.ppermute(later[b], "etp", others[b]) for b in range(1, etp_size)]

        cols = lambda n: pl.BlockSpec((n, block), lambda i: (0, i))
        tok = pl.BlockSpec((block, d), lambda i: (i, 0))
        output, d_hidden, dwr_part, aux_loss = pl.pallas_call(
            functools.partial(combine_kernel, n_tokens, tile),
            out_shape=(
                jax.ShapeDtypeStruct((rows, d), BF16),
                jax.ShapeDtypeStruct((rows, d), BF16),
                jax.ShapeDtypeStruct((n_experts, d), F32),
                jax.ShapeDtypeStruct((1, 1), F32),
            ),
            grid=(steps,),
            in_specs=[smem, anywhere, vmem, vmem, tok, tok, cols(2), cols(8), cols(n_experts)],
            out_specs=(tok, tok, pl.BlockSpec((n_experts, d), lambda i: (0, 0)), smem),
            scratch_shapes=[
                pltpu.VMEM((all_slots, 2 * d), F32),
                pltpu.VMEM((2, tile, 2 * d), BF16),
                pltpu.VMEM((block // 8, 8, 2 * d), F32),
                pltpu.VMEM((block // 8, 8, 2 * d), F32),
                dma((2,)),
            ],
            compiler_params=pltpu.CompilerParams(vmem_limit_bytes=big),
            cost_estimate=pl.CostEstimate(flops=60_000_000_000, bytes_accessed=30_000_000, transcendentals=0),
            name="combine",
        )(pos, back.reshape(all_slots, 2 * d), table, wr_t, hidden, d_out, ids_t, gates, probs)

        dwr = pl.pallas_call(
            functools.partial(sum_kernel, ep_size, etp_size),
            out_shape=jax.ShapeDtypeStruct((n_experts, d), F32),
            in_specs=[vmem],
            out_specs=vmem,
            scratch_shapes=[
                pltpu.VMEM((n_dev, 8, 128), F32), pltpu.VMEM((8, 128), F32), pltpu.VMEM((n_dev, 8, 128), F32),
                dma, dma, dma, dma,
            ],
            compiler_params=pltpu.CompilerParams(collective_id=1, has_side_effects=True),
            cost_estimate=pl.CostEstimate(flops=10_000_000_000, bytes_accessed=100_000, transcendentals=0),
            name="sum_router",
        )(dwr_part)
        g_gate, g_up, g_down = pl.pallas_call(
            functools.partial(assemble_kernel, etp_size, early),
            out_shape=(jax.ShapeDtypeStruct((local_experts, d, part), F32),) * 3,
            in_specs=[anywhere] * (2 * etp_size),
            out_specs=(anywhere,) * 3,
            scratch_shapes=[pltpu.VMEM((6 * etp_size, max(early, n_slots - early), d, part), F32), dma((6 * etp_size,)), dma((6 * etp_size,))],
            compiler_params=pltpu.CompilerParams(vmem_limit_bytes=big),
            name="assemble",
        )(*grads)
        return output, d_hidden, dwr.T, aux_loss.reshape(()), g_gate, g_up, g_down

    return jax.shard_map(layer, mesh=mesh, in_specs=(tok_spec, P(), tok_spec, tok_spec, gate_spec, gate_spec, down_spec), out_specs=(tok_spec, tok_spec, P(), P(), gate_spec, gate_spec, down_spec), check_vma=False)
```

```python
import functools
import jax
import jax.numpy as jnp
from jax import lax
from jax.experimental import pallas as pl
from jax.experimental.pallas import tpu as pltpu
from jax.sharding import PartitionSpec as P

AUX_COEF = 0.01
OUT_SCALE = 2.0
GROUP = 128
F32 = jnp.float32
BF16 = jnp.bfloat16
HI = lax.Precision.HIGHEST
MESH = pl.DeviceIdType.MESH
NT = (((1,), (1,)), ((), ()))
TN = (((0,), (0,)), ((), ()))


def dot(a, b, dims=(((1,), (0,)), ((), ())), precision=None):
    return lax.dot_general(a, b, dims, precision=precision, preferred_element_type=F32)


def flip(index, mask, bits):
    total = 0
    for bit in range(bits):
        total = total + ((index // 2**bit + mask // 2**bit) % 2) * 2**bit
    return total


def route_kernel(per_expert, hidden_ref, wr_ref, ids_ref, pos_ref, gate_ref, prob_ref, stat_ref):
    n_experts = wr_ref.shape[0]
    rows = hidden_ref.shape[0]
    block = min(512, rows)
    iota_e = lax.broadcasted_iota(jnp.int32, (n_experts, block), 0)
    upper = (lax.broadcasted_iota(jnp.int32, (block, block), 0) < lax.broadcasted_iota(jnp.int32, (block, block), 1)).astype(BF16)
    ones = jnp.ones((8, block), BF16)
    ones_f = jnp.ones((8, block), F32)
    wr = wr_ref[...]
    wr_hi = wr.astype(BF16)
    rest = wr - wr_hi.astype(F32)
    wr_mid = rest.astype(BF16)
    wr_lo = (rest - wr_mid.astype(F32)).astype(BF16)
    gate_ref[...] = jnp.zeros_like(gate_ref)
    carry = jnp.zeros((n_experts, 1), F32)
    counts = jnp.zeros((8, n_experts), F32)
    probs = jnp.zeros((8, n_experts), F32)
    for i in range(rows // block):
        cols = pl.ds(i * block, block)
        h = hidden_ref[cols, :]
        z = dot(wr_lo, h, NT) + dot(wr_mid, h, NT) + dot(wr_hi, h, NT)
        e = jnp.exp(z - jnp.max(z, axis=0, keepdims=True))
        p = e / jnp.sum(e, axis=0, keepdims=True)
        prob_ref[:, cols] = p
        id0 = ids_ref[0:1, cols]
        id1 = ids_ref[1:2, cols]
        hit0 = iota_e == id0
        hit1 = iota_e == id1
        p0 = jnp.sum(jnp.where(hit0, p, 0.0), axis=0, keepdims=True)
        p1 = jnp.sum(jnp.where(hit1, p, 0.0), axis=0, keepdims=True)
        den = p0 + p1
        gate_ref[0:1, cols] = p0 / den
        gate_ref[1:2, cols] = p1 / den
        hits = jnp.where(hit0 | hit1, 1.0, 0.0).astype(F32)
        hits_b = hits.astype(BF16)
        rank = dot(hits_b, upper) + carry
        r0 = jnp.sum(jnp.where(hit0, rank, 0.0), axis=0, keepdims=True)
        r1 = jnp.sum(jnp.where(hit1, rank, 0.0), axis=0, keepdims=True)
        pos_ref[0:1, cols] = id0 * per_expert + r0.astype(jnp.int32)
        pos_ref[1:2, cols] = id1 * per_expert + r1.astype(jnp.int32)
        carry = carry + jnp.sum(hits, axis=1, keepdims=True)
        counts = counts + dot(ones, hits_b, NT)
        probs = probs + dot(ones_f, p, NT, HI)
    stat_ref[:, 0:n_experts] = counts
    stat_ref[:, n_experts:2 * n_experts] = probs


def scatter_kernel(steps, pos_ref, gate_ref, hidden_ref, dout_ref, send_ref, first_ref, second_ref, slots_ref):
    step = pl.program_id(0)
    block, d = hidden_ref.shape
    tile = send_ref.shape[0]

    @pl.when(step < steps)
    def _():
        x = hidden_ref[...].astype(F32)
        m = OUT_SCALE * dout_ref[...].astype(F32)
        g = gate_ref[...].T
        x = x.reshape(block // 8, 8, d)
        first_ref[:, :, 0:d] = x
        first_ref[:, :, d:2 * d] = (g[:, 0:1] * m).reshape(block // 8, 8, d)
        second_ref[:, :, 0:d] = x
        second_ref[:, :, d:2 * d] = (g[:, 1:2] * m).reshape(block // 8, 8, d)

        def group(c, _):
            for i in range(GROUP):
                for k, ref in enumerate((first_ref, second_ref)):
                    q = pos_ref[step * (block // GROUP) + c, k, i]
                    slots_ref[pl.ds(q, 1), :] = ref[c * (GROUP // 8) + i // 8, i % 8:i % 8 + 1, :]
            return 0

        lax.fori_loop(0, block // GROUP, group, 0)

    @pl.when(step >= steps)
    def _():
        start = pl.multiple_of((step - steps) * tile, tile)
        send_ref[...] = slots_ref[pl.ds(start, tile), :].astype(BF16)


def expert_kernel(
    ep, etp, capacity, send_ref, stat_ref, *refs,
):
    own, near, twin = refs[0:2], refs[2:4], refs[4:6]
    back_ref = refs[6]
    mine, onward, mine_in, onward_in = refs[7:9], refs[9:11], refs[11:13], refs[13:15]
    tab_out_ref, x_ref, w13_ref, w2f_ref, ga13_ref, ga2_ref, ga2t_ref, xm_ref, u_ref, dab_ref, tab_ref = refs[15:26]
    stat_send, stat_recv, w_recv, relay_send, relay_recv, x_send, x_recv, back_send, back_recv, g_done, g_send, g_recv = refs[26:]
    n_dev = ep * etp
    n_slots, n_src, rows, _ = x_ref.shape
    per = n_slots // 2
    ring = ga13_ref.shape[0]
    d = w2f_ref.shape[2]
    ff = w2f_ref.shape[1]
    part = ff // etp
    bits = n_dev.bit_length() - 1
    src_bits = n_src.bit_length() - 1
    me_o = lax.axis_index("ep")
    me_t = lax.axis_index("etp")
    me = me_o * etp + me_t
    z = me_t // 2
    y = me_t % 2
    t_y = flip(me_t, 1, 2)
    t_z = flip(me_t, 2, 2)
    t_yz = flip(me_t, 3, 2)

    def pick(kind, first, second):
        return first + kind * (second - first)

    def place(kind, w):
        return pick(kind, w * 2 + y, z * 2 + w)

    def remote(src, dst, send, recv, o, t):
        pltpu.make_async_remote_copy(src_ref=src, dst_ref=dst, send_sem=send, recv_sem=recv, device_id={"ep": o, "etp": t}, device_id_type=MESH).start()

    def wait_bytes(ref, sem):
        pltpu.make_async_copy(ref, ref, sem).wait()

    barrier = pltpu.get_barrier_semaphore()

    def hello(i, _):
        peer = (me + i) % n_dev
        pl.semaphore_signal(barrier, inc=1, device_id={"ep": peer // etp, "etp": peer % etp}, device_id_type=MESH)
        return 0

    lax.fori_loop(1, n_dev, hello, 0)
    pl.semaphore_wait(barrier, n_dev - 1)

    def lanes(offset, t):
        return pl.ds(pl.multiple_of(offset + t * part, part), part)

    def places(kind, t):
        group = slice(kind * per, (kind + 1) * per)
        return w13_ref.at[group, :, lanes(0, t)], w13_ref.at[group, :, lanes(ff, t)], w2f_ref.at[group, lanes(0, t), :]

    for kind in range(2):
        beside, across = (t_z, t_y) if kind == 0 else (t_y, t_z)
        for w, dst in enumerate(places(kind, beside)):
            remote(near[kind].at[w * per:(w + 1) * per], dst, relay_send.at[kind], relay_recv.at[kind], me_o, across)
        for n, (ref, t) in enumerate(((own[kind], me_t), (near[kind], beside), (twin[kind], across))):
            for w, dst in enumerate(places(kind, t)):
                pltpu.make_async_copy(ref.at[w * per:(w + 1) * per], dst, w_recv.at[kind * 3 + n]).start()

    def send_stats(i, _):
        peer = flip(me, (i * 11) % n_dev, bits)
        remote(stat_ref, tab_ref.at[me], stat_send, stat_recv, peer // etp, peer % etp)
        return 0

    lax.fori_loop(1, n_dev, send_stats, 0)
    tab_ref[me] = stat_ref[...]

    def expert_of(o, kind, w, k):
        return o * (4 * per) + kind * (2 * per) + w * per + k

    def send_slot(i, _):
        kind, k = i % 2, i // 2
        here = me_o * 2 + pick(kind, z, y)
        pltpu.make_async_copy(send_ref.at[expert_of(me_o, kind, pick(kind, z, y), k)], x_ref.at[i, here], x_recv.at[i]).start()

        def tokens(m, _):
            there = flip(here, (m * 3) % n_src, src_bits)
            o, w = there // 2, there % 2
            remote(send_ref.at[expert_of(o, kind, w, k)], x_ref.at[i, here], x_send, x_recv.at[i], o, place(kind, w))
            return 0

        lax.fori_loop(1, n_src, tokens, 0)
        return 0

    lax.fori_loop(0, n_slots, send_slot, 0)

    wait_bytes(tab_ref.at[0:n_dev - 1], stat_recv)
    tab_out_ref[...] = tab_ref[...]
    table = tab_ref[:, 0, :]
    shape = table.shape
    below = (lax.broadcasted_iota(jnp.int32, (n_dev, n_dev), 1) < lax.broadcasted_iota(jnp.int32, (n_dev, n_dev), 0)).astype(F32)
    keep = jnp.minimum(table, capacity - dot(below, table, precision=HI))
    src_iota = lax.broadcasted_iota(jnp.int32, shape, 0)
    lane_iota = lax.broadcasted_iota(jnp.int32, shape, 1)
    row_iota = lax.broadcasted_iota(jnp.int32, (rows, 2 * d), 0).astype(F32)

    for kind in range(2):
        for n, ref in enumerate((own[kind], near[kind], twin[kind])):
            wait_bytes(ref, w_recv.at[kind * 3 + n])
    for kind in range(2):
        wait_bytes(near[kind], relay_recv.at[kind])

    def do_slot(i, _):
        kind, k = i % 2, i // 2
        at = kind * per + k
        r = i % ring
        v = pick(kind, z, y)
        expert = expert_of(me_o, kind, v, k)

        @pl.when(i >= ring)
        def _():
            wait_bytes(mine[0].at[0:6], g_done.at[r])
            wait_bytes(mine[0].at[0:6], g_send.at[r])

        wait_bytes(x_ref.at[i], x_recv.at[i])
        ga13_ref[r] = jnp.zeros((d, 2 * ff), F32)
        ga2t_ref[...] = jnp.zeros((d, ff), F32)

        def give_back(b):
            o = flip(me_o, b, 2)
            for w in range(2):
                away = (o - me_o) * (o - me_o) + (w - v) * (w - v)

                @pl.when(away == 0)
                def _():
                    pltpu.make_async_copy(x_ref.at[i, o * 2 + w], back_ref.at[expert], back_recv).start()

                @pl.when(away != 0)
                def _():
                    remote(x_ref.at[i, o * 2 + w], back_ref.at[expert], back_send, back_recv, o, place(kind, w))

        def do_block(b, _):
            o = flip(me_o, b, 2)
            for w in range(2):
                limit = jnp.sum(jnp.where((src_iota == o * etp + place(kind, w)) & (lane_iota == expert), keep, 0.0), keepdims=True)
                full = x_ref[i, o * 2 + w].astype(F32)
                xm_ref[w * rows:(w + 1) * rows, :] = jnp.where(row_iota < limit, full, 0.0).astype(BF16)
            x = xm_ref[:, 0:d]
            c = xm_ref[:, d:2 * d]
            for q in range(etp):
                here = slice(q * part, (q + 1) * part)
                there = slice(ff + q * part, ff + (q + 1) * part)
                a = dot(x, w13_ref[at, :, here])
                up = dot(x, w13_ref[at, :, there])
                du = dot(c, w2f_ref[at, here, :], NT)
                sig = jax.nn.sigmoid(a)
                silu = a * sig
                u_ref[:, here] = (silu * up).astype(BF16)
                dab_ref[:, here] = (du * up * sig * (1.0 + a * (1.0 - sig))).astype(BF16)
                dab_ref[:, there] = (du * silu).astype(BF16)
            out = dot(u_ref[...], w2f_ref[at]).astype(BF16)
            dx = dot(dab_ref[...], w13_ref[at], NT).astype(BF16)
            for w in range(2):
                x_ref[i, o * 2 + w, :, 0:d] = out[w * rows:(w + 1) * rows]
                x_ref[i, o * 2 + w, :, d:2 * d] = dx[w * rows:(w + 1) * rows]
            ga13_ref[r] += dot(x, dab_ref[...], TN)
            ga2t_ref[...] += dot(c, u_ref[...], TN)

            @pl.when(b > 0)
            def _():
                give_back(b - 1)

            return 0

        lax.fori_loop(0, ep, do_block, 0)
        ga2_ref[r] = ga2t_ref[...].T
        give_back(ep - 1)

        def parts(t):
            return ga13_ref.at[r, :, lanes(0, t)], ga13_ref.at[r, :, lanes(ff, t)], ga2_ref.at[r, lanes(0, t), :]

        for one in range(2):
            @pl.when(kind == one)
            def _():
                beside, across = (t_z, t_y) if one == 0 else (t_y, t_z)
                for w in range(3):
                    remote(parts(across)[w], mine_in[one].at[w * per + k], g_send.at[r], g_recv.at[one], me_o, across)
                    remote(parts(t_yz)[w], onward_in[one].at[w * per + k], g_send.at[r], g_recv.at[2 + one], me_o, across)
                    pltpu.make_async_copy(parts(me_t)[w], mine[one].at[w * per + k], g_done.at[r]).start()
                    pltpu.make_async_copy(parts(beside)[w], onward[one].at[w * per + k], g_done.at[r]).start()

        return 0

    lax.fori_loop(0, n_slots, do_slot, 0)

    others = (n_src - 1) * n_slots
    wait_bytes(tab_ref.at[0:n_dev - 1], stat_send)
    for kind in range(2):
        wait_bytes(near[kind], relay_send.at[kind])
    wait_bytes(send_ref.at[0:others], x_send)
    wait_bytes(send_ref.at[0:others], back_send)
    for r in range(ring):
        wait_bytes(mine[0].at[0:6], g_done.at[r])
        wait_bytes(mine[0].at[0:6], g_send.at[r])
    wait_bytes(back_ref, back_recv)
    for kind in range(2):
        wait_bytes(mine_in[kind], g_recv.at[kind])
        wait_bytes(onward_in[kind], g_recv.at[2 + kind])


def combine_kernel(
    n_tokens, chunk,
    pos_ref, back_ref, tab_ref, wr_ref, hidden_ref, dout_ref, ids_ref, gate_ref, prob_ref,
    out_ref, dh_ref, dwr_ref, aux_ref,
    rows_ref, stage_ref, first_ref, second_ref, sem,
):
    step = pl.program_id(0)
    block, d = hidden_ref.shape
    n_experts = wr_ref.shape[0]
    n_chunks = rows_ref.shape[0] // chunk

    totals = jnp.sum(tab_ref[:, 0:1, :], axis=0)
    frac = totals[:, 0:n_experts] / (2 * n_tokens)

    def fetch(i, slot):
        start = pl.multiple_of(i * chunk, chunk)
        return pltpu.make_async_copy(back_ref.at[pl.ds(start, chunk), :], stage_ref.at[slot], sem.at[slot])

    @pl.when(step == 0)
    def _():
        fetch(0, 0).start()

        def body(i, _):
            slot = i % 2

            @pl.when(i + 1 < n_chunks)
            def _():
                fetch(i + 1, 1 - slot).start()

            fetch(i, slot).wait()
            rows_ref[pl.ds(pl.multiple_of(i * chunk, chunk), chunk), :] = stage_ref[slot].astype(F32)
            return 0

        lax.fori_loop(0, n_chunks, body, 0)
        dwr_ref[...] = jnp.zeros_like(dwr_ref)
        mean_prob = totals[:, n_experts:2 * n_experts] / n_tokens
        aux_ref[0, 0] = AUX_COEF * n_experts * jnp.sum(frac * mean_prob)

    def group(c, _):
        for i in range(GROUP):
            for k, ref in enumerate((first_ref, second_ref)):
                q = pos_ref[step * (block // GROUP) + c, k, i]
                ref[c * (GROUP // 8) + i // 8, i % 8:i % 8 + 1, :] = rows_ref[pl.ds(q, 1), :]
        return 0

    lax.fori_loop(0, block // GROUP, group, 0)

    h = hidden_ref[...].astype(F32)
    dy = dout_ref[...].astype(F32)
    m = OUT_SCALE * dy
    y0 = first_ref[:, :, 0:d].reshape(block, d)
    y1 = second_ref[:, :, 0:d].reshape(block, d)
    dx = (first_ref[:, :, d:2 * d] + second_ref[:, :, d:2 * d]).reshape(block, d)
    g = gate_ref[...].T
    out_ref[...] = (h + OUT_SCALE * (g[:, 0:1] * y0 + g[:, 1:2] * y1)).astype(BF16)

    ones = jnp.ones((8, d), F32)
    dg0 = dot(ones, m * y0, NT, HI)[0:1]
    dg1 = dot(ones, m * y1, NT, HI)[0:1]
    p = prob_ref[...]
    iota_e = lax.broadcasted_iota(jnp.int32, p.shape, 0)
    hit0 = iota_e == ids_ref[0:1, :]
    hit1 = iota_e == ids_ref[1:2, :]
    den = jnp.sum(jnp.where(hit0 | hit1, p, 0.0), axis=0, keepdims=True)
    mean = gate_ref[0:1, :] * dg0 + gate_ref[1:2, :] * dg1
    eye = lax.broadcasted_iota(jnp.int32, (n_experts, n_experts), 0) == lax.broadcasted_iota(jnp.int32, (n_experts, n_experts), 1)
    ct = (AUX_COEF * n_experts / n_tokens) * jnp.sum(jnp.where(eye, frac, 0.0), axis=1, keepdims=True)
    dp = jnp.where(hit0, (dg0 - mean) / den, 0.0) + jnp.where(hit1, (dg1 - mean) / den, 0.0) + ct
    dz = p * (dp - jnp.sum(p * dp, axis=0, keepdims=True))
    dwr_ref[...] += dot(dz, h, precision=HI)
    dh_ref[...] = (dy + dx + dot(dz, wr_ref[...], TN, HI)).astype(BF16)


def sum_kernel(ep, etp, part_ref, out_ref, box_ref, mine_ref, all_ref, send1, recv1, send2, recv2):
    n_dev = ep * etp
    across = part_ref.shape[1] // 128
    me = lax.axis_index("ep") * etp + lax.axis_index("etp")

    def where_is(peer):
        return {"ep": peer // etp, "etp": peer % etp}

    def tile(ref, i):
        return ref.at[pl.ds(pl.multiple_of((i // across) * 8, 8), 8), pl.ds(pl.multiple_of((i % across) * 128, 128), 128)]

    def wait_bytes(ref, sem):
        pltpu.make_async_copy(ref, ref, sem).wait()

    barrier = pltpu.get_barrier_semaphore()

    def hello(i, _):
        pl.semaphore_signal(barrier, inc=1, device_id=where_is((me + i) % n_dev), device_id_type=MESH)
        return 0

    lax.fori_loop(1, n_dev, hello, 0)
    pl.semaphore_wait(barrier, n_dev - 1)

    def first(i, _):
        peer = (me + i) % n_dev
        pltpu.make_async_remote_copy(tile(part_ref, peer), box_ref.at[me], send1, recv1, device_id=where_is(peer), device_id_type=MESH).start()
        return 0

    lax.fori_loop(1, n_dev, first, 0)
    pltpu.make_async_copy(tile(part_ref, me), box_ref.at[me], recv1).start()
    wait_bytes(box_ref, recv1)
    mine_ref[...] = jnp.sum(box_ref[...], axis=0)

    def second(i, _):
        peer = (me + i) % n_dev
        pltpu.make_async_remote_copy(mine_ref, all_ref.at[me], send2, recv2, device_id=where_is(peer), device_id_type=MESH).start()
        return 0

    lax.fori_loop(1, n_dev, second, 0)
    all_ref[me] = mine_ref[...]
    wait_bytes(all_ref.at[0:n_dev - 1], recv2)
    for i in range(n_dev):
        out_ref[(i // across) * 8:(i // across) * 8 + 8, (i % across) * 128:(i % across) * 128 + 128] = all_ref[i]
    wait_bytes(box_ref.at[0:n_dev - 1], send1)
    wait_bytes(all_ref.at[0:n_dev - 1], send2)


def own_sum_kernel(per, *refs):
    mine, mine_in, outs = refs[0:2], refs[2:4], refs[4:7]
    a_ref, b_ref, a_sem, b_sem, out_sem = refs[7:]
    me_t = lax.axis_index("etp")
    starts = (me_t // 2) * per, 2 * per + (me_t % 2) * per
    every = [(kind, w) for kind in range(2) for w in range(3)]

    def copies(i):
        kind, w = every[i]
        here = slice(w * per, (w + 1) * per)
        return (
            pltpu.make_async_copy(mine[kind].at[here], a_ref.at[i], a_sem.at[i]),
            pltpu.make_async_copy(mine_in[kind].at[here], b_ref.at[i], b_sem.at[i]),
            pltpu.make_async_copy(a_ref.at[i], outs[w].at[pl.ds(starts[kind], per)], out_sem.at[i]),
        )

    for i in range(len(every)):
        for copy in copies(i)[0:2]:
            copy.start()
    for i in range(len(every)):
        load, other, store = copies(i)
        load.wait()
        other.wait()
        a_ref[i] += b_ref[i]
        store.start()
    for i in range(len(every)):
        pltpu.make_async_copy(a_ref.at[i], outs[every[i][1]].at[pl.ds(starts[every[i][0]], per)], out_sem.at[i]).wait()


def assemble_kernel(per, *refs):
    came, outs = refs[0:2], refs[5:8]
    stage_ref, in_sem, out_sem = refs[8:]
    me_t = lax.axis_index("etp")
    starts = (1 - me_t // 2) * per, 2 * per + (1 - me_t % 2) * per
    every = [(kind, w) for kind in range(2) for w in range(3)]

    def load(i):
        kind, w = every[i]
        return pltpu.make_async_copy(came[kind].at[w * per:(w + 1) * per], stage_ref.at[i], in_sem.at[i])

    def store(i):
        kind, w = every[i]
        return pltpu.make_async_copy(stage_ref.at[i], outs[w].at[pl.ds(starts[kind], per)], out_sem.at[i])

    for i in range(len(every)):
        load(i).start()
    for i in range(len(every)):
        load(i).wait()
        store(i).start()
    for i in range(len(every)):
        store(i).wait()


def solution(mesh):
    ep_size = mesh.shape["ep"]
    etp_size = mesh.shape["etp"]
    n_dev = ep_size * etp_size
    all_axes = ("ep", "etp")
    tok_spec = P(all_axes, None)
    gate_spec = P("ep", None, "etp")
    down_spec = P("ep", "etp", None)

    def layer(hidden, w_router, expert_ids, d_out, w_gate, w_up, w_down):
        rows, d = hidden.shape
        n_experts = w_router.shape[1]
        n_tokens = rows * n_dev
        capacity = (5 * n_tokens + 2 * n_experts - 1) // (2 * n_experts)
        per_expert = 7 * rows // (2 * n_experts)
        n_slots = n_experts // n_dev
        local_experts, _, part = w_gate.shape
        ff = part * etp_size
        all_slots = n_experts * per_expert
        assert etp_size == 4 and ep_size == 4
        me_t = lax.axis_index("etp")
        z, y = me_t // 2, me_t % 2
        per = n_experts // ep_size // 4
        swap_y = [(t, t ^ 1) for t in range(4)]
        swap_z = [(t, t ^ 2) for t in range(4)]

        def parts_at(start):
            return jnp.concatenate([lax.dynamic_slice_in_dim(w, start, per) for w in (w_gate, w_up, w_down)])

        near = [lax.ppermute(parts_at((1 - z) * per), "etp", swap_z), lax.ppermute(parts_at((3 - y) * per), "etp", swap_y)]
        own = [parts_at(z * per), parts_at((2 + y) * per)]
        twin = [lax.ppermute(own[0], "etp", swap_y), lax.ppermute(own[1], "etp", swap_z)]
        ids_t = expert_ids.T
        wr_t = w_router.T

        vmem = pl.BlockSpec(memory_space=pltpu.VMEM)
        smem = pl.BlockSpec(memory_space=pltpu.SMEM)
        anywhere = pl.BlockSpec(memory_space=pl.ANY)
        big = 60 * 1024 * 1024

        pos, gates, probs, stats = pl.pallas_call(
            functools.partial(route_kernel, per_expert),
            out_shape=(
                jax.ShapeDtypeStruct((2, rows), jnp.int32),
                jax.ShapeDtypeStruct((8, rows), F32),
                jax.ShapeDtypeStruct((n_experts, rows), F32),
                jax.ShapeDtypeStruct((8, 2 * n_experts), F32),
            ),
            in_specs=[vmem] * 3,
            out_specs=(vmem,) * 4,
            cost_estimate=pl.CostEstimate(flops=5_000_000_000, bytes_accessed=4_000_000, transcendentals=0),
            name="route",
        )(hidden, wr_t, ids_t)

        block = min(512, rows)
        steps = rows // block
        pos = pos.reshape(2, rows // GROUP, GROUP).transpose(1, 0, 2)
        tile = n_slots * per_expert
        tiles = all_slots // tile
        send = pl.pallas_call(
            functools.partial(scatter_kernel, steps),
            out_shape=jax.ShapeDtypeStruct((all_slots, 2 * d), BF16),
            grid=(steps + tiles,),
            in_specs=[
                smem,
                pl.BlockSpec((8, block), lambda i: (0, jnp.minimum(i, steps - 1))),
                pl.BlockSpec((block, d), lambda i: (jnp.minimum(i, steps - 1), 0)),
                pl.BlockSpec((block, d), lambda i: (jnp.minimum(i, steps - 1), 0)),
            ],
            out_specs=pl.BlockSpec((tile, 2 * d), lambda i: (jnp.maximum(i - steps, 0), 0)),
            scratch_shapes=[pltpu.VMEM((block // 8, 8, 2 * d), F32)] * 2 + [pltpu.VMEM((all_slots, 2 * d), F32)],
            compiler_params=pltpu.CompilerParams(vmem_limit_bytes=big),
            cost_estimate=pl.CostEstimate(flops=50_000_000_000, bytes_accessed=20_000_000, transcendentals=0),
            name="scatter",
        )(pos, gates, hidden, d_out)
        send = send.reshape(n_experts, per_expert, 2 * d)

        dma = pltpu.SemaphoreType.DMA
        assert part == d
        slots = 2 * per
        sources = n_dev // 2
        ring = 4
        grad = jax.ShapeDtypeStruct((3 * per, d, part), F32)
        back, *rest = pl.pallas_call(
            functools.partial(expert_kernel, ep_size, etp_size, float(capacity)),
            out_shape=(
                jax.ShapeDtypeStruct((n_experts, per_expert, 2 * d), BF16),
                *(grad,) * 8,
                jax.ShapeDtypeStruct((n_dev, 8, 2 * n_experts), F32),
            ),
            in_specs=[anywhere, vmem] + [anywhere] * 6,
            out_specs=(anywhere,) * 9 + (vmem,),
            scratch_shapes=[
                pltpu.VMEM((slots, sources, per_expert, 2 * d), BF16),
                pltpu.VMEM((slots, d, 2 * ff), BF16),
                pltpu.VMEM((slots, ff, d), BF16),
                pltpu.VMEM((ring, d, 2 * ff), F32),
                pltpu.VMEM((ring, ff, d), F32),
                pltpu.VMEM((d, ff), F32),
                pltpu.VMEM((2 * per_expert, 2 * d), BF16),
                pltpu.VMEM((2 * per_expert, ff), BF16),
                pltpu.VMEM((2 * per_expert, 2 * ff), BF16),
                pltpu.VMEM((n_dev, 8, 2 * n_experts), F32),
                dma, dma, dma((6,)), dma((2,)), dma((2,)), dma, dma((slots,)), dma, dma, dma((ring,)), dma((ring,)), dma((4,)),
            ],
            cost_estimate=pl.CostEstimate(flops=300_000_000_000, bytes_accessed=60_000_000, transcendentals=0),
            compiler_params=pltpu.CompilerParams(collective_id=0, has_side_effects=True, vmem_limit_bytes=big),
            name="experts",
        )(send, stats, *own, *near, *twin)
        table = rest[-1]
        mine, onward, mine_in, onward_in = rest[0:2], rest[2:4], rest[4:6], rest[6:8]
        came = [
            lax.ppermute(onward[0] + onward_in[0], "etp", swap_z),
            lax.ppermute(onward[1] + onward_in[1], "etp", swap_y),
        ]

        cols = lambda n: pl.BlockSpec((n, block), lambda i: (0, i))
        tok = pl.BlockSpec((block, d), lambda i: (i, 0))
        output, d_hidden, dwr_part, aux_loss = pl.pallas_call(
            functools.partial(combine_kernel, n_tokens, tile),
            out_shape=(
                jax.ShapeDtypeStruct((rows, d), BF16),
                jax.ShapeDtypeStruct((rows, d), BF16),
                jax.ShapeDtypeStruct((n_experts, d), F32),
                jax.ShapeDtypeStruct((1, 1), F32),
            ),
            grid=(steps,),
            in_specs=[smem, anywhere, vmem, vmem, tok, tok, cols(2), cols(8), cols(n_experts)],
            out_specs=(tok, tok, pl.BlockSpec((n_experts, d), lambda i: (0, 0)), smem),
            scratch_shapes=[
                pltpu.VMEM((all_slots, 2 * d), F32),
                pltpu.VMEM((2, tile, 2 * d), BF16),
                pltpu.VMEM((block // 8, 8, 2 * d), F32),
                pltpu.VMEM((block // 8, 8, 2 * d), F32),
                dma((2,)),
            ],
            compiler_params=pltpu.CompilerParams(vmem_limit_bytes=big),
            cost_estimate=pl.CostEstimate(flops=60_000_000_000, bytes_accessed=30_000_000, transcendentals=0),
            name="combine",
        )(pos, back.reshape(all_slots, 2 * d), table, wr_t, hidden, d_out, ids_t, gates, probs)

        dwr = pl.pallas_call(
            functools.partial(sum_kernel, ep_size, etp_size),
            out_shape=jax.ShapeDtypeStruct((n_experts, d), F32),
            in_specs=[vmem],
            out_specs=vmem,
            scratch_shapes=[
                pltpu.VMEM((n_dev, 8, 128), F32), pltpu.VMEM((8, 128), F32), pltpu.VMEM((n_dev, 8, 128), F32),
                dma, dma, dma, dma,
            ],
            compiler_params=pltpu.CompilerParams(collective_id=1, has_side_effects=True),
            cost_estimate=pl.CostEstimate(flops=10_000_000_000, bytes_accessed=100_000, transcendentals=0),
            name="sum_router",
        )(dwr_part)
        results = (jax.ShapeDtypeStruct((local_experts, d, part), F32),) * 3
        half = pl.pallas_call(
            functools.partial(own_sum_kernel, per),
            out_shape=results,
            in_specs=[anywhere] * 4,
            out_specs=(anywhere,) * 3,
            scratch_shapes=[pltpu.VMEM((6, per, d, part), F32)] * 2 + [dma((6,))] * 3,
            cost_estimate=pl.CostEstimate(flops=8_000_000_000, bytes_accessed=20_000_000, transcendentals=0),
            compiler_params=pltpu.CompilerParams(vmem_limit_bytes=big),
            name="own_sum",
        )(*mine, *mine_in)
        g_gate, g_up, g_down = pl.pallas_call(
            functools.partial(assemble_kernel, per),
            out_shape=results,
            in_specs=[anywhere] * 5,
            out_specs=(anywhere,) * 3,
            input_output_aliases={2: 0, 3: 1, 4: 2},
            scratch_shapes=[pltpu.VMEM((6, per, d, part), F32), dma((6,)), dma((6,))],
            compiler_params=pltpu.CompilerParams(vmem_limit_bytes=big),
            name="assemble",
        )(*came, *half)
        return output, d_hidden, dwr.T, aux_loss.reshape(()), g_gate, g_up, g_down

    return jax.shard_map(layer, mesh=mesh, in_specs=(tok_spec, P(), tok_spec, tok_spec, gate_spec, gate_spec, down_spec), out_specs=(tok_spec, tok_spec, P(), P(), gate_spec, gate_spec, down_spec), check_vma=False)
```

```python
import functools
import jax
import jax.numpy as jnp
from jax import lax
from jax.experimental import pallas as pl
from jax.experimental.pallas import tpu as pltpu
from jax.sharding import PartitionSpec as P

AUX_COEF = 0.01
OUT_SCALE = 2.0
GROUP = 128
F32 = jnp.float32
BF16 = jnp.bfloat16
HI = lax.Precision.HIGHEST
MESH = pl.DeviceIdType.MESH
NT = (((1,), (1,)), ((), ()))
TN = (((0,), (0,)), ((), ()))


def dot(a, b, dims=(((1,), (0,)), ((), ())), precision=None):
    return lax.dot_general(a, b, dims, precision=precision, preferred_element_type=F32)


def flip(index, mask, bits):
    total = 0
    for bit in range(bits):
        total = total + ((index // 2**bit + mask // 2**bit) % 2) * 2**bit
    return total


def route_kernel(per_expert, hidden_ref, wr_ref, ids_ref, pos_ref, gate_ref, prob_ref, stat_ref):
    n_experts = wr_ref.shape[0]
    rows = hidden_ref.shape[0]
    block = min(512, rows)
    iota_e = lax.broadcasted_iota(jnp.int32, (n_experts, block), 0)
    upper = (lax.broadcasted_iota(jnp.int32, (block, block), 0) < lax.broadcasted_iota(jnp.int32, (block, block), 1)).astype(BF16)
    ones = jnp.ones((8, block), BF16)
    ones_f = jnp.ones((8, block), F32)
    wr = wr_ref[...]
    wr_hi = wr.astype(BF16)
    rest = wr - wr_hi.astype(F32)
    wr_mid = rest.astype(BF16)
    wr_lo = (rest - wr_mid.astype(F32)).astype(BF16)
    gate_ref[...] = jnp.zeros_like(gate_ref)
    carry = jnp.zeros((n_experts, 1), F32)
    counts = jnp.zeros((8, n_experts), F32)
    probs = jnp.zeros((8, n_experts), F32)
    for i in range(rows // block):
        cols = pl.ds(i * block, block)
        h = hidden_ref[cols, :]
        z = dot(wr_lo, h, NT) + dot(wr_mid, h, NT) + dot(wr_hi, h, NT)
        e = jnp.exp(z - jnp.max(z, axis=0, keepdims=True))
        p = e / jnp.sum(e, axis=0, keepdims=True)
        prob_ref[:, cols] = p
        id0 = ids_ref[0:1, cols]
        id1 = ids_ref[1:2, cols]
        hit0 = iota_e == id0
        hit1 = iota_e == id1
        p0 = jnp.sum(jnp.where(hit0, p, 0.0), axis=0, keepdims=True)
        p1 = jnp.sum(jnp.where(hit1, p, 0.0), axis=0, keepdims=True)
        den = p0 + p1
        gate_ref[0:1, cols] = p0 / den
        gate_ref[1:2, cols] = p1 / den
        hits = jnp.where(hit0 | hit1, 1.0, 0.0).astype(F32)
        hits_b = hits.astype(BF16)
        rank = dot(hits_b, upper) + carry
        r0 = jnp.sum(jnp.where(hit0, rank, 0.0), axis=0, keepdims=True)
        r1 = jnp.sum(jnp.where(hit1, rank, 0.0), axis=0, keepdims=True)
        pos_ref[0:1, cols] = id0 * per_expert + r0.astype(jnp.int32)
        pos_ref[1:2, cols] = id1 * per_expert + r1.astype(jnp.int32)
        carry = carry + jnp.sum(hits, axis=1, keepdims=True)
        counts = counts + dot(ones, hits_b, NT)
        probs = probs + dot(ones_f, p, NT, HI)
    stat_ref[:, 0:n_experts] = counts
    stat_ref[:, n_experts:2 * n_experts] = probs


def scatter_kernel(steps, pos_ref, gate_ref, hidden_ref, dout_ref, send_ref, first_ref, second_ref, slots_ref):
    step = pl.program_id(0)
    block, d = hidden_ref.shape
    tile = send_ref.shape[0]

    @pl.when(step < steps)
    def _():
        x = hidden_ref[...].astype(F32)
        m = OUT_SCALE * dout_ref[...].astype(F32)
        g = gate_ref[...].T
        x = x.reshape(block // 8, 8, d)
        first_ref[:, :, 0:d] = x
        first_ref[:, :, d:2 * d] = (g[:, 0:1] * m).reshape(block // 8, 8, d)
        second_ref[:, :, 0:d] = x
        second_ref[:, :, d:2 * d] = (g[:, 1:2] * m).reshape(block // 8, 8, d)

        def group(c, _):
            for i in range(GROUP):
                for k, ref in enumerate((first_ref, second_ref)):
                    q = pos_ref[step * (block // GROUP) + c, k, i]
                    slots_ref[pl.ds(q, 1), :] = ref[c * (GROUP // 8) + i // 8, i % 8:i % 8 + 1, :]
            return 0

        lax.fori_loop(0, block // GROUP, group, 0)

    @pl.when(step >= steps)
    def _():
        start = pl.multiple_of((step - steps) * tile, tile)
        send_ref[...] = slots_ref[pl.ds(start, tile), :].astype(BF16)


def expert_kernel(
    ep, etp, capacity, send_ref, stat_ref, *refs,
):
    own, near, twin, refs = refs[0:3], (refs[3:6], refs[6:9]), (refs[9:12], refs[12:15]), refs[15:]
    back_ref = refs[0]
    mine, mine_in, onward, onward_in = refs[1:3], refs[3:5], (refs[5:8], refs[8:11]), (refs[11:14], refs[14:17])
    tab_out_ref, x_ref, w13_ref, w2f_ref, ga13_ref, ga2_ref, ga2t_ref, xm_ref, u_ref, dab_ref, tab_ref = refs[17:28]
    stat_send, stat_recv, w_recv, relay_send, relay_recv, x_send, x_recv, back_send, back_recv, g_done, g_send, g_recv = refs[28:]
    n_dev = ep * etp
    n_slots, n_src, rows, _ = x_ref.shape
    per = n_slots // 2
    ring = ga13_ref.shape[0]
    d = w2f_ref.shape[2]
    ff = w2f_ref.shape[1]
    part = ff // etp
    bits = n_dev.bit_length() - 1
    src_bits = n_src.bit_length() - 1
    me_o = lax.axis_index("ep")
    me_t = lax.axis_index("etp")
    me = me_o * etp + me_t
    z = me_t // 2
    y = me_t % 2
    t_y = flip(me_t, 1, 2)
    t_z = flip(me_t, 2, 2)
    t_yz = flip(me_t, 3, 2)

    def pick(kind, first, second):
        return first + kind * (second - first)

    def place(kind, w):
        return pick(kind, w * 2 + y, z * 2 + w)

    def remote(src, dst, send, recv, o, t):
        pltpu.make_async_remote_copy(src_ref=src, dst_ref=dst, send_sem=send, recv_sem=recv, device_id={"ep": o, "etp": t}, device_id_type=MESH).start()

    def wait_bytes(ref, sem):
        pltpu.make_async_copy(ref, ref, sem).wait()

    barrier = pltpu.get_barrier_semaphore()

    def hello(i, _):
        peer = (me + i) % n_dev
        pl.semaphore_signal(barrier, inc=1, device_id={"ep": peer // etp, "etp": peer % etp}, device_id_type=MESH)
        return 0

    lax.fori_loop(1, n_dev, hello, 0)
    pl.semaphore_wait(barrier, n_dev - 1)

    def lanes(offset, t):
        return pl.ds(pl.multiple_of(offset + t * part, part), part)

    def places(kind, t):
        group = slice(kind * per, (kind + 1) * per)
        return w13_ref.at[group, :, lanes(0, t)], w13_ref.at[group, :, lanes(ff, t)], w2f_ref.at[group, lanes(0, t), :]

    relays, loads = [], []
    for kind in range(2):
        beside, across = (t_z, t_y) if kind == 0 else (t_y, t_z)
        start = pick(kind, z * per, (2 + y) * per)
        for w in range(3):
            n = kind * 3 + w
            relays.append(pltpu.make_async_remote_copy(
                src_ref=near[kind][w], dst_ref=places(kind, beside)[w], send_sem=relay_send.at[n], recv_sem=relay_recv.at[n],
                device_id={"ep": me_o, "etp": across}, device_id_type=MESH,
            ))
            for ref, t in ((own[w].at[pl.ds(start, per)], me_t), (near[kind][w], beside), (twin[kind][w], across)):
                loads.append(pltpu.make_async_copy(ref, places(kind, t)[w], w_recv.at[len(loads)]))
    for copy in relays + loads:
        copy.start()

    def send_stats(i, _):
        peer = flip(me, (i * 11) % n_dev, bits)
        remote(stat_ref, tab_ref.at[me], stat_send, stat_recv, peer // etp, peer % etp)
        return 0

    lax.fori_loop(1, n_dev, send_stats, 0)
    tab_ref[me] = stat_ref[...]

    def expert_of(o, kind, w, k):
        return o * (4 * per) + kind * (2 * per) + w * per + k

    def send_slot(i, _):
        kind, k = i % 2, i // 2
        here = me_o * 2 + pick(kind, z, y)
        pltpu.make_async_copy(send_ref.at[expert_of(me_o, kind, pick(kind, z, y), k)], x_ref.at[i, here], x_recv.at[i]).start()

        def tokens(m, _):
            there = flip(here, (m * 3) % n_src, src_bits)
            o, w = there // 2, there % 2
            remote(send_ref.at[expert_of(o, kind, w, k)], x_ref.at[i, here], x_send, x_recv.at[i], o, place(kind, w))
            return 0

        lax.fori_loop(1, n_src, tokens, 0)
        return 0

    lax.fori_loop(0, n_slots, send_slot, 0)

    wait_bytes(tab_ref.at[0:n_dev - 1], stat_recv)
    tab_out_ref[...] = tab_ref[...]
    table = tab_ref[:, 0, :]
    shape = table.shape
    below = (lax.broadcasted_iota(jnp.int32, (n_dev, n_dev), 1) < lax.broadcasted_iota(jnp.int32, (n_dev, n_dev), 0)).astype(F32)
    keep = jnp.minimum(table, capacity - dot(below, table, precision=HI))
    src_iota = lax.broadcasted_iota(jnp.int32, shape, 0)
    lane_iota = lax.broadcasted_iota(jnp.int32, shape, 1)
    row_iota = lax.broadcasted_iota(jnp.int32, (rows, 2 * d), 0).astype(F32)

    for copy in loads:
        copy.wait()
    for copy in relays:
        copy.wait_recv()

    def do_slot(i, _):
        kind, k = i % 2, i // 2
        at = kind * per + k
        r = i % ring
        v = pick(kind, z, y)
        expert = expert_of(me_o, kind, v, k)

        @pl.when(i >= ring)
        def _():
            wait_bytes(mine[0].at[0:6], g_done.at[r])
            wait_bytes(mine[0].at[0:6], g_send.at[r])

        wait_bytes(x_ref.at[i], x_recv.at[i])
        ga13_ref[r] = jnp.zeros((d, 2 * ff), F32)
        ga2t_ref[...] = jnp.zeros((d, ff), F32)

        def give_back(b):
            o = flip(me_o, b, 2)
            for w in range(2):
                away = (o - me_o) * (o - me_o) + (w - v) * (w - v)

                @pl.when(away == 0)
                def _():
                    pltpu.make_async_copy(x_ref.at[i, o * 2 + w], back_ref.at[expert], back_recv).start()

                @pl.when(away != 0)
                def _():
                    remote(x_ref.at[i, o * 2 + w], back_ref.at[expert], back_send, back_recv, o, place(kind, w))

        def do_block(b, _):
            o = flip(me_o, b, 2)
            for w in range(2):
                limit = jnp.sum(jnp.where((src_iota == o * etp + place(kind, w)) & (lane_iota == expert), keep, 0.0), keepdims=True)
                full = x_ref[i, o * 2 + w].astype(F32)
                xm_ref[w * rows:(w + 1) * rows, :] = jnp.where(row_iota < limit, full, 0.0).astype(BF16)
            x = xm_ref[:, 0:d]
            c = xm_ref[:, d:2 * d]
            for q in range(etp):
                here = slice(q * part, (q + 1) * part)
                there = slice(ff + q * part, ff + (q + 1) * part)
                a = dot(x, w13_ref[at, :, here])
                up = dot(x, w13_ref[at, :, there])
                du = dot(c, w2f_ref[at, here, :], NT)
                sig = jax.nn.sigmoid(a)
                silu = a * sig
                u_ref[:, here] = (silu * up).astype(BF16)
                dab_ref[:, here] = (du * up * sig * (1.0 + a * (1.0 - sig))).astype(BF16)
                dab_ref[:, there] = (du * silu).astype(BF16)
            out = dot(u_ref[...], w2f_ref[at]).astype(BF16)
            dx = dot(dab_ref[...], w13_ref[at], NT).astype(BF16)
            for w in range(2):
                x_ref[i, o * 2 + w, :, 0:d] = out[w * rows:(w + 1) * rows]
                x_ref[i, o * 2 + w, :, d:2 * d] = dx[w * rows:(w + 1) * rows]
            ga13_ref[r] += dot(x, dab_ref[...], TN)
            ga2t_ref[...] += dot(c, u_ref[...], TN)

            @pl.when(b > 0)
            def _():
                give_back(b - 1)

            return 0

        lax.fori_loop(0, ep, do_block, 0)
        ga2_ref[r] = ga2t_ref[...].T
        give_back(ep - 1)

        def parts(t):
            return ga13_ref.at[r, :, lanes(0, t)], ga13_ref.at[r, :, lanes(ff, t)], ga2_ref.at[r, lanes(0, t), :]

        for one in range(2):
            @pl.when(kind == one)
            def _():
                beside, across = (t_z, t_y) if one == 0 else (t_y, t_z)
                for w in range(3):
                    remote(parts(across)[w], mine_in[one].at[w * per + k], g_send.at[r], g_recv.at[one], me_o, across)
                    remote(parts(t_yz)[w], onward_in[one][w].at[k], g_send.at[r], g_recv.at[2 + one * 3 + w], me_o, across)
                    pltpu.make_async_copy(parts(me_t)[w], mine[one].at[w * per + k], g_done.at[r]).start()
                    pltpu.make_async_copy(parts(beside)[w], onward[one][w].at[k], g_done.at[r]).start()

        return 0

    lax.fori_loop(0, n_slots, do_slot, 0)

    others = (n_src - 1) * n_slots
    wait_bytes(tab_ref.at[0:n_dev - 1], stat_send)
    for copy in relays:
        copy.wait_send()
    wait_bytes(send_ref.at[0:others], x_send)
    wait_bytes(send_ref.at[0:others], back_send)
    for r in range(ring):
        wait_bytes(mine[0].at[0:6], g_done.at[r])
        wait_bytes(mine[0].at[0:6], g_send.at[r])
    wait_bytes(back_ref, back_recv)
    for kind in range(2):
        wait_bytes(mine_in[kind], g_recv.at[kind])
        for w in range(3):
            wait_bytes(onward_in[kind][w], g_recv.at[2 + kind * 3 + w])


def combine_kernel(
    n_tokens, chunk,
    pos_ref, back_ref, tab_ref, wr_ref, hidden_ref, dout_ref, ids_ref, gate_ref, prob_ref,
    out_ref, dh_ref, dwr_ref, aux_ref,
    rows_ref, stage_ref, first_ref, second_ref, sem,
):
    step = pl.program_id(0)
    block, d = hidden_ref.shape
    n_experts = wr_ref.shape[0]
    n_chunks = rows_ref.shape[0] // chunk

    totals = jnp.sum(tab_ref[:, 0:1, :], axis=0)
    frac = totals[:, 0:n_experts] / (2 * n_tokens)

    def fetch(i, slot):
        start = pl.multiple_of(i * chunk, chunk)
        return pltpu.make_async_copy(back_ref.at[pl.ds(start, chunk), :], stage_ref.at[slot], sem.at[slot])

    @pl.when(step == 0)
    def _():
        fetch(0, 0).start()

        def body(i, _):
            slot = i % 2

            @pl.when(i + 1 < n_chunks)
            def _():
                fetch(i + 1, 1 - slot).start()

            fetch(i, slot).wait()
            rows_ref[pl.ds(pl.multiple_of(i * chunk, chunk), chunk), :] = stage_ref[slot].astype(F32)
            return 0

        lax.fori_loop(0, n_chunks, body, 0)
        dwr_ref[...] = jnp.zeros_like(dwr_ref)
        mean_prob = totals[:, n_experts:2 * n_experts] / n_tokens
        aux_ref[0, 0] = AUX_COEF * n_experts * jnp.sum(frac * mean_prob)

    def group(c, _):
        for i in range(GROUP):
            for k, ref in enumerate((first_ref, second_ref)):
                q = pos_ref[step * (block // GROUP) + c, k, i]
                ref[c * (GROUP // 8) + i // 8, i % 8:i % 8 + 1, :] = rows_ref[pl.ds(q, 1), :]
        return 0

    lax.fori_loop(0, block // GROUP, group, 0)

    h = hidden_ref[...].astype(F32)
    dy = dout_ref[...].astype(F32)
    m = OUT_SCALE * dy
    y0 = first_ref[:, :, 0:d].reshape(block, d)
    y1 = second_ref[:, :, 0:d].reshape(block, d)
    dx = (first_ref[:, :, d:2 * d] + second_ref[:, :, d:2 * d]).reshape(block, d)
    g = gate_ref[...].T
    out_ref[...] = (h + OUT_SCALE * (g[:, 0:1] * y0 + g[:, 1:2] * y1)).astype(BF16)

    ones = jnp.ones((8, d), F32)
    dg0 = dot(ones, m * y0, NT, HI)[0:1]
    dg1 = dot(ones, m * y1, NT, HI)[0:1]
    p = prob_ref[...]
    iota_e = lax.broadcasted_iota(jnp.int32, p.shape, 0)
    hit0 = iota_e == ids_ref[0:1, :]
    hit1 = iota_e == ids_ref[1:2, :]
    den = jnp.sum(jnp.where(hit0 | hit1, p, 0.0), axis=0, keepdims=True)
    mean = gate_ref[0:1, :] * dg0 + gate_ref[1:2, :] * dg1
    eye = lax.broadcasted_iota(jnp.int32, (n_experts, n_experts), 0) == lax.broadcasted_iota(jnp.int32, (n_experts, n_experts), 1)
    ct = (AUX_COEF * n_experts / n_tokens) * jnp.sum(jnp.where(eye, frac, 0.0), axis=1, keepdims=True)
    dp = jnp.where(hit0, (dg0 - mean) / den, 0.0) + jnp.where(hit1, (dg1 - mean) / den, 0.0) + ct
    dz = p * (dp - jnp.sum(p * dp, axis=0, keepdims=True))
    dwr_ref[...] += dot(dz, h, precision=HI)
    dh_ref[...] = (dy + dx + dot(dz, wr_ref[...], TN, HI)).astype(BF16)


def sum_kernel(ep, etp, part_ref, out_ref, box_ref, mine_ref, all_ref, send1, recv1, send2, recv2):
    n_dev = ep * etp
    across = part_ref.shape[1] // 128
    me = lax.axis_index("ep") * etp + lax.axis_index("etp")

    def where_is(peer):
        return {"ep": peer // etp, "etp": peer % etp}

    def tile(ref, i):
        return ref.at[pl.ds(pl.multiple_of((i // across) * 8, 8), 8), pl.ds(pl.multiple_of((i % across) * 128, 128), 128)]

    def wait_bytes(ref, sem):
        pltpu.make_async_copy(ref, ref, sem).wait()

    barrier = pltpu.get_barrier_semaphore()

    def hello(i, _):
        pl.semaphore_signal(barrier, inc=1, device_id=where_is((me + i) % n_dev), device_id_type=MESH)
        return 0

    lax.fori_loop(1, n_dev, hello, 0)
    pl.semaphore_wait(barrier, n_dev - 1)

    def first(i, _):
        peer = (me + i) % n_dev
        pltpu.make_async_remote_copy(tile(part_ref, peer), box_ref.at[me], send1, recv1, device_id=where_is(peer), device_id_type=MESH).start()
        return 0

    lax.fori_loop(1, n_dev, first, 0)
    pltpu.make_async_copy(tile(part_ref, me), box_ref.at[me], recv1).start()
    wait_bytes(box_ref, recv1)
    mine_ref[...] = jnp.sum(box_ref[...], axis=0)

    def second(i, _):
        peer = (me + i) % n_dev
        pltpu.make_async_remote_copy(mine_ref, all_ref.at[me], send2, recv2, device_id=where_is(peer), device_id_type=MESH).start()
        return 0

    lax.fori_loop(1, n_dev, second, 0)
    all_ref[me] = mine_ref[...]
    wait_bytes(all_ref.at[0:n_dev - 1], recv2)
    for i in range(n_dev):
        out_ref[(i // across) * 8:(i // across) * 8 + 8, (i % across) * 128:(i % across) * 128 + 128] = all_ref[i]
    wait_bytes(box_ref.at[0:n_dev - 1], send1)
    wait_bytes(all_ref.at[0:n_dev - 1], send2)


def own_sum_kernel(per, *refs):
    mine, mine_in, outs = refs[0:2], refs[2:4], refs[4:7]
    a_ref, b_ref, a_sem, b_sem, out_sem = refs[7:]
    me_t = lax.axis_index("etp")
    starts = (me_t // 2) * per, 2 * per + (me_t % 2) * per
    every = [(kind, w) for kind in range(2) for w in range(3)]

    def copies(i):
        kind, w = every[i]
        here = slice(w * per, (w + 1) * per)
        return (
            pltpu.make_async_copy(mine[kind].at[here], a_ref.at[i], a_sem.at[i]),
            pltpu.make_async_copy(mine_in[kind].at[here], b_ref.at[i], b_sem.at[i]),
            pltpu.make_async_copy(a_ref.at[i], outs[w].at[pl.ds(starts[kind], per)], out_sem.at[i]),
        )

    for i in range(len(every)):
        for copy in copies(i)[0:2]:
            copy.start()
    for i in range(len(every)):
        load, other, store = copies(i)
        load.wait()
        other.wait()
        a_ref[i] += b_ref[i]
        store.start()
    for i in range(len(every)):
        pltpu.make_async_copy(a_ref.at[i], outs[every[i][1]].at[pl.ds(starts[every[i][0]], per)], out_sem.at[i]).wait()


def assemble_kernel(per, *refs):
    came, outs = refs[0:6], refs[9:12]
    stage_ref, in_sem, out_sem = refs[12:]
    me_t = lax.axis_index("etp")
    starts = (1 - me_t // 2) * per, 2 * per + (1 - me_t % 2) * per
    loads = [pltpu.make_async_copy(came[i], stage_ref.at[i], in_sem.at[i]) for i in range(6)]
    stores = [pltpu.make_async_copy(stage_ref.at[i], outs[i // 2].at[pl.ds(starts[i % 2], per)], out_sem.at[i]) for i in range(6)]
    for load in loads:
        load.start()
    for load, store in zip(loads, stores):
        load.wait()
        store.start()
    for store in stores:
        store.wait()


def solution(mesh):
    ep_size = mesh.shape["ep"]
    etp_size = mesh.shape["etp"]
    n_dev = ep_size * etp_size
    all_axes = ("ep", "etp")
    tok_spec = P(all_axes, None)
    gate_spec = P("ep", None, "etp")
    down_spec = P("ep", "etp", None)

    def layer(hidden, w_router, expert_ids, d_out, w_gate, w_up, w_down):
        rows, d = hidden.shape
        n_experts = w_router.shape[1]
        n_tokens = rows * n_dev
        capacity = (5 * n_tokens + 2 * n_experts - 1) // (2 * n_experts)
        per_expert = 7 * rows // (2 * n_experts)
        n_slots = n_experts // n_dev
        local_experts, _, part = w_gate.shape
        ff = part * etp_size
        all_slots = n_experts * per_expert
        assert etp_size == 4 and ep_size == 4
        me_t = lax.axis_index("etp")
        z, y = me_t // 2, me_t % 2
        per = n_experts // ep_size // 4
        swap_y = [(t, t ^ 1) for t in range(4)]
        swap_z = [(t, t ^ 2) for t in range(4)]

        weights = w_gate, w_up, w_down

        def parts_at(w, start):
            return lax.dynamic_slice_in_dim(w, start, per)

        near, twin = ([], []), ([], [])
        for w in weights:
            near[0].append(lax.ppermute(parts_at(w, (1 - z) * per), "etp", swap_z))
            near[1].append(lax.ppermute(parts_at(w, (3 - y) * per), "etp", swap_y))
            twin[0].append(lax.ppermute(parts_at(w, z * per), "etp", swap_y))
            twin[1].append(lax.ppermute(parts_at(w, (2 + y) * per), "etp", swap_z))
        ids_t = expert_ids.T
        wr_t = w_router.T

        vmem = pl.BlockSpec(memory_space=pltpu.VMEM)
        smem = pl.BlockSpec(memory_space=pltpu.SMEM)
        anywhere = pl.BlockSpec(memory_space=pl.ANY)
        big = 60 * 1024 * 1024

        pos, gates, probs, stats = pl.pallas_call(
            functools.partial(route_kernel, per_expert),
            out_shape=(
                jax.ShapeDtypeStruct((2, rows), jnp.int32),
                jax.ShapeDtypeStruct((8, rows), F32),
                jax.ShapeDtypeStruct((n_experts, rows), F32),
                jax.ShapeDtypeStruct((8, 2 * n_experts), F32),
            ),
            in_specs=[vmem] * 3,
            out_specs=(vmem,) * 4,
            cost_estimate=pl.CostEstimate(flops=5_000_000_000, bytes_accessed=4_000_000, transcendentals=0),
            name="route",
        )(hidden, wr_t, ids_t)

        block = min(512, rows)
        steps = rows // block
        pos = pos.reshape(2, rows // GROUP, GROUP).transpose(1, 0, 2)
        tile = n_slots * per_expert
        tiles = all_slots // tile
        send = pl.pallas_call(
            functools.partial(scatter_kernel, steps),
            out_shape=jax.ShapeDtypeStruct((all_slots, 2 * d), BF16),
            grid=(steps + tiles,),
            in_specs=[
                smem,
                pl.BlockSpec((8, block), lambda i: (0, jnp.minimum(i, steps - 1))),
                pl.BlockSpec((block, d), lambda i: (jnp.minimum(i, steps - 1), 0)),
                pl.BlockSpec((block, d), lambda i: (jnp.minimum(i, steps - 1), 0)),
            ],
            out_specs=pl.BlockSpec((tile, 2 * d), lambda i: (jnp.maximum(i - steps, 0), 0)),
            scratch_shapes=[pltpu.VMEM((block // 8, 8, 2 * d), F32)] * 2 + [pltpu.VMEM((all_slots, 2 * d), F32)],
            compiler_params=pltpu.CompilerParams(vmem_limit_bytes=big),
            cost_estimate=pl.CostEstimate(flops=50_000_000_000, bytes_accessed=20_000_000, transcendentals=0),
            name="scatter",
        )(pos, gates, hidden, d_out)
        send = send.reshape(n_experts, per_expert, 2 * d)

        dma = pltpu.SemaphoreType.DMA
        assert part == d
        slots = 2 * per
        sources = n_dev // 2
        ring = 4
        grad = jax.ShapeDtypeStruct((3 * per, d, part), F32)
        back, *rest = pl.pallas_call(
            functools.partial(expert_kernel, ep_size, etp_size, float(capacity)),
            out_shape=(
                jax.ShapeDtypeStruct((n_experts, per_expert, 2 * d), BF16),
                *(grad,) * 4,
                *(jax.ShapeDtypeStruct((per, d, part), F32),) * 12,
                jax.ShapeDtypeStruct((n_dev, 8, 2 * n_experts), F32),
            ),
            in_specs=[anywhere, vmem] + [anywhere] * 15,
            out_specs=(anywhere,) * 17 + (vmem,),
            scratch_shapes=[
                pltpu.VMEM((slots, sources, per_expert, 2 * d), BF16),
                pltpu.VMEM((slots, d, 2 * ff), BF16),
                pltpu.VMEM((slots, ff, d), BF16),
                pltpu.VMEM((ring, d, 2 * ff), F32),
                pltpu.VMEM((ring, ff, d), F32),
                pltpu.VMEM((d, ff), F32),
                pltpu.VMEM((2 * per_expert, 2 * d), BF16),
                pltpu.VMEM((2 * per_expert, ff), BF16),
                pltpu.VMEM((2 * per_expert, 2 * ff), BF16),
                pltpu.VMEM((n_dev, 8, 2 * n_experts), F32),
                dma, dma, dma((18,)), dma((6,)), dma((6,)), dma, dma((slots,)), dma, dma, dma((ring,)), dma((ring,)), dma((8,)),
            ],
            cost_estimate=pl.CostEstimate(flops=300_000_000_000, bytes_accessed=60_000_000, transcendentals=0),
            compiler_params=pltpu.CompilerParams(collective_id=0, has_side_effects=True, vmem_limit_bytes=big),
            name="experts",
        )(send, stats, *weights, *near[0], *near[1], *twin[0], *twin[1])
        table = rest[-1]
        mine, mine_in, onward, onward_in = rest[0:2], rest[2:4], rest[4:10], rest[10:16]
        came = []
        for w in range(3):
            for kind, swap in ((0, swap_z), (1, swap_y)):
                came.append(lax.ppermute(onward[kind * 3 + w] + onward_in[kind * 3 + w], "etp", swap))

        cols = lambda n: pl.BlockSpec((n, block), lambda i: (0, i))
        tok = pl.BlockSpec((block, d), lambda i: (i, 0))
        output, d_hidden, dwr_part, aux_loss = pl.pallas_call(
            functools.partial(combine_kernel, n_tokens, tile),
            out_shape=(
                jax.ShapeDtypeStruct((rows, d), BF16),
                jax.ShapeDtypeStruct((rows, d), BF16),
                jax.ShapeDtypeStruct((n_experts, d), F32),
                jax.ShapeDtypeStruct((1, 1), F32),
            ),
            grid=(steps,),
            in_specs=[smem, anywhere, vmem, vmem, tok, tok, cols(2), cols(8), cols(n_experts)],
            out_specs=(tok, tok, pl.BlockSpec((n_experts, d), lambda i: (0, 0)), smem),
            scratch_shapes=[
                pltpu.VMEM((all_slots, 2 * d), F32),
                pltpu.VMEM((2, tile, 2 * d), BF16),
                pltpu.VMEM((block // 8, 8, 2 * d), F32),
                pltpu.VMEM((block // 8, 8, 2 * d), F32),
                dma((2,)),
            ],
            compiler_params=pltpu.CompilerParams(vmem_limit_bytes=big),
            cost_estimate=pl.CostEstimate(flops=60_000_000_000, bytes_accessed=30_000_000, transcendentals=0),
            name="combine",
        )(pos, back.reshape(all_slots, 2 * d), table, wr_t, hidden, d_out, ids_t, gates, probs)

        results = (jax.ShapeDtypeStruct((local_experts, d, part), F32),) * 3
        half = pl.pallas_call(
            functools.partial(own_sum_kernel, per),
            out_shape=results,
            in_specs=[anywhere] * 4,
            out_specs=(anywhere,) * 3,
            scratch_shapes=[pltpu.VMEM((6, per, d, part), F32)] * 2 + [dma((6,))] * 3,
            cost_estimate=pl.CostEstimate(flops=8_000_000_000, bytes_accessed=20_000_000, transcendentals=0),
            compiler_params=pltpu.CompilerParams(vmem_limit_bytes=big),
            name="own_sum",
        )(*mine, *mine_in)
        dwr_part, *half = lax.optimization_barrier((dwr_part, *half))
        dwr = pl.pallas_call(
            functools.partial(sum_kernel, ep_size, etp_size),
            out_shape=jax.ShapeDtypeStruct((n_experts, d), F32),
            in_specs=[vmem],
            out_specs=vmem,
            scratch_shapes=[
                pltpu.VMEM((n_dev, 8, 128), F32), pltpu.VMEM((8, 128), F32), pltpu.VMEM((n_dev, 8, 128), F32),
                dma, dma, dma, dma,
            ],
            compiler_params=pltpu.CompilerParams(collective_id=1, has_side_effects=True),
            cost_estimate=pl.CostEstimate(flops=10_000_000_000, bytes_accessed=100_000, transcendentals=0),
            name="sum_router",
        )(dwr_part)
        g_gate, g_up, g_down = pl.pallas_call(
            functools.partial(assemble_kernel, per),
            out_shape=results,
            in_specs=[anywhere] * 9,
            out_specs=(anywhere,) * 3,
            input_output_aliases={6: 0, 7: 1, 8: 2},
            scratch_shapes=[pltpu.VMEM((6, per, d, part), F32), dma((6,)), dma((6,))],
            compiler_params=pltpu.CompilerParams(vmem_limit_bytes=big),
            name="assemble",
        )(*came, *half)
        return output, d_hidden, dwr.T, aux_loss.reshape(()), g_gate, g_up, g_down

    return jax.shard_map(layer, mesh=mesh, in_specs=(tok_spec, P(), tok_spec, tok_spec, gate_spec, gate_spec, down_spec), out_specs=(tok_spec, tok_spec, P(), P(), gate_spec, gate_spec, down_spec), check_vma=False)
```

```python
import functools
import jax
import jax.numpy as jnp
from jax import lax
from jax.experimental import pallas as pl
from jax.experimental.pallas import tpu as pltpu
from jax.sharding import PartitionSpec as P

AUX_COEF = 0.01
OUT_SCALE = 2.0
GROUP = 128
F32 = jnp.float32
BF16 = jnp.bfloat16
HI = lax.Precision.HIGHEST
MESH = pl.DeviceIdType.MESH
NT = (((1,), (1,)), ((), ()))
TN = (((0,), (0,)), ((), ()))


def dot(a, b, dims=(((1,), (0,)), ((), ())), precision=None):
    return lax.dot_general(a, b, dims, precision=precision, preferred_element_type=F32)


def flip(index, mask, bits):
    total = 0
    for bit in range(bits):
        total = total + ((index // 2**bit + mask // 2**bit) % 2) * 2**bit
    return total


def route_kernel(per_expert, hidden_ref, wr_ref, ids_ref, pos_ref, gate_ref, prob_ref, stat_ref):
    n_experts = wr_ref.shape[0]
    rows = hidden_ref.shape[0]
    block = min(512, rows)
    iota_e = lax.broadcasted_iota(jnp.int32, (n_experts, block), 0)
    upper = (lax.broadcasted_iota(jnp.int32, (block, block), 0) < lax.broadcasted_iota(jnp.int32, (block, block), 1)).astype(BF16)
    ones = jnp.ones((8, block), BF16)
    ones_f = jnp.ones((8, block), F32)
    wr = wr_ref[...]
    wr_hi = wr.astype(BF16)
    rest = wr - wr_hi.astype(F32)
    wr_mid = rest.astype(BF16)
    wr_lo = (rest - wr_mid.astype(F32)).astype(BF16)
    gate_ref[...] = jnp.zeros_like(gate_ref)
    carry = jnp.zeros((n_experts, 1), F32)
    counts = jnp.zeros((8, n_experts), F32)
    probs = jnp.zeros((8, n_experts), F32)
    for i in range(rows // block):
        cols = pl.ds(i * block, block)
        h = hidden_ref[cols, :]
        z = dot(wr_lo, h, NT) + dot(wr_mid, h, NT) + dot(wr_hi, h, NT)
        e = jnp.exp(z - jnp.max(z, axis=0, keepdims=True))
        p = e / jnp.sum(e, axis=0, keepdims=True)
        prob_ref[:, cols] = p
        id0 = ids_ref[0:1, cols]
        id1 = ids_ref[1:2, cols]
        hit0 = iota_e == id0
        hit1 = iota_e == id1
        p0 = jnp.sum(jnp.where(hit0, p, 0.0), axis=0, keepdims=True)
        p1 = jnp.sum(jnp.where(hit1, p, 0.0), axis=0, keepdims=True)
        den = p0 + p1
        gate_ref[0:1, cols] = p0 / den
        gate_ref[1:2, cols] = p1 / den
        hits = jnp.where(hit0 | hit1, 1.0, 0.0).astype(F32)
        hits_b = hits.astype(BF16)
        rank = dot(hits_b, upper) + carry
        r0 = jnp.sum(jnp.where(hit0, rank, 0.0), axis=0, keepdims=True)
        r1 = jnp.sum(jnp.where(hit1, rank, 0.0), axis=0, keepdims=True)
        pos_ref[0:1, cols] = id0 * per_expert + r0.astype(jnp.int32)
        pos_ref[1:2, cols] = id1 * per_expert + r1.astype(jnp.int32)
        carry = carry + jnp.sum(hits, axis=1, keepdims=True)
        counts = counts + dot(ones, hits_b, NT)
        probs = probs + dot(ones_f, p, NT, HI)
    stat_ref[:, 0:n_experts] = counts
    stat_ref[:, n_experts:2 * n_experts] = probs


def scatter_kernel(steps, pos_ref, gate_ref, hidden_ref, dout_ref, send_ref, first_ref, second_ref, slots_ref):
    step = pl.program_id(0)
    block, d = hidden_ref.shape
    tile = send_ref.shape[0]

    @pl.when(step < steps)
    def _():
        x = hidden_ref[...].astype(F32)
        m = OUT_SCALE * dout_ref[...].astype(F32)
        g = gate_ref[...].T
        x = x.reshape(block // 8, 8, d)
        first_ref[:, :, 0:d] = x
        first_ref[:, :, d:2 * d] = (g[:, 0:1] * m).reshape(block // 8, 8, d)
        second_ref[:, :, 0:d] = x
        second_ref[:, :, d:2 * d] = (g[:, 1:2] * m).reshape(block // 8, 8, d)

        def group(c, _):
            for i in range(GROUP):
                for k, ref in enumerate((first_ref, second_ref)):
                    q = pos_ref[step * (block // GROUP) + c, k, i]
                    slots_ref[pl.ds(q, 1), :] = ref[c * (GROUP // 8) + i // 8, i % 8:i % 8 + 1, :]
            return 0

        lax.fori_loop(0, block // GROUP, group, 0)

    @pl.when(step >= steps)
    def _():
        start = pl.multiple_of((step - steps) * tile, tile)
        send_ref[...] = slots_ref[pl.ds(start, tile), :].astype(BF16)


def expert_kernel(
    ep, etp, capacity, send_ref, stat_ref, *refs,
):
    own, near, twin, refs = refs[0:3], (refs[3:6], refs[6:9]), (refs[9:12], refs[12:15]), refs[15:]
    back_ref = refs[0]
    mine, onward = (refs[1:4], refs[4:7]), (refs[7:10], refs[10:13])
    tab_out_ref, x_ref, w13_ref, w2f_ref, ga13_ref, ga2_ref, ga2t_ref, twin_ref, xm_ref, u_ref, dab_ref, tab_ref = refs[13:25]
    stat_send, stat_recv, w_recv, relay_send, relay_recv, x_send, x_recv, back_send, back_recv, g_done, g_send, g_recv = refs[25:]
    n_dev = ep * etp
    n_slots, n_src, rows, _ = x_ref.shape
    per = n_slots // 2
    ring = ga13_ref.shape[0]
    d = w2f_ref.shape[2]
    ff = w2f_ref.shape[1]
    part = ff // etp
    bits = n_dev.bit_length() - 1
    src_bits = n_src.bit_length() - 1
    me_o = lax.axis_index("ep")
    me_t = lax.axis_index("etp")
    me = me_o * etp + me_t
    z = me_t // 2
    y = me_t % 2
    t_y = flip(me_t, 1, 2)
    t_z = flip(me_t, 2, 2)
    t_yz = flip(me_t, 3, 2)

    def pick(kind, first, second):
        return first + kind * (second - first)

    def place(kind, w):
        return pick(kind, w * 2 + y, z * 2 + w)

    def remote(src, dst, send, recv, o, t):
        pltpu.make_async_remote_copy(src_ref=src, dst_ref=dst, send_sem=send, recv_sem=recv, device_id={"ep": o, "etp": t}, device_id_type=MESH).start()

    def wait_bytes(ref, sem):
        pltpu.make_async_copy(ref, ref, sem).wait()

    barrier = pltpu.get_barrier_semaphore()

    def hello(i, _):
        peer = (me + i) % n_dev
        pl.semaphore_signal(barrier, inc=1, device_id={"ep": peer // etp, "etp": peer % etp}, device_id_type=MESH)
        return 0

    lax.fori_loop(1, n_dev, hello, 0)
    pl.semaphore_wait(barrier, n_dev - 1)

    def lanes(offset, t):
        return pl.ds(pl.multiple_of(offset + t * part, part), part)

    def places(kind, t):
        group = slice(kind * per, (kind + 1) * per)
        return w13_ref.at[group, :, lanes(0, t)], w13_ref.at[group, :, lanes(ff, t)], w2f_ref.at[group, lanes(0, t), :]

    relays, loads = [], []
    for kind in range(2):
        beside, across = (t_z, t_y) if kind == 0 else (t_y, t_z)
        start = pick(kind, z * per, (2 + y) * per)
        for w in range(3):
            n = kind * 3 + w
            relays.append(pltpu.make_async_remote_copy(
                src_ref=near[kind][w], dst_ref=places(kind, beside)[w], send_sem=relay_send.at[n], recv_sem=relay_recv.at[n],
                device_id={"ep": me_o, "etp": across}, device_id_type=MESH,
            ))
            for ref, t in ((own[w].at[pl.ds(start, per)], me_t), (near[kind][w], beside), (twin[kind][w], across)):
                loads.append(pltpu.make_async_copy(ref, places(kind, t)[w], w_recv.at[len(loads)]))
    for copy in relays + loads:
        copy.start()

    def send_stats(i, _):
        peer = flip(me, (i * 11) % n_dev, bits)
        remote(stat_ref, tab_ref.at[me], stat_send, stat_recv, peer // etp, peer % etp)
        return 0

    lax.fori_loop(1, n_dev, send_stats, 0)
    tab_ref[me] = stat_ref[...]

    def expert_of(o, kind, w, k):
        return o * (4 * per) + kind * (2 * per) + w * per + k

    def send_slot(i, _):
        kind, k = i % 2, i // 2
        here = me_o * 2 + pick(kind, z, y)
        pltpu.make_async_copy(send_ref.at[expert_of(me_o, kind, pick(kind, z, y), k)], x_ref.at[i, here], x_recv.at[i]).start()

        def tokens(m, _):
            there = flip(here, (m * 3) % n_src, src_bits)
            o, w = there // 2, there % 2
            remote(send_ref.at[expert_of(o, kind, w, k)], x_ref.at[i, here], x_send, x_recv.at[i], o, place(kind, w))
            return 0

        lax.fori_loop(1, n_src, tokens, 0)
        return 0

    lax.fori_loop(0, n_slots, send_slot, 0)

    wait_bytes(tab_ref.at[0:n_dev - 1], stat_recv)
    tab_out_ref[...] = tab_ref[...]
    table = tab_ref[:, 0, :]
    shape = table.shape
    below = (lax.broadcasted_iota(jnp.int32, (n_dev, n_dev), 1) < lax.broadcasted_iota(jnp.int32, (n_dev, n_dev), 0)).astype(F32)
    keep = jnp.minimum(table, capacity - dot(below, table, precision=HI))
    src_iota = lax.broadcasted_iota(jnp.int32, shape, 0)
    lane_iota = lax.broadcasted_iota(jnp.int32, shape, 1)
    row_iota = lax.broadcasted_iota(jnp.int32, (rows, 2 * d), 0).astype(F32)

    for copy in loads:
        copy.wait()
    for copy in relays:
        copy.wait_recv()

    def do_slot(i, _):
        kind, k = i % 2, i // 2
        at = kind * per + k
        r = i % ring
        v = pick(kind, z, y)
        expert = expert_of(me_o, kind, v, k)

        @pl.when(i >= ring)
        def _():
            wait_bytes(twin_ref.at[0], g_send.at[r])

        wait_bytes(x_ref.at[i], x_recv.at[i])
        ga13_ref[r] = jnp.zeros((d, 2 * ff), F32)
        ga2t_ref[...] = jnp.zeros((d, ff), F32)

        def give_back(b):
            o = flip(me_o, b, 2)
            for w in range(2):
                away = (o - me_o) * (o - me_o) + (w - v) * (w - v)

                @pl.when(away == 0)
                def _():
                    pltpu.make_async_copy(x_ref.at[i, o * 2 + w], back_ref.at[expert], back_recv).start()

                @pl.when(away != 0)
                def _():
                    remote(x_ref.at[i, o * 2 + w], back_ref.at[expert], back_send, back_recv, o, place(kind, w))

        def do_block(b, _):
            o = flip(me_o, b, 2)
            for w in range(2):
                limit = jnp.sum(jnp.where((src_iota == o * etp + place(kind, w)) & (lane_iota == expert), keep, 0.0), keepdims=True)
                full = x_ref[i, o * 2 + w].astype(F32)
                xm_ref[w * rows:(w + 1) * rows, :] = jnp.where(row_iota < limit, full, 0.0).astype(BF16)
            x = xm_ref[:, 0:d]
            c = xm_ref[:, d:2 * d]
            for q in range(etp):
                here = slice(q * part, (q + 1) * part)
                there = slice(ff + q * part, ff + (q + 1) * part)
                a = dot(x, w13_ref[at, :, here])
                up = dot(x, w13_ref[at, :, there])
                du = dot(c, w2f_ref[at, here, :], NT)
                sig = jax.nn.sigmoid(a)
                silu = a * sig
                u_ref[:, here] = (silu * up).astype(BF16)
                dab_ref[:, here] = (du * up * sig * (1.0 + a * (1.0 - sig))).astype(BF16)
                dab_ref[:, there] = (du * silu).astype(BF16)
            out = dot(u_ref[...], w2f_ref[at]).astype(BF16)
            dx = dot(dab_ref[...], w13_ref[at], NT).astype(BF16)
            for w in range(2):
                x_ref[i, o * 2 + w, :, 0:d] = out[w * rows:(w + 1) * rows]
                x_ref[i, o * 2 + w, :, d:2 * d] = dx[w * rows:(w + 1) * rows]
            ga13_ref[r] += dot(x, dab_ref[...], TN)
            ga2t_ref[...] += dot(c, u_ref[...], TN)

            @pl.when(b > 0)
            def _():
                give_back(b - 1)

            return 0

        lax.fori_loop(0, ep, do_block, 0)
        ga2_ref[r] = ga2t_ref[...].T
        give_back(ep - 1)

        for one in range(2):
            @pl.when(kind == one)
            def _():
                across = t_y if one == 0 else t_z
                for w in range(3):
                    remote(parts(r, across)[w], twin_ref.at[i, w], g_send.at[r], g_recv.at[i], me_o, across)
                    remote(parts(r, t_yz)[w], twin_ref.at[i, 3 + w], g_send.at[r], g_recv.at[i], me_o, across)

        @pl.when(i >= 2)
        def _():
            add_twin(i - 2)

        return 0

    def parts(r, t):
        return ga13_ref.at[r, :, lanes(0, t)], ga13_ref.at[r, :, lanes(ff, t)], ga2_ref.at[r, lanes(0, t), :]

    def add_twin(i):
        kind, k = i % 2, i // 2
        r = i % ring
        wait_bytes(twin_ref.at[i], g_recv.at[i])
        for one in range(2):
            @pl.when(kind == one)
            def _():
                beside = t_z if one == 0 else t_y
                for w in range(3):
                    twin_ref[i, w] += parts(r, me_t)[w][...]
                    twin_ref[i, 3 + w] += parts(r, beside)[w][...]
                for w in range(3):
                    pltpu.make_async_copy(twin_ref.at[i, w], mine[one][w].at[k], g_done).start()
                    pltpu.make_async_copy(twin_ref.at[i, 3 + w], onward[one][w].at[k], g_done).start()

    lax.fori_loop(0, n_slots, do_slot, 0)
    lax.fori_loop(n_slots - 2, n_slots, lambda i, _: (add_twin(i), 0)[1], 0)

    others = (n_src - 1) * n_slots
    wait_bytes(tab_ref.at[0:n_dev - 1], stat_send)
    for copy in relays:
        copy.wait_send()
    wait_bytes(send_ref.at[0:others], x_send)
    wait_bytes(send_ref.at[0:others], back_send)
    for r in range(ring):
        wait_bytes(twin_ref.at[0], g_send.at[r])
    wait_bytes(back_ref, back_recv)
    wait_bytes(twin_ref, g_done)


def combine_kernel(
    n_tokens, chunk,
    pos_ref, back_ref, tab_ref, wr_ref, hidden_ref, dout_ref, ids_ref, gate_ref, prob_ref,
    out_ref, dh_ref, dwr_ref, aux_ref,
    rows_ref, stage_ref, first_ref, second_ref, sem,
):
    step = pl.program_id(0)
    block, d = hidden_ref.shape
    n_experts = wr_ref.shape[0]
    n_chunks = rows_ref.shape[0] // chunk

    totals = jnp.sum(tab_ref[:, 0:1, :], axis=0)
    frac = totals[:, 0:n_experts] / (2 * n_tokens)

    def fetch(i, slot):
        start = pl.multiple_of(i * chunk, chunk)
        return pltpu.make_async_copy(back_ref.at[pl.ds(start, chunk), :], stage_ref.at[slot], sem.at[slot])

    @pl.when(step == 0)
    def _():
        fetch(0, 0).start()

        def body(i, _):
            slot = i % 2

            @pl.when(i + 1 < n_chunks)
            def _():
                fetch(i + 1, 1 - slot).start()

            fetch(i, slot).wait()
            rows_ref[pl.ds(pl.multiple_of(i * chunk, chunk), chunk), :] = stage_ref[slot].astype(F32)
            return 0

        lax.fori_loop(0, n_chunks, body, 0)
        dwr_ref[...] = jnp.zeros_like(dwr_ref)
        mean_prob = totals[:, n_experts:2 * n_experts] / n_tokens
        aux_ref[0, 0] = AUX_COEF * n_experts * jnp.sum(frac * mean_prob)

    def group(c, _):
        for i in range(GROUP):
            for k, ref in enumerate((first_ref, second_ref)):
                q = pos_ref[step * (block // GROUP) + c, k, i]
                ref[c * (GROUP // 8) + i // 8, i % 8:i % 8 + 1, :] = rows_ref[pl.ds(q, 1), :]
        return 0

    lax.fori_loop(0, block // GROUP, group, 0)

    h = hidden_ref[...].astype(F32)
    dy = dout_ref[...].astype(F32)
    m = OUT_SCALE * dy
    y0 = first_ref[:, :, 0:d].reshape(block, d)
    y1 = second_ref[:, :, 0:d].reshape(block, d)
    dx = (first_ref[:, :, d:2 * d] + second_ref[:, :, d:2 * d]).reshape(block, d)
    g = gate_ref[...].T
    out_ref[...] = (h + OUT_SCALE * (g[:, 0:1] * y0 + g[:, 1:2] * y1)).astype(BF16)

    ones = jnp.ones((8, d), F32)
    dg0 = dot(ones, m * y0, NT, HI)[0:1]
    dg1 = dot(ones, m * y1, NT, HI)[0:1]
    p = prob_ref[...]
    iota_e = lax.broadcasted_iota(jnp.int32, p.shape, 0)
    hit0 = iota_e == ids_ref[0:1, :]
    hit1 = iota_e == ids_ref[1:2, :]
    den = jnp.sum(jnp.where(hit0 | hit1, p, 0.0), axis=0, keepdims=True)
    mean = gate_ref[0:1, :] * dg0 + gate_ref[1:2, :] * dg1
    eye = lax.broadcasted_iota(jnp.int32, (n_experts, n_experts), 0) == lax.broadcasted_iota(jnp.int32, (n_experts, n_experts), 1)
    ct = (AUX_COEF * n_experts / n_tokens) * jnp.sum(jnp.where(eye, frac, 0.0), axis=1, keepdims=True)
    dp = jnp.where(hit0, (dg0 - mean) / den, 0.0) + jnp.where(hit1, (dg1 - mean) / den, 0.0) + ct
    dz = p * (dp - jnp.sum(p * dp, axis=0, keepdims=True))
    dwr_ref[...] += dot(dz, h, precision=HI)
    dh_ref[...] = (dy + dx + dot(dz, wr_ref[...], TN, HI)).astype(BF16)


def sum_kernel(ep, etp, part_ref, out_ref, box_ref, mine_ref, all_ref, send1, recv1, send2, recv2):
    n_dev = ep * etp
    across = part_ref.shape[1] // 128
    me = lax.axis_index("ep") * etp + lax.axis_index("etp")

    def where_is(peer):
        return {"ep": peer // etp, "etp": peer % etp}

    def tile(ref, i):
        return ref.at[pl.ds(pl.multiple_of((i // across) * 8, 8), 8), pl.ds(pl.multiple_of((i % across) * 128, 128), 128)]

    def wait_bytes(ref, sem):
        pltpu.make_async_copy(ref, ref, sem).wait()

    barrier = pltpu.get_barrier_semaphore()

    def hello(i, _):
        pl.semaphore_signal(barrier, inc=1, device_id=where_is((me + i) % n_dev), device_id_type=MESH)
        return 0

    lax.fori_loop(1, n_dev, hello, 0)
    pl.semaphore_wait(barrier, n_dev - 1)

    def first(i, _):
        peer = (me + i) % n_dev
        pltpu.make_async_remote_copy(tile(part_ref, peer), box_ref.at[me], send1, recv1, device_id=where_is(peer), device_id_type=MESH).start()
        return 0

    lax.fori_loop(1, n_dev, first, 0)
    pltpu.make_async_copy(tile(part_ref, me), box_ref.at[me], recv1).start()
    wait_bytes(box_ref, recv1)
    mine_ref[...] = jnp.sum(box_ref[...], axis=0)

    def second(i, _):
        peer = (me + i) % n_dev
        pltpu.make_async_remote_copy(mine_ref, all_ref.at[me], send2, recv2, device_id=where_is(peer), device_id_type=MESH).start()
        return 0

    lax.fori_loop(1, n_dev, second, 0)
    all_ref[me] = mine_ref[...]
    wait_bytes(all_ref.at[0:n_dev - 1], recv2)
    for i in range(n_dev):
        out_ref[(i // across) * 8:(i // across) * 8 + 8, (i % across) * 128:(i % across) * 128 + 128] = all_ref[i]
    wait_bytes(box_ref.at[0:n_dev - 1], send1)
    wait_bytes(all_ref.at[0:n_dev - 1], send2)


def assemble_kernel(per, came, *refs):
    parts, outs = refs[0:6], refs[-6:-3]
    stage_ref, in_sem, out_sem = refs[-3:]
    me_t = lax.axis_index("etp")
    z, y = me_t // 2, me_t % 2
    starts = ((1 - z) * per, (3 - y) * per) if came else (z * per, (2 + y) * per)
    loads = [pltpu.make_async_copy(parts[i], stage_ref.at[i], in_sem.at[i]) for i in range(6)]
    stores = [pltpu.make_async_copy(stage_ref.at[i], outs[i % 3].at[pl.ds(starts[i // 3], per)], out_sem.at[i]) for i in range(6)]
    for load in loads:
        load.start()
    for load, store in zip(loads, stores):
        load.wait()
        store.start()
    for store in stores:
        store.wait()


def solution(mesh):
    ep_size = mesh.shape["ep"]
    etp_size = mesh.shape["etp"]
    n_dev = ep_size * etp_size
    all_axes = ("ep", "etp")
    tok_spec = P(all_axes, None)
    gate_spec = P("ep", None, "etp")
    down_spec = P("ep", "etp", None)

    def layer(hidden, w_router, expert_ids, d_out, w_gate, w_up, w_down):
        rows, d = hidden.shape
        n_experts = w_router.shape[1]
        n_tokens = rows * n_dev
        capacity = (5 * n_tokens + 2 * n_experts - 1) // (2 * n_experts)
        per_expert = 7 * rows // (2 * n_experts)
        n_slots = n_experts // n_dev
        local_experts, _, part = w_gate.shape
        ff = part * etp_size
        all_slots = n_experts * per_expert
        assert etp_size == 4 and ep_size == 4
        me_t = lax.axis_index("etp")
        z, y = me_t // 2, me_t % 2
        per = n_experts // ep_size // 4
        swap_y = [(t, t ^ 1) for t in range(4)]
        swap_z = [(t, t ^ 2) for t in range(4)]

        weights = w_gate, w_up, w_down

        def parts_at(w, start):
            return lax.dynamic_slice_in_dim(w, start, per)

        near, twin = ([], []), ([], [])
        for w in weights:
            near[0].append(lax.ppermute(parts_at(w, (1 - z) * per), "etp", swap_z))
            near[1].append(lax.ppermute(parts_at(w, (3 - y) * per), "etp", swap_y))
            twin[0].append(lax.ppermute(parts_at(w, z * per), "etp", swap_y))
            twin[1].append(lax.ppermute(parts_at(w, (2 + y) * per), "etp", swap_z))
        ids_t = expert_ids.T
        wr_t = w_router.T

        vmem = pl.BlockSpec(memory_space=pltpu.VMEM)
        smem = pl.BlockSpec(memory_space=pltpu.SMEM)
        anywhere = pl.BlockSpec(memory_space=pl.ANY)
        big = 60 * 1024 * 1024

        pos, gates, probs, stats = pl.pallas_call(
            functools.partial(route_kernel, per_expert),
            out_shape=(
                jax.ShapeDtypeStruct((2, rows), jnp.int32),
                jax.ShapeDtypeStruct((8, rows), F32),
                jax.ShapeDtypeStruct((n_experts, rows), F32),
                jax.ShapeDtypeStruct((8, 2 * n_experts), F32),
            ),
            in_specs=[vmem] * 3,
            out_specs=(vmem,) * 4,
            cost_estimate=pl.CostEstimate(flops=5_000_000_000, bytes_accessed=4_000_000, transcendentals=0),
            name="route",
        )(hidden, wr_t, ids_t)

        block = min(512, rows)
        steps = rows // block
        pos = pos.reshape(2, rows // GROUP, GROUP).transpose(1, 0, 2)
        tile = n_slots * per_expert
        tiles = all_slots // tile
        send = pl.pallas_call(
            functools.partial(scatter_kernel, steps),
            out_shape=jax.ShapeDtypeStruct((all_slots, 2 * d), BF16),
            grid=(steps + tiles,),
            in_specs=[
                smem,
                pl.BlockSpec((8, block), lambda i: (0, jnp.minimum(i, steps - 1))),
                pl.BlockSpec((block, d), lambda i: (jnp.minimum(i, steps - 1), 0)),
                pl.BlockSpec((block, d), lambda i: (jnp.minimum(i, steps - 1), 0)),
            ],
            out_specs=pl.BlockSpec((tile, 2 * d), lambda i: (jnp.maximum(i - steps, 0), 0)),
            scratch_shapes=[pltpu.VMEM((block // 8, 8, 2 * d), F32)] * 2 + [pltpu.VMEM((all_slots, 2 * d), F32)],
            compiler_params=pltpu.CompilerParams(vmem_limit_bytes=big),
            cost_estimate=pl.CostEstimate(flops=50_000_000_000, bytes_accessed=20_000_000, transcendentals=0),
            name="scatter",
        )(pos, gates, hidden, d_out)
        send = send.reshape(n_experts, per_expert, 2 * d)

        dma = pltpu.SemaphoreType.DMA
        assert part == d
        slots = 2 * per
        sources = n_dev // 2
        ring = 3
        results = (jax.ShapeDtypeStruct((local_experts, d, part), F32),) * 3
        back, *rest = pl.pallas_call(
            functools.partial(expert_kernel, ep_size, etp_size, float(capacity)),
            out_shape=(
                jax.ShapeDtypeStruct((n_experts, per_expert, 2 * d), BF16),
                *(jax.ShapeDtypeStruct((per, d, part), F32),) * 12,
                jax.ShapeDtypeStruct((n_dev, 8, 2 * n_experts), F32),
            ),
            in_specs=[anywhere, vmem] + [anywhere] * 15,
            out_specs=(anywhere,) * 13 + (vmem,),
            scratch_shapes=[
                pltpu.VMEM((slots, sources, per_expert, 2 * d), BF16),
                pltpu.VMEM((slots, d, 2 * ff), BF16),
                pltpu.VMEM((slots, ff, d), BF16),
                pltpu.VMEM((ring, d, 2 * ff), F32),
                pltpu.VMEM((ring, ff, d), F32),
                pltpu.VMEM((d, ff), F32),
                pltpu.VMEM((slots, 6, d, part), F32),
                pltpu.VMEM((2 * per_expert, 2 * d), BF16),
                pltpu.VMEM((2 * per_expert, ff), BF16),
                pltpu.VMEM((2 * per_expert, 2 * ff), BF16),
                pltpu.VMEM((n_dev, 8, 2 * n_experts), F32),
                dma, dma, dma((18,)), dma((6,)), dma((6,)), dma, dma((slots,)), dma, dma, dma, dma((ring,)), dma((slots,)),
            ],
            cost_estimate=pl.CostEstimate(flops=300_000_000_000, bytes_accessed=60_000_000, transcendentals=0),
            compiler_params=pltpu.CompilerParams(collective_id=0, has_side_effects=True, vmem_limit_bytes=big),
            name="experts",
        )(send, stats, *weights, *near[0], *near[1], *twin[0], *twin[1])
        table = rest[-1]
        mine, onward = rest[0:6], rest[6:12]
        came = [None] * 6
        for w in range(3):
            for kind, swap in ((0, swap_z), (1, swap_y)):
                came[kind * 3 + w] = lax.ppermute(onward[kind * 3 + w], "etp", swap)

        cols = lambda n: pl.BlockSpec((n, block), lambda i: (0, i))
        tok = pl.BlockSpec((block, d), lambda i: (i, 0))
        output, d_hidden, dwr_part, aux_loss = pl.pallas_call(
            functools.partial(combine_kernel, n_tokens, tile),
            out_shape=(
                jax.ShapeDtypeStruct((rows, d), BF16),
                jax.ShapeDtypeStruct((rows, d), BF16),
                jax.ShapeDtypeStruct((n_experts, d), F32),
                jax.ShapeDtypeStruct((1, 1), F32),
            ),
            grid=(steps,),
            in_specs=[smem, anywhere, vmem, vmem, tok, tok, cols(2), cols(8), cols(n_experts)],
            out_specs=(tok, tok, pl.BlockSpec((n_experts, d), lambda i: (0, 0)), smem),
            scratch_shapes=[
                pltpu.VMEM((all_slots, 2 * d), F32),
                pltpu.VMEM((2, tile, 2 * d), BF16),
                pltpu.VMEM((block // 8, 8, 2 * d), F32),
                pltpu.VMEM((block // 8, 8, 2 * d), F32),
                dma((2,)),
            ],
            compiler_params=pltpu.CompilerParams(vmem_limit_bytes=big),
            cost_estimate=pl.CostEstimate(flops=60_000_000_000, bytes_accessed=30_000_000, transcendentals=0),
            name="combine",
        )(pos, back.reshape(all_slots, 2 * d), table, wr_t, hidden, d_out, ids_t, gates, probs)

        stages = [pltpu.VMEM((6, per, d, part), F32), dma((6,)), dma((6,))]
        half = pl.pallas_call(
            functools.partial(assemble_kernel, per, False),
            out_shape=results,
            in_specs=[anywhere] * 6,
            out_specs=(anywhere,) * 3,
            scratch_shapes=stages,
            cost_estimate=pl.CostEstimate(flops=5_000_000_000, bytes_accessed=12_000_000, transcendentals=0),
            compiler_params=pltpu.CompilerParams(vmem_limit_bytes=big),
            name="place_own",
        )(*mine)
        dwr_part, *half = lax.optimization_barrier((dwr_part, *half))
        dwr = pl.pallas_call(
            functools.partial(sum_kernel, ep_size, etp_size),
            out_shape=jax.ShapeDtypeStruct((n_experts, d), F32),
            in_specs=[vmem],
            out_specs=vmem,
            scratch_shapes=[
                pltpu.VMEM((n_dev, 8, 128), F32), pltpu.VMEM((8, 128), F32), pltpu.VMEM((n_dev, 8, 128), F32),
                dma, dma, dma, dma,
            ],
            compiler_params=pltpu.CompilerParams(collective_id=1, has_side_effects=True),
            cost_estimate=pl.CostEstimate(flops=10_000_000_000, bytes_accessed=100_000, transcendentals=0),
            name="sum_router",
        )(dwr_part)
        g_gate, g_up, g_down = pl.pallas_call(
            functools.partial(assemble_kernel, per, True),
            out_shape=results,
            in_specs=[anywhere] * 9,
            out_specs=(anywhere,) * 3,
            input_output_aliases={6: 0, 7: 1, 8: 2},
            scratch_shapes=stages,
            compiler_params=pltpu.CompilerParams(vmem_limit_bytes=big),
            name="assemble",
        )(*came, *half)
        return output, d_hidden, dwr.T, aux_loss.reshape(()), g_gate, g_up, g_down

    return jax.shard_map(layer, mesh=mesh, in_specs=(tok_spec, P(), tok_spec, tok_spec, gate_spec, gate_spec, down_spec), out_specs=(tok_spec, tok_spec, P(), P(), gate_spec, gate_spec, down_spec), check_vma=False)
```

```python
import functools
import jax
import jax.numpy as jnp
from jax import lax
from jax.experimental import pallas as pl
from jax.experimental.pallas import tpu as pltpu
from jax.sharding import PartitionSpec as P

AUX_COEF = 0.01
OUT_SCALE = 2.0
GROUP = 128
F32 = jnp.float32
BF16 = jnp.bfloat16
HI = lax.Precision.HIGHEST
MESH = pl.DeviceIdType.MESH
NT = (((1,), (1,)), ((), ()))
TN = (((0,), (0,)), ((), ()))


def dot(a, b, dims=(((1,), (0,)), ((), ())), precision=None):
    return lax.dot_general(a, b, dims, precision=precision, preferred_element_type=F32)


def flip(index, mask, bits):
    total = 0
    for bit in range(bits):
        total = total + ((index // 2**bit + mask // 2**bit) % 2) * 2**bit
    return total


def route_kernel(per_expert, hidden_ref, wr_ref, ids_ref, pos_ref, gate_ref, prob_ref, stat_ref):
    n_experts = wr_ref.shape[0]
    rows = hidden_ref.shape[0]
    block = min(512, rows)
    iota_e = lax.broadcasted_iota(jnp.int32, (n_experts, block), 0)
    upper = (lax.broadcasted_iota(jnp.int32, (block, block), 0) < lax.broadcasted_iota(jnp.int32, (block, block), 1)).astype(BF16)
    ones = jnp.ones((8, block), BF16)
    ones_f = jnp.ones((8, block), F32)
    wr = wr_ref[...]
    wr_hi = wr.astype(BF16)
    rest = wr - wr_hi.astype(F32)
    wr_mid = rest.astype(BF16)
    wr_lo = (rest - wr_mid.astype(F32)).astype(BF16)
    gate_ref[...] = jnp.zeros_like(gate_ref)
    carry = jnp.zeros((n_experts, 1), F32)
    counts = jnp.zeros((8, n_experts), F32)
    probs = jnp.zeros((8, n_experts), F32)
    for i in range(rows // block):
        cols = pl.ds(i * block, block)
        h = hidden_ref[cols, :]
        z = dot(wr_lo, h, NT) + dot(wr_mid, h, NT) + dot(wr_hi, h, NT)
        e = jnp.exp(z - jnp.max(z, axis=0, keepdims=True))
        p = e / jnp.sum(e, axis=0, keepdims=True)
        prob_ref[:, cols] = p
        id0 = ids_ref[0:1, cols]
        id1 = ids_ref[1:2, cols]
        hit0 = iota_e == id0
        hit1 = iota_e == id1
        p0 = jnp.sum(jnp.where(hit0, p, 0.0), axis=0, keepdims=True)
        p1 = jnp.sum(jnp.where(hit1, p, 0.0), axis=0, keepdims=True)
        den = p0 + p1
        gate_ref[0:1, cols] = p0 / den
        gate_ref[1:2, cols] = p1 / den
        hits = jnp.where(hit0 | hit1, 1.0, 0.0).astype(F32)
        hits_b = hits.astype(BF16)
        rank = dot(hits_b, upper) + carry
        r0 = jnp.sum(jnp.where(hit0, rank, 0.0), axis=0, keepdims=True)
        r1 = jnp.sum(jnp.where(hit1, rank, 0.0), axis=0, keepdims=True)
        pos_ref[0:1, cols] = id0 * per_expert + r0.astype(jnp.int32)
        pos_ref[1:2, cols] = id1 * per_expert + r1.astype(jnp.int32)
        carry = carry + jnp.sum(hits, axis=1, keepdims=True)
        counts = counts + dot(ones, hits_b, NT)
        probs = probs + dot(ones_f, p, NT, HI)
    stat_ref[:, 0:n_experts] = counts
    stat_ref[:, n_experts:2 * n_experts] = probs


def scatter_kernel(steps, pos_ref, gate_ref, hidden_ref, dout_ref, send_ref, first_ref, second_ref, slots_ref):
    step = pl.program_id(0)
    block, d = hidden_ref.shape
    tile = send_ref.shape[0]

    @pl.when(step < steps)
    def _():
        x = hidden_ref[...].astype(F32)
        m = OUT_SCALE * dout_ref[...].astype(F32)
        g = gate_ref[...].T
        x = x.reshape(block // 8, 8, d)
        first_ref[:, :, 0:d] = x
        first_ref[:, :, d:2 * d] = (g[:, 0:1] * m).reshape(block // 8, 8, d)
        second_ref[:, :, 0:d] = x
        second_ref[:, :, d:2 * d] = (g[:, 1:2] * m).reshape(block // 8, 8, d)

        def group(c, _):
            for i in range(GROUP):
                for k, ref in enumerate((first_ref, second_ref)):
                    q = pos_ref[step * (block // GROUP) + c, k, i]
                    slots_ref[pl.ds(q, 1), :] = ref[c * (GROUP // 8) + i // 8, i % 8:i % 8 + 1, :]
            return 0

        lax.fori_loop(0, block // GROUP, group, 0)

    @pl.when(step >= steps)
    def _():
        start = pl.multiple_of((step - steps) * tile, tile)
        send_ref[...] = slots_ref[pl.ds(start, tile), :].astype(BF16)


def expert_kernel(
    ep, etp, capacity, send_ref, stat_ref, *refs,
):
    own, near, twin, refs = refs[0:3], (refs[3:6], refs[6:9]), (refs[9:12], refs[12:15]), refs[15:]
    back_ref = refs[0]
    mine, onward = (refs[1:4], refs[4:7]), (refs[7:10], refs[10:13])
    tab_out_ref, x_ref, w13_ref, w2f_ref, ga13_ref, ga2_ref, ga2t_ref, twin_ref, xm_ref, u_ref, dab_ref, tab_ref = refs[13:25]
    stat_send, stat_recv, w_recv, relay_send, relay_recv, x_send, x_recv, back_send, back_recv, g_done, g_send, g_recv = refs[25:]
    n_dev = ep * etp
    n_slots, n_src, rows, _ = x_ref.shape
    per = n_slots // 2
    ring = ga13_ref.shape[0]
    d = w2f_ref.shape[2]
    ff = w2f_ref.shape[1]
    part = ff // etp
    bits = n_dev.bit_length() - 1
    src_bits = n_src.bit_length() - 1
    me_o = lax.axis_index("ep")
    me_t = lax.axis_index("etp")
    me = me_o * etp + me_t
    z = me_t // 2
    y = me_t % 2
    t_y = flip(me_t, 1, 2)
    t_z = flip(me_t, 2, 2)
    t_yz = flip(me_t, 3, 2)

    def pick(kind, first, second):
        return first + kind * (second - first)

    def place(kind, w):
        return pick(kind, w * 2 + y, z * 2 + w)

    def remote(src, dst, send, recv, o, t):
        pltpu.make_async_remote_copy(src_ref=src, dst_ref=dst, send_sem=send, recv_sem=recv, device_id={"ep": o, "etp": t}, device_id_type=MESH).start()

    def wait_bytes(ref, sem):
        pltpu.make_async_copy(ref, ref, sem).wait()

    barrier = pltpu.get_barrier_semaphore()

    def hello(i, _):
        peer = (me + i) % n_dev
        pl.semaphore_signal(barrier, inc=1, device_id={"ep": peer // etp, "etp": peer % etp}, device_id_type=MESH)
        return 0

    lax.fori_loop(1, n_dev, hello, 0)
    pl.semaphore_wait(barrier, n_dev - 1)

    def lanes(offset, t):
        return pl.ds(pl.multiple_of(offset + t * part, part), part)

    def places(kind, t):
        group = slice(kind * per, (kind + 1) * per)
        return w13_ref.at[group, :, lanes(0, t)], w13_ref.at[group, :, lanes(ff, t)], w2f_ref.at[group, lanes(0, t), :]

    relays, loads = [], []
    for kind in range(2):
        beside, across = (t_z, t_y) if kind == 0 else (t_y, t_z)
        start = pick(kind, z * per, (2 + y) * per)
        for w in range(3):
            n = kind * 3 + w
            relays.append(pltpu.make_async_remote_copy(
                src_ref=near[kind][w], dst_ref=places(kind, beside)[w], send_sem=relay_send.at[n], recv_sem=relay_recv.at[n],
                device_id={"ep": me_o, "etp": across}, device_id_type=MESH,
            ))
            for ref, t in ((own[w].at[pl.ds(start, per)], me_t), (near[kind][w], beside), (twin[kind][w], across)):
                loads.append(pltpu.make_async_copy(ref, places(kind, t)[w], w_recv.at[len(loads)]))
    for copy in relays + loads:
        copy.start()

    def send_stats(i, _):
        peer = flip(me, (i * 11) % n_dev, bits)
        remote(stat_ref, tab_ref.at[me], stat_send, stat_recv, peer // etp, peer % etp)
        return 0

    lax.fori_loop(1, n_dev, send_stats, 0)
    tab_ref[me] = stat_ref[...]

    def expert_of(o, kind, w, k):
        return o * (4 * per) + kind * (2 * per) + w * per + k

    def send_slot(i, _):
        kind, k = i % 2, i // 2
        here = me_o * 2 + pick(kind, z, y)
        pltpu.make_async_copy(send_ref.at[expert_of(me_o, kind, pick(kind, z, y), k)], x_ref.at[i, here], x_recv.at[i]).start()

        def tokens(m, _):
            there = flip(here, (m * 3) % n_src, src_bits)
            o, w = there // 2, there % 2
            remote(send_ref.at[expert_of(o, kind, w, k)], x_ref.at[i, here], x_send, x_recv.at[i], o, place(kind, w))
            return 0

        lax.fori_loop(1, n_src, tokens, 0)
        return 0

    lax.fori_loop(0, n_slots, send_slot, 0)

    wait_bytes(tab_ref.at[0:n_dev - 1], stat_recv)
    tab_out_ref[...] = tab_ref[...]
    table = tab_ref[:, 0, :]
    shape = table.shape
    below = (lax.broadcasted_iota(jnp.int32, (n_dev, n_dev), 1) < lax.broadcasted_iota(jnp.int32, (n_dev, n_dev), 0)).astype(F32)
    keep = jnp.minimum(table, capacity - dot(below, table, precision=HI))
    src_iota = lax.broadcasted_iota(jnp.int32, shape, 0)
    lane_iota = lax.broadcasted_iota(jnp.int32, shape, 1)
    row_iota = lax.broadcasted_iota(jnp.int32, (rows, 2 * d), 0).astype(F32)

    for copy in loads:
        copy.wait()
    for copy in relays:
        copy.wait_recv()

    def do_slot(i, _):
        kind, k = i % 2, i // 2
        at = kind * per + k
        r = i % ring
        v = pick(kind, z, y)
        expert = expert_of(me_o, kind, v, k)

        @pl.when(i >= ring)
        def _():
            wait_bytes(twin_ref.at[0], g_send.at[r])

        wait_bytes(x_ref.at[i], x_recv.at[i])
        ga13_ref[r] = jnp.zeros((d, 2 * ff), F32)
        ga2t_ref[...] = jnp.zeros((d, ff), F32)

        def give_back(b):
            o = flip(me_o, b, 2)
            for w in range(2):
                away = (o - me_o) * (o - me_o) + (w - v) * (w - v)

                @pl.when(away == 0)
                def _():
                    pltpu.make_async_copy(x_ref.at[i, o * 2 + w], back_ref.at[expert], back_recv).start()

                @pl.when(away != 0)
                def _():
                    remote(x_ref.at[i, o * 2 + w], back_ref.at[expert], back_send, back_recv, o, place(kind, w))

        def do_block(b, _):
            o = flip(me_o, b, 2)
            for w in range(2):
                limit = jnp.sum(jnp.where((src_iota == o * etp + place(kind, w)) & (lane_iota == expert), keep, 0.0), keepdims=True)
                full = x_ref[i, o * 2 + w].astype(F32)
                xm_ref[w * rows:(w + 1) * rows, :] = jnp.where(row_iota < limit, full, 0.0).astype(BF16)
            x = xm_ref[:, 0:d]
            c = xm_ref[:, d:2 * d]
            for q in range(etp):
                here = slice(q * part, (q + 1) * part)
                there = slice(ff + q * part, ff + (q + 1) * part)
                a = dot(x, w13_ref[at, :, here])
                up = dot(x, w13_ref[at, :, there])
                du = dot(c, w2f_ref[at, here, :], NT)
                sig = jax.nn.sigmoid(a)
                silu = a * sig
                u_ref[:, here] = (silu * up).astype(BF16)
                dab_ref[:, here] = (du * up * sig * (1.0 + a * (1.0 - sig))).astype(BF16)
                dab_ref[:, there] = (du * silu).astype(BF16)
            out = dot(u_ref[...], w2f_ref[at]).astype(BF16)
            dx = dot(dab_ref[...], w13_ref[at], NT).astype(BF16)
            for w in range(2):
                x_ref[i, o * 2 + w, :, 0:d] = out[w * rows:(w + 1) * rows]
                x_ref[i, o * 2 + w, :, d:2 * d] = dx[w * rows:(w + 1) * rows]
            ga13_ref[r] += dot(x, dab_ref[...], TN)
            ga2t_ref[...] += dot(c, u_ref[...], TN)

            @pl.when(b > 0)
            def _():
                give_back(b - 1)

            return 0

        lax.fori_loop(0, ep, do_block, 0)
        ga2_ref[r] = ga2t_ref[...].T
        give_back(ep - 1)

        for one in range(2):
            @pl.when(kind == one)
            def _():
                across = t_y if one == 0 else t_z
                for w in range(3):
                    remote(parts(r, across)[w], twin_ref.at[i, w], g_send.at[r], g_recv.at[i], me_o, across)
                    remote(parts(r, t_yz)[w], twin_ref.at[i, 3 + w], g_send.at[r], g_recv.at[i], me_o, across)

        @pl.when(i >= 2)
        def _():
            add_twin(i - 2)

        return 0

    def parts(r, t):
        return ga13_ref.at[r, :, lanes(0, t)], ga13_ref.at[r, :, lanes(ff, t)], ga2_ref.at[r, lanes(0, t), :]

    def add_twin(i):
        kind, k = i % 2, i // 2
        r = i % ring
        wait_bytes(twin_ref.at[i], g_recv.at[i])
        for one in range(2):
            @pl.when(kind == one)
            def _():
                beside = t_z if one == 0 else t_y
                for w in range(3):
                    twin_ref[i, w] += parts(r, me_t)[w][...]
                    twin_ref[i, 3 + w] += parts(r, beside)[w][...]
                for w in range(3):
                    pltpu.make_async_copy(twin_ref.at[i, w], mine[one][w].at[k], g_done).start()
                    pltpu.make_async_copy(twin_ref.at[i, 3 + w], onward[one][w].at[k], g_done).start()

    lax.fori_loop(0, n_slots, do_slot, 0)
    lax.fori_loop(n_slots - 2, n_slots, lambda i, _: (add_twin(i), 0)[1], 0)

    others = (n_src - 1) * n_slots
    wait_bytes(tab_ref.at[0:n_dev - 1], stat_send)
    for copy in relays:
        copy.wait_send()
    wait_bytes(send_ref.at[0:others], x_send)
    wait_bytes(send_ref.at[0:others], back_send)
    for r in range(ring):
        wait_bytes(twin_ref.at[0], g_send.at[r])
    wait_bytes(back_ref, back_recv)
    wait_bytes(twin_ref, g_done)


def combine_kernel(
    n_tokens, chunk,
    pos_ref, back_ref, tab_ref, wr_ref, hidden_ref, dout_ref, ids_ref, gate_ref, prob_ref,
    out_ref, dh_ref, dwr_ref, aux_ref,
    rows_ref, stage_ref, first_ref, second_ref, sem,
):
    step = pl.program_id(0)
    block, d = hidden_ref.shape
    n_experts = wr_ref.shape[0]
    n_chunks = rows_ref.shape[0] // chunk

    totals = jnp.sum(tab_ref[:, 0:1, :], axis=0)
    frac = totals[:, 0:n_experts] / (2 * n_tokens)

    def fetch(i, slot):
        start = pl.multiple_of(i * chunk, chunk)
        return pltpu.make_async_copy(back_ref.at[pl.ds(start, chunk), :], stage_ref.at[slot], sem.at[slot])

    @pl.when(step == 0)
    def _():
        fetch(0, 0).start()

        def body(i, _):
            slot = i % 2

            @pl.when(i + 1 < n_chunks)
            def _():
                fetch(i + 1, 1 - slot).start()

            fetch(i, slot).wait()
            rows_ref[pl.ds(pl.multiple_of(i * chunk, chunk), chunk), :] = stage_ref[slot].astype(F32)
            return 0

        lax.fori_loop(0, n_chunks, body, 0)
        dwr_ref[...] = jnp.zeros_like(dwr_ref)
        mean_prob = totals[:, n_experts:2 * n_experts] / n_tokens
        aux_ref[0, 0] = AUX_COEF * n_experts * jnp.sum(frac * mean_prob)

    def group(c, _):
        for i in range(GROUP):
            for k, ref in enumerate((first_ref, second_ref)):
                q = pos_ref[step * (block // GROUP) + c, k, i]
                ref[c * (GROUP // 8) + i // 8, i % 8:i % 8 + 1, :] = rows_ref[pl.ds(q, 1), :]
        return 0

    lax.fori_loop(0, block // GROUP, group, 0)

    h = hidden_ref[...].astype(F32)
    dy = dout_ref[...].astype(F32)
    m = OUT_SCALE * dy
    y0 = first_ref[:, :, 0:d].reshape(block, d)
    y1 = second_ref[:, :, 0:d].reshape(block, d)
    dx = (first_ref[:, :, d:2 * d] + second_ref[:, :, d:2 * d]).reshape(block, d)
    g = gate_ref[...].T
    out_ref[...] = (h + OUT_SCALE * (g[:, 0:1] * y0 + g[:, 1:2] * y1)).astype(BF16)

    ones = jnp.ones((8, d), F32)
    dg0 = dot(ones, m * y0, NT, HI)[0:1]
    dg1 = dot(ones, m * y1, NT, HI)[0:1]
    p = prob_ref[...]
    iota_e = lax.broadcasted_iota(jnp.int32, p.shape, 0)
    hit0 = iota_e == ids_ref[0:1, :]
    hit1 = iota_e == ids_ref[1:2, :]
    den = jnp.sum(jnp.where(hit0 | hit1, p, 0.0), axis=0, keepdims=True)
    mean = gate_ref[0:1, :] * dg0 + gate_ref[1:2, :] * dg1
    eye = lax.broadcasted_iota(jnp.int32, (n_experts, n_experts), 0) == lax.broadcasted_iota(jnp.int32, (n_experts, n_experts), 1)
    ct = (AUX_COEF * n_experts / n_tokens) * jnp.sum(jnp.where(eye, frac, 0.0), axis=1, keepdims=True)
    dp = jnp.where(hit0, (dg0 - mean) / den, 0.0) + jnp.where(hit1, (dg1 - mean) / den, 0.0) + ct
    dz = p * (dp - jnp.sum(p * dp, axis=0, keepdims=True))
    dwr_ref[...] += dot(dz, h, precision=HI)
    dh_ref[...] = (dy + dx + dot(dz, wr_ref[...], TN, HI)).astype(BF16)


def sum_kernel(ep, etp, part_ref, out_ref, box_ref, mine_ref, all_ref, send1, recv1, send2, recv2):
    n_dev = ep * etp
    across = part_ref.shape[1] // 128
    me = lax.axis_index("ep") * etp + lax.axis_index("etp")

    def where_is(peer):
        return {"ep": peer // etp, "etp": peer % etp}

    def tile(ref, i):
        return ref.at[pl.ds(pl.multiple_of((i // across) * 8, 8), 8), pl.ds(pl.multiple_of((i % across) * 128, 128), 128)]

    def wait_bytes(ref, sem):
        pltpu.make_async_copy(ref, ref, sem).wait()

    barrier = pltpu.get_barrier_semaphore()

    def hello(i, _):
        pl.semaphore_signal(barrier, inc=1, device_id=where_is((me + i) % n_dev), device_id_type=MESH)
        return 0

    lax.fori_loop(1, n_dev, hello, 0)
    pl.semaphore_wait(barrier, n_dev - 1)

    def first(i, _):
        peer = (me + i) % n_dev
        pltpu.make_async_remote_copy(tile(part_ref, peer), box_ref.at[me], send1, recv1, device_id=where_is(peer), device_id_type=MESH).start()
        return 0

    lax.fori_loop(1, n_dev, first, 0)
    pltpu.make_async_copy(tile(part_ref, me), box_ref.at[me], recv1).start()
    wait_bytes(box_ref, recv1)
    mine_ref[...] = jnp.sum(box_ref[...], axis=0)

    def second(i, _):
        peer = (me + i) % n_dev
        pltpu.make_async_remote_copy(mine_ref, all_ref.at[me], send2, recv2, device_id=where_is(peer), device_id_type=MESH).start()
        return 0

    lax.fori_loop(1, n_dev, second, 0)
    all_ref[me] = mine_ref[...]
    wait_bytes(all_ref.at[0:n_dev - 1], recv2)
    for i in range(n_dev):
        out_ref[(i // across) * 8:(i // across) * 8 + 8, (i % across) * 128:(i % across) * 128 + 128] = all_ref[i]
    wait_bytes(box_ref.at[0:n_dev - 1], send1)
    wait_bytes(all_ref.at[0:n_dev - 1], send2)


def place_kernel(per, plan, n_outs, *refs):
    parts, outs = refs[0:len(plan)], refs[-3 - n_outs:-3]
    stage_ref, in_sem, out_sem = refs[-3:]
    me_t = lax.axis_index("etp")
    z, y = me_t // 2, me_t % 2
    starts = (z * per, (2 + y) * per), ((1 - z) * per, (3 - y) * per)
    loads, stores = [], []
    for i, (out, kind, came) in enumerate(plan):
        loads.append(pltpu.make_async_copy(parts[i], stage_ref.at[i], in_sem.at[i]))
        stores.append(pltpu.make_async_copy(stage_ref.at[i], outs[out].at[pl.ds(starts[came][kind], per)], out_sem.at[i]))
    for load in loads:
        load.start()
    for load, store in zip(loads, stores):
        load.wait()
        store.start()
    for store in stores:
        store.wait()


def solution(mesh):
    ep_size = mesh.shape["ep"]
    etp_size = mesh.shape["etp"]
    n_dev = ep_size * etp_size
    all_axes = ("ep", "etp")
    tok_spec = P(all_axes, None)
    gate_spec = P("ep", None, "etp")
    down_spec = P("ep", "etp", None)

    def layer(hidden, w_router, expert_ids, d_out, w_gate, w_up, w_down):
        rows, d = hidden.shape
        n_experts = w_router.shape[1]
        n_tokens = rows * n_dev
        capacity = (5 * n_tokens + 2 * n_experts - 1) // (2 * n_experts)
        per_expert = 7 * rows // (2 * n_experts)
        n_slots = n_experts // n_dev
        local_experts, _, part = w_gate.shape
        ff = part * etp_size
        all_slots = n_experts * per_expert
        assert etp_size == 4 and ep_size == 4
        me_t = lax.axis_index("etp")
        z, y = me_t // 2, me_t % 2
        per = n_experts // ep_size // 4
        swap_y = [(t, t ^ 1) for t in range(4)]
        swap_z = [(t, t ^ 2) for t in range(4)]

        weights = w_gate, w_up, w_down

        def parts_at(w, start):
            return lax.dynamic_slice_in_dim(w, start, per)

        near, twin = ([], []), ([], [])
        for w in weights:
            near[0].append(lax.ppermute(parts_at(w, (1 - z) * per), "etp", swap_z))
            near[1].append(lax.ppermute(parts_at(w, (3 - y) * per), "etp", swap_y))
            twin[0].append(lax.ppermute(parts_at(w, z * per), "etp", swap_y))
            twin[1].append(lax.ppermute(parts_at(w, (2 + y) * per), "etp", swap_z))
        ids_t = expert_ids.T
        wr_t = w_router.T

        vmem = pl.BlockSpec(memory_space=pltpu.VMEM)
        smem = pl.BlockSpec(memory_space=pltpu.SMEM)
        anywhere = pl.BlockSpec(memory_space=pl.ANY)
        big = 60 * 1024 * 1024

        pos, gates, probs, stats = pl.pallas_call(
            functools.partial(route_kernel, per_expert),
            out_shape=(
                jax.ShapeDtypeStruct((2, rows), jnp.int32),
                jax.ShapeDtypeStruct((8, rows), F32),
                jax.ShapeDtypeStruct((n_experts, rows), F32),
                jax.ShapeDtypeStruct((8, 2 * n_experts), F32),
            ),
            in_specs=[vmem] * 3,
            out_specs=(vmem,) * 4,
            cost_estimate=pl.CostEstimate(flops=5_000_000_000, bytes_accessed=4_000_000, transcendentals=0),
            name="route",
        )(hidden, wr_t, ids_t)

        block = min(512, rows)
        steps = rows // block
        pos = pos.reshape(2, rows // GROUP, GROUP).transpose(1, 0, 2)
        tile = n_slots * per_expert
        tiles = all_slots // tile
        send = pl.pallas_call(
            functools.partial(scatter_kernel, steps),
            out_shape=jax.ShapeDtypeStruct((all_slots, 2 * d), BF16),
            grid=(steps + tiles,),
            in_specs=[
                smem,
                pl.BlockSpec((8, block), lambda i: (0, jnp.minimum(i, steps - 1))),
                pl.BlockSpec((block, d), lambda i: (jnp.minimum(i, steps - 1), 0)),
                pl.BlockSpec((block, d), lambda i: (jnp.minimum(i, steps - 1), 0)),
            ],
            out_specs=pl.BlockSpec((tile, 2 * d), lambda i: (jnp.maximum(i - steps, 0), 0)),
            scratch_shapes=[pltpu.VMEM((block // 8, 8, 2 * d), F32)] * 2 + [pltpu.VMEM((all_slots, 2 * d), F32)],
            compiler_params=pltpu.CompilerParams(vmem_limit_bytes=big),
            cost_estimate=pl.CostEstimate(flops=50_000_000_000, bytes_accessed=20_000_000, transcendentals=0),
            name="scatter",
        )(pos, gates, hidden, d_out)
        send = send.reshape(n_experts, per_expert, 2 * d)

        dma = pltpu.SemaphoreType.DMA
        assert part == d
        slots = 2 * per
        sources = n_dev // 2
        ring = 3
        results = (jax.ShapeDtypeStruct((local_experts, d, part), F32),) * 3
        back, *rest = pl.pallas_call(
            functools.partial(expert_kernel, ep_size, etp_size, float(capacity)),
            out_shape=(
                jax.ShapeDtypeStruct((n_experts, per_expert, 2 * d), BF16),
                *(jax.ShapeDtypeStruct((per, d, part), F32),) * 12,
                jax.ShapeDtypeStruct((n_dev, 8, 2 * n_experts), F32),
            ),
            in_specs=[anywhere, vmem] + [anywhere] * 15,
            out_specs=(anywhere,) * 13 + (vmem,),
            scratch_shapes=[
                pltpu.VMEM((slots, sources, per_expert, 2 * d), BF16),
                pltpu.VMEM((slots, d, 2 * ff), BF16),
                pltpu.VMEM((slots, ff, d), BF16),
                pltpu.VMEM((ring, d, 2 * ff), F32),
                pltpu.VMEM((ring, ff, d), F32),
                pltpu.VMEM((d, ff), F32),
                pltpu.VMEM((slots, 6, d, part), F32),
                pltpu.VMEM((2 * per_expert, 2 * d), BF16),
                pltpu.VMEM((2 * per_expert, ff), BF16),
                pltpu.VMEM((2 * per_expert, 2 * ff), BF16),
                pltpu.VMEM((n_dev, 8, 2 * n_experts), F32),
                dma, dma, dma((18,)), dma((6,)), dma((6,)), dma, dma((slots,)), dma, dma, dma, dma((ring,)), dma((slots,)),
            ],
            cost_estimate=pl.CostEstimate(flops=300_000_000_000, bytes_accessed=60_000_000, transcendentals=0),
            compiler_params=pltpu.CompilerParams(collective_id=0, has_side_effects=True, vmem_limit_bytes=big),
            name="experts",
        )(send, stats, *weights, *near[0], *near[1], *twin[0], *twin[1])
        table = rest[-1]
        mine, onward = rest[0:6], rest[6:12]
        came = [None] * 6
        for w in range(3):
            for kind, swap in ((0, swap_z), (1, swap_y)):
                came[kind * 3 + w] = lax.ppermute(onward[kind * 3 + w], "etp", swap)

        cols = lambda n: pl.BlockSpec((n, block), lambda i: (0, i))
        tok = pl.BlockSpec((block, d), lambda i: (i, 0))
        output, d_hidden, dwr_part, aux_loss = pl.pallas_call(
            functools.partial(combine_kernel, n_tokens, tile),
            out_shape=(
                jax.ShapeDtypeStruct((rows, d), BF16),
                jax.ShapeDtypeStruct((rows, d), BF16),
                jax.ShapeDtypeStruct((n_experts, d), F32),
                jax.ShapeDtypeStruct((1, 1), F32),
            ),
            grid=(steps,),
            in_specs=[smem, anywhere, vmem, vmem, tok, tok, cols(2), cols(8), cols(n_experts)],
            out_specs=(tok, tok, pl.BlockSpec((n_experts, d), lambda i: (0, 0)), smem),
            scratch_shapes=[
                pltpu.VMEM((all_slots, 2 * d), F32),
                pltpu.VMEM((2, tile, 2 * d), BF16),
                pltpu.VMEM((block // 8, 8, 2 * d), F32),
                pltpu.VMEM((block // 8, 8, 2 * d), F32),
                dma((2,)),
            ],
            compiler_params=pltpu.CompilerParams(vmem_limit_bytes=big),
            cost_estimate=pl.CostEstimate(flops=60_000_000_000, bytes_accessed=30_000_000, transcendentals=0),
            name="combine",
        )(pos, back.reshape(all_slots, 2 * d), table, wr_t, hidden, d_out, ids_t, gates, probs)

        def place(name, plan, parts, n_outs, into=()):
            return pl.pallas_call(
                functools.partial(place_kernel, per, plan, n_outs),
                out_shape=results[:n_outs],
                in_specs=[anywhere] * (len(parts) + len(into)),
                out_specs=(anywhere,) * n_outs,
                input_output_aliases={len(parts) + i: i for i in range(len(into))},
                scratch_shapes=[pltpu.VMEM((len(parts), per, d, part), F32), dma((len(parts),)), dma((len(parts),))],
                cost_estimate=pl.CostEstimate(flops=1_000_000_000 * len(parts), bytes_accessed=2_000_000 * len(parts), transcendentals=0),
                compiler_params=pltpu.CompilerParams(vmem_limit_bytes=big),
                name=name,
            )(*parts, *into)

        plan = [(w, kind, 0) for w in (2, 0, 1) for kind in range(2)] + [(w, kind, 1) for w in range(2) for kind in range(2)]
        half = place("place", plan, [(mine, came)[c][kind * 3 + w] for w, kind, c in plan], 3)
        dwr_part, *half = lax.optimization_barrier((dwr_part, *half))
        dwr = pl.pallas_call(
            functools.partial(sum_kernel, ep_size, etp_size),
            out_shape=jax.ShapeDtypeStruct((n_experts, d), F32),
            in_specs=[vmem],
            out_specs=vmem,
            scratch_shapes=[
                pltpu.VMEM((n_dev, 8, 128), F32), pltpu.VMEM((8, 128), F32), pltpu.VMEM((n_dev, 8, 128), F32),
                dma, dma, dma, dma,
            ],
            compiler_params=pltpu.CompilerParams(collective_id=1, has_side_effects=True),
            cost_estimate=pl.CostEstimate(flops=10_000_000_000, bytes_accessed=100_000, transcendentals=0),
            name="sum_router",
        )(dwr_part)
        g_gate, g_up = half[0:2]
        g_down, = place("place_last", [(0, 0, 1), (0, 1, 1)], [came[2], came[5]], 1, half[2:3])
        return output, d_hidden, dwr.T, aux_loss.reshape(()), g_gate, g_up, g_down

    return jax.shard_map(layer, mesh=mesh, in_specs=(tok_spec, P(), tok_spec, tok_spec, gate_spec, gate_spec, down_spec), out_specs=(tok_spec, tok_spec, P(), P(), gate_spec, gate_spec, down_spec), check_vma=False)
```

```python
import functools
import jax
import jax.numpy as jnp
from jax import lax
from jax.experimental import pallas as pl
from jax.experimental.pallas import tpu as pltpu
from jax.sharding import PartitionSpec as P


AUX_COEF = 0.01
OUT_SCALE = 2.0
GROUP = 128
F32 = jnp.float32
BF16 = jnp.bfloat16
HI = lax.Precision.HIGHEST
MESH = pl.DeviceIdType.MESH
NT = (((1,), (1,)), ((), ()))
TN = (((0,), (0,)), ((), ()))


def dot(a, b, dims=(((1,), (0,)), ((), ())), precision=None):
    return lax.dot_general(a, b, dims, precision=precision, preferred_element_type=F32)


def flip(index, mask, bits):
    total = 0
    for bit in range(bits):
        total = total + ((index // 2**bit + mask // 2**bit) % 2) * 2**bit
    return total


def route_kernel(per_expert, hidden_ref, wr_ref, ids_ref, pos_ref, gate_ref, prob_ref, stat_ref):
    n_experts = wr_ref.shape[0]
    rows = hidden_ref.shape[0]
    block = min(512, rows)
    iota_e = lax.broadcasted_iota(jnp.int32, (n_experts, block), 0)
    upper = (lax.broadcasted_iota(jnp.int32, (block, block), 0) < lax.broadcasted_iota(jnp.int32, (block, block), 1)).astype(BF16)
    ones = jnp.ones((8, block), BF16)
    ones_f = jnp.ones((8, block), F32)
    wr = wr_ref[...]
    wr_hi = wr.astype(BF16)
    rest = wr - wr_hi.astype(F32)
    wr_mid = rest.astype(BF16)
    wr_lo = (rest - wr_mid.astype(F32)).astype(BF16)
    gate_ref[...] = jnp.zeros_like(gate_ref)
    carry = jnp.zeros((n_experts, 1), F32)
    counts = jnp.zeros((8, n_experts), F32)
    probs = jnp.zeros((8, n_experts), F32)
    for i in range(rows // block):
        cols = pl.ds(i * block, block)
        h = hidden_ref[cols, :]
        z = dot(wr_lo, h, NT) + dot(wr_mid, h, NT) + dot(wr_hi, h, NT)
        e = jnp.exp(z - jnp.max(z, axis=0, keepdims=True))
        p = e / jnp.sum(e, axis=0, keepdims=True)
        prob_ref[:, cols] = p
        id0 = ids_ref[0:1, cols]
        id1 = ids_ref[1:2, cols]
        hit0 = iota_e == id0
        hit1 = iota_e == id1
        p0 = jnp.sum(jnp.where(hit0, p, 0.0), axis=0, keepdims=True)
        p1 = jnp.sum(jnp.where(hit1, p, 0.0), axis=0, keepdims=True)
        den = p0 + p1
        gate_ref[0:1, cols] = p0 / den
        gate_ref[1:2, cols] = p1 / den
        hits = jnp.where(hit0 | hit1, 1.0, 0.0).astype(F32)
        hits_b = hits.astype(BF16)
        rank = dot(hits_b, upper) + carry
        r0 = jnp.sum(jnp.where(hit0, rank, 0.0), axis=0, keepdims=True)
        r1 = jnp.sum(jnp.where(hit1, rank, 0.0), axis=0, keepdims=True)
        pos_ref[0:1, cols] = id0 * per_expert + r0.astype(jnp.int32)
        pos_ref[1:2, cols] = id1 * per_expert + r1.astype(jnp.int32)
        carry = carry + jnp.sum(hits, axis=1, keepdims=True)
        counts = counts + dot(ones, hits_b, NT)
        probs = probs + dot(ones_f, p, NT, HI)
    stat_ref[:, 0:n_experts] = counts
    stat_ref[:, n_experts:2 * n_experts] = probs


def scatter_kernel(steps, pos_ref, gate_ref, hidden_ref, dout_ref, send_ref, first_ref, second_ref, slots_ref):
    step = pl.program_id(0)
    block, d = hidden_ref.shape
    tile = send_ref.shape[0]

    @pl.when(step < steps)
    def _():
        x = hidden_ref[...].astype(F32)
        m = OUT_SCALE * dout_ref[...].astype(F32)
        g = gate_ref[...].T
        x = x.reshape(block // 8, 8, d)
        first_ref[:, :, 0:d] = x
        first_ref[:, :, d:2 * d] = (g[:, 0:1] * m).reshape(block // 8, 8, d)
        second_ref[:, :, 0:d] = x
        second_ref[:, :, d:2 * d] = (g[:, 1:2] * m).reshape(block // 8, 8, d)

        def group(c, _):
            for i in range(GROUP):
                for k, ref in enumerate((first_ref, second_ref)):
                    q = pos_ref[step * (block // GROUP) + c, k, i]
                    slots_ref[pl.ds(q, 1), :] = ref[c * (GROUP // 8) + i // 8, i % 8:i % 8 + 1, :]
            return 0

        lax.fori_loop(0, block // GROUP, group, 0)

    @pl.when(step >= steps)
    def _():
        start = pl.multiple_of((step - steps) * tile, tile)
        send_ref[...] = slots_ref[pl.ds(start, tile), :].astype(BF16)


def expert_kernel(
    ep, etp, capacity, send_ref, stat_ref, *refs,
):
    own, near, twin, refs = refs[0:3], (refs[3:6], refs[6:9]), (refs[9:12], refs[12:15]), refs[15:]
    back_ref = refs[0]
    mine, onward_in, onward_out = (refs[1:4], refs[4:7]), refs[7:9], refs[9:11]
    tab_out_ref, x_ref, w13_ref, w2f_ref, ga13_ref, ga2_ref, ga2t_ref, twin_ref, xm_ref, u_ref, dab_ref, tab_ref = refs[11:23]
    stat_send, stat_recv, w_recv, relay_send, relay_recv, x_send, x_recv, back_send, back_recv, g_done, g_send, g_recv = refs[23:]
    n_dev = ep * etp
    n_slots, n_src, rows, _ = x_ref.shape
    per = n_slots // 2
    ring = ga13_ref.shape[0]
    d = w2f_ref.shape[2]
    ff = w2f_ref.shape[1]
    part = ff // etp
    bits = n_dev.bit_length() - 1
    src_bits = n_src.bit_length() - 1
    me_o = lax.axis_index("ep")
    me_t = lax.axis_index("etp")
    me = me_o * etp + me_t
    z = me_t // 2
    y = me_t % 2
    t_y = flip(me_t, 1, 2)
    t_z = flip(me_t, 2, 2)
    t_yz = flip(me_t, 3, 2)

    def pick(kind, first, second):
        return first + kind * (second - first)

    def place(kind, w):
        return pick(kind, w * 2 + y, z * 2 + w)

    def remote(src, dst, send, recv, o, t):
        pltpu.make_async_remote_copy(src_ref=src, dst_ref=dst, send_sem=send, recv_sem=recv, device_id={"ep": o, "etp": t}, device_id_type=MESH).start()

    def wait_bytes(ref, sem):
        pltpu.make_async_copy(ref, ref, sem).wait()

    barrier = pltpu.get_barrier_semaphore()

    def hello(i, _):
        peer = (me + i) % n_dev
        pl.semaphore_signal(barrier, inc=1, device_id={"ep": peer // etp, "etp": peer % etp}, device_id_type=MESH)
        return 0

    lax.fori_loop(1, n_dev, hello, 0)
    pl.semaphore_wait(barrier, n_dev - 1)

    def lanes(offset, t):
        return pl.ds(pl.multiple_of(offset + t * part, part), part)

    def places(kind, t):
        group = slice(kind * per, (kind + 1) * per)
        return w13_ref.at[group, :, lanes(0, t)], w13_ref.at[group, :, lanes(ff, t)], w2f_ref.at[group, lanes(0, t), :]

    relays, loads = [], []
    for kind in range(2):
        beside, across = (t_z, t_y) if kind == 0 else (t_y, t_z)
        start = pick(kind, z * per, (2 + y) * per)
        for w in range(3):
            n = kind * 3 + w
            relays.append(pltpu.make_async_remote_copy(
                src_ref=near[kind][w], dst_ref=places(kind, beside)[w], send_sem=relay_send.at[n], recv_sem=relay_recv.at[n],
                device_id={"ep": me_o, "etp": across}, device_id_type=MESH,
            ))
            for ref, t in ((own[w].at[pl.ds(start, per)], me_t), (near[kind][w], beside), (twin[kind][w], across)):
                loads.append(pltpu.make_async_copy(ref, places(kind, t)[w], w_recv.at[len(loads)]))
    for copy in relays + loads:
        copy.start()

    def send_stats(i, _):
        peer = flip(me, (i * 11) % n_dev, bits)
        remote(stat_ref, tab_ref.at[me], stat_send, stat_recv, peer // etp, peer % etp)
        return 0

    lax.fori_loop(1, n_dev, send_stats, 0)
    tab_ref[me] = stat_ref[...]

    def expert_of(o, kind, w, k):
        return o * (4 * per) + kind * (2 * per) + w * per + k

    def send_slot(i, _):
        kind, k = i % 2, i // 2
        here = me_o * 2 + pick(kind, z, y)
        pltpu.make_async_copy(send_ref.at[expert_of(me_o, kind, pick(kind, z, y), k)], x_ref.at[i, here], x_recv.at[i]).start()

        def tokens(m, _):
            there = flip(here, (m * 3) % n_src, src_bits)
            o, w = there // 2, there % 2
            remote(send_ref.at[expert_of(o, kind, w, k)], x_ref.at[i, here], x_send, x_recv.at[i], o, place(kind, w))
            return 0

        lax.fori_loop(1, n_src, tokens, 0)
        return 0

    lax.fori_loop(0, n_slots, send_slot, 0)

    wait_bytes(tab_ref.at[0:n_dev - 1], stat_recv)
    tab_out_ref[...] = tab_ref[...]
    table = tab_ref[:, 0, :]
    shape = table.shape
    below = (lax.broadcasted_iota(jnp.int32, (n_dev, n_dev), 1) < lax.broadcasted_iota(jnp.int32, (n_dev, n_dev), 0)).astype(F32)
    keep = jnp.minimum(table, capacity - dot(below, table, precision=HI))
    src_iota = lax.broadcasted_iota(jnp.int32, shape, 0)
    lane_iota = lax.broadcasted_iota(jnp.int32, shape, 1)
    row_iota = lax.broadcasted_iota(jnp.int32, (rows, 2 * d), 0).astype(F32)

    for copy in loads:
        copy.wait()
    for copy in relays:
        copy.wait_recv()

    def do_slot(i, _):
        kind, k = i % 2, i // 2
        at = kind * per + k
        r = i % ring
        v = pick(kind, z, y)
        expert = expert_of(me_o, kind, v, k)

        @pl.when(i >= ring)
        def _():
            wait_bytes(twin_ref.at[0], g_send.at[r])

        wait_bytes(x_ref.at[i], x_recv.at[i])
        ga13_ref[r] = jnp.zeros((d, 2 * ff), F32)
        ga2t_ref[...] = jnp.zeros((d, ff), F32)

        def give_back(b):
            o = flip(me_o, b, 2)
            for w in range(2):
                away = (o - me_o) * (o - me_o) + (w - v) * (w - v)

                @pl.when(away == 0)
                def _():
                    pltpu.make_async_copy(x_ref.at[i, o * 2 + w], back_ref.at[expert], back_recv).start()

                @pl.when(away != 0)
                def _():
                    remote(x_ref.at[i, o * 2 + w], back_ref.at[expert], back_send, back_recv, o, place(kind, w))

        def do_block(b, _):
            o = flip(me_o, b, 2)
            for w in range(2):
                limit = jnp.sum(jnp.where((src_iota == o * etp + place(kind, w)) & (lane_iota == expert), keep, 0.0), keepdims=True)
                full = x_ref[i, o * 2 + w].astype(F32)
                xm_ref[w * rows:(w + 1) * rows, :] = jnp.where(row_iota < limit, full, 0.0).astype(BF16)
            x = xm_ref[:, 0:d]
            c = xm_ref[:, d:2 * d]
            for q in range(etp):
                here = slice(q * part, (q + 1) * part)
                there = slice(ff + q * part, ff + (q + 1) * part)
                a = dot(x, w13_ref[at, :, here])
                up = dot(x, w13_ref[at, :, there])
                du = dot(c, w2f_ref[at, here, :], NT)
                sig = jax.nn.sigmoid(a)
                silu = a * sig
                u_ref[:, here] = (silu * up).astype(BF16)
                dab_ref[:, here] = (du * up * sig * (1.0 + a * (1.0 - sig))).astype(BF16)
                dab_ref[:, there] = (du * silu).astype(BF16)
            out = dot(u_ref[...], w2f_ref[at]).astype(BF16)
            dx = dot(dab_ref[...], w13_ref[at], NT).astype(BF16)
            for w in range(2):
                x_ref[i, o * 2 + w, :, 0:d] = out[w * rows:(w + 1) * rows]
                x_ref[i, o * 2 + w, :, d:2 * d] = dx[w * rows:(w + 1) * rows]
            ga13_ref[r] += dot(x, dab_ref[...], TN)
            ga2t_ref[...] += dot(c, u_ref[...], TN)

            @pl.when(b > 0)
            def _():
                give_back(b - 1)

            return 0

        lax.fori_loop(0, ep, do_block, 0)
        ga2_ref[r] = ga2t_ref[...].T
        give_back(ep - 1)

        for one in range(2):
            @pl.when(kind == one)
            def _():
                across = t_y if one == 0 else t_z
                for w in range(3):
                    remote(parts(r, across)[w], twin_ref.at[i, w], g_send.at[r], g_recv.at[i], me_o, across)
                    remote(parts(r, t_yz)[w], twin_ref.at[i, 3 + w], g_send.at[r], g_recv.at[i], me_o, across)

        @pl.when(i >= 2)
        def _():
            add_twin(i - 2)

        return 0

    def parts(r, t):
        return ga13_ref.at[r, :, lanes(0, t)], ga13_ref.at[r, :, lanes(ff, t)], ga2_ref.at[r, lanes(0, t), :]

    def add_twin(i):
        kind, k = i % 2, i // 2
        r = i % ring
        wait_bytes(twin_ref.at[i], g_recv.at[i])
        for one in range(2):
            @pl.when(kind == one)
            def _():
                beside = t_z if one == 0 else t_y
                for w in range(3):
                    twin_ref[i, w] += parts(r, me_t)[w][...]
                    twin_ref[i, 3 + w] += parts(r, beside)[w][...]
                for w in range(3):
                    pltpu.make_async_copy(twin_ref.at[i, w], mine[one][w].at[k], g_done).start()
                    onward = onward_in[one].at[w * per + k] if w < 2 else onward_out[one].at[k]
                    pltpu.make_async_copy(twin_ref.at[i, 3 + w], onward, g_done).start()

    lax.fori_loop(0, n_slots, do_slot, 0)
    lax.fori_loop(n_slots - 2, n_slots, lambda i, _: (add_twin(i), 0)[1], 0)

    others = (n_src - 1) * n_slots
    wait_bytes(tab_ref.at[0:n_dev - 1], stat_send)
    for copy in relays:
        copy.wait_send()
    wait_bytes(send_ref.at[0:others], x_send)
    wait_bytes(send_ref.at[0:others], back_send)
    for r in range(ring):
        wait_bytes(twin_ref.at[0], g_send.at[r])
    wait_bytes(back_ref, back_recv)
    wait_bytes(twin_ref, g_done)


def combine_kernel(
    n_tokens, chunk,
    pos_ref, back_ref, tab_ref, wr_ref, hidden_ref, dout_ref, ids_ref, gate_ref, prob_ref,
    out_ref, dh_ref, dwr_ref, aux_ref,
    rows_ref, stage_ref, first_ref, second_ref, sem,
):
    step = pl.program_id(0)
    block, d = hidden_ref.shape
    n_experts = wr_ref.shape[0]
    n_chunks = rows_ref.shape[0] // chunk

    totals = jnp.sum(tab_ref[:, 0:1, :], axis=0)
    frac = totals[:, 0:n_experts] / (2 * n_tokens)

    def fetch(i, slot):
        start = pl.multiple_of(i * chunk, chunk)
        return pltpu.make_async_copy(back_ref.at[pl.ds(start, chunk), :], stage_ref.at[slot], sem.at[slot])

    @pl.when(step == 0)
    def _():
        fetch(0, 0).start()

        def body(i, _):
            slot = i % 2

            @pl.when(i + 1 < n_chunks)
            def _():
                fetch(i + 1, 1 - slot).start()

            fetch(i, slot).wait()
            rows_ref[pl.ds(pl.multiple_of(i * chunk, chunk), chunk), :] = stage_ref[slot].astype(F32)
            return 0

        lax.fori_loop(0, n_chunks, body, 0)
        dwr_ref[...] = jnp.zeros_like(dwr_ref)
        mean_prob = totals[:, n_experts:2 * n_experts] / n_tokens
        aux_ref[0, 0] = AUX_COEF * n_experts * jnp.sum(frac * mean_prob)

    def group(c, _):
        for i in range(GROUP):
            for k, ref in enumerate((first_ref, second_ref)):
                q = pos_ref[step * (block // GROUP) + c, k, i]
                ref[c * (GROUP // 8) + i // 8, i % 8:i % 8 + 1, :] = rows_ref[pl.ds(q, 1), :]
        return 0

    lax.fori_loop(0, block // GROUP, group, 0)

    h = hidden_ref[...].astype(F32)
    dy = dout_ref[...].astype(F32)
    m = OUT_SCALE * dy
    y0 = first_ref[:, :, 0:d].reshape(block, d)
    y1 = second_ref[:, :, 0:d].reshape(block, d)
    dx = (first_ref[:, :, d:2 * d] + second_ref[:, :, d:2 * d]).reshape(block, d)
    g = gate_ref[...].T
    out_ref[...] = (h + OUT_SCALE * (g[:, 0:1] * y0 + g[:, 1:2] * y1)).astype(BF16)

    ones = jnp.ones((8, d), F32)
    dg0 = dot(ones, m * y0, NT, HI)[0:1]
    dg1 = dot(ones, m * y1, NT, HI)[0:1]
    p = prob_ref[...]
    iota_e = lax.broadcasted_iota(jnp.int32, p.shape, 0)
    hit0 = iota_e == ids_ref[0:1, :]
    hit1 = iota_e == ids_ref[1:2, :]
    den = jnp.sum(jnp.where(hit0 | hit1, p, 0.0), axis=0, keepdims=True)
    mean = gate_ref[0:1, :] * dg0 + gate_ref[1:2, :] * dg1
    eye = lax.broadcasted_iota(jnp.int32, (n_experts, n_experts), 0) == lax.broadcasted_iota(jnp.int32, (n_experts, n_experts), 1)
    ct = (AUX_COEF * n_experts / n_tokens) * jnp.sum(jnp.where(eye, frac, 0.0), axis=1, keepdims=True)
    dp = jnp.where(hit0, (dg0 - mean) / den, 0.0) + jnp.where(hit1, (dg1 - mean) / den, 0.0) + ct
    dz = p * (dp - jnp.sum(p * dp, axis=0, keepdims=True))
    dwr_ref[...] += dot(dz, h, precision=HI)
    dh_ref[...] = (dy + dx + dot(dz, wr_ref[...], TN, HI)).astype(BF16)


def sum_kernel(ep, etp, part_ref, out_ref, box_ref, mine_ref, all_ref, send1, recv1, send2, recv2):
    n_dev = ep * etp
    across = part_ref.shape[1] // 128
    me = lax.axis_index("ep") * etp + lax.axis_index("etp")

    def where_is(peer):
        return {"ep": peer // etp, "etp": peer % etp}

    def tile(ref, i):
        return ref.at[pl.ds(pl.multiple_of((i // across) * 8, 8), 8), pl.ds(pl.multiple_of((i % across) * 128, 128), 128)]

    def wait_bytes(ref, sem):
        pltpu.make_async_copy(ref, ref, sem).wait()

    barrier = pltpu.get_barrier_semaphore()

    def hello(i, _):
        pl.semaphore_signal(barrier, inc=1, device_id=where_is((me + i) % n_dev), device_id_type=MESH)
        return 0

    lax.fori_loop(1, n_dev, hello, 0)
    pl.semaphore_wait(barrier, n_dev - 1)

    def first(i, _):
        peer = (me + i) % n_dev
        pltpu.make_async_remote_copy(tile(part_ref, peer), box_ref.at[me], send1, recv1, device_id=where_is(peer), device_id_type=MESH).start()
        return 0

    lax.fori_loop(1, n_dev, first, 0)
    pltpu.make_async_copy(tile(part_ref, me), box_ref.at[me], recv1).start()
    wait_bytes(box_ref, recv1)
    mine_ref[...] = jnp.sum(box_ref[...], axis=0)

    def second(i, _):
        peer = (me + i) % n_dev
        pltpu.make_async_remote_copy(mine_ref, all_ref.at[me], send2, recv2, device_id=where_is(peer), device_id_type=MESH).start()
        return 0

    lax.fori_loop(1, n_dev, second, 0)
    all_ref[me] = mine_ref[...]
    wait_bytes(all_ref.at[0:n_dev - 1], recv2)
    for i in range(n_dev):
        out_ref[(i // across) * 8:(i // across) * 8 + 8, (i % across) * 128:(i % across) * 128 + 128] = all_ref[i]
    wait_bytes(box_ref.at[0:n_dev - 1], send1)
    wait_bytes(all_ref.at[0:n_dev - 1], send2)


def starts_of(per):
    me_t = lax.axis_index("etp")
    z, y = me_t // 2, me_t % 2
    return (z * per, (2 + y) * per), ((1 - z) * per, (3 - y) * per)


def place_kernel(per, plan, *refs):
    parts, outs = refs[:-6], refs[-6:-3]
    stage_ref, in_sem, out_sem = refs[-3:]
    starts = starts_of(per)
    loads, stores = [], []
    for i, (ref, row, out, kind, came) in enumerate(plan):
        loads.append(pltpu.make_async_copy(parts[ref].at[row:row + per], stage_ref.at[i], in_sem.at[i]))
        stores.append(pltpu.make_async_copy(stage_ref.at[i], outs[out].at[pl.ds(starts[came][kind], per)], out_sem.at[i]))
    for load in loads:
        load.start()
    for load, store in zip(loads, stores):
        load.wait()
        store.start()
    for store in stores:
        store.wait()


def place_last_kernel(per, first_ref, second_ref, _, out_ref, sem):
    starts = starts_of(per)[1]
    copies = [pltpu.make_async_copy(ref, out_ref.at[pl.ds(starts[i], per)], sem.at[i]) for i, ref in enumerate((first_ref, second_ref))]
    for copy in copies:
        copy.start()
    for copy in copies:
        copy.wait()


def solution(mesh):
    ep_size = mesh.shape["ep"]
    etp_size = mesh.shape["etp"]
    n_dev = ep_size * etp_size
    all_axes = ("ep", "etp")
    tok_spec = P(all_axes, None)
    gate_spec = P("ep", None, "etp")
    down_spec = P("ep", "etp", None)

    def layer(hidden, w_router, expert_ids, d_out, w_gate, w_up, w_down):
        rows, d = hidden.shape
        n_experts = w_router.shape[1]
        n_tokens = rows * n_dev
        capacity = (5 * n_tokens + 2 * n_experts - 1) // (2 * n_experts)
        per_expert = 7 * rows // (2 * n_experts)
        n_slots = n_experts // n_dev
        local_experts, _, part = w_gate.shape
        ff = part * etp_size
        all_slots = n_experts * per_expert
        assert etp_size == 4 and ep_size == 4
        me_t = lax.axis_index("etp")
        z, y = me_t // 2, me_t % 2
        per = n_experts // ep_size // 4
        swap_y = [(t, t ^ 1) for t in range(4)]
        swap_z = [(t, t ^ 2) for t in range(4)]

        weights = w_gate, w_up, w_down

        def parts_at(w, start):
            return lax.dynamic_slice_in_dim(w, start, per)

        near, twin = ([], []), ([], [])
        for w in weights:
            near[0].append(lax.ppermute(parts_at(w, (1 - z) * per), "etp", swap_z))
            near[1].append(lax.ppermute(parts_at(w, (3 - y) * per), "etp", swap_y))
            twin[0].append(lax.ppermute(parts_at(w, z * per), "etp", swap_y))
            twin[1].append(lax.ppermute(parts_at(w, (2 + y) * per), "etp", swap_z))
        ids_t = expert_ids.T
        wr_t = w_router.T

        vmem = pl.BlockSpec(memory_space=pltpu.VMEM)
        smem = pl.BlockSpec(memory_space=pltpu.SMEM)
        anywhere = pl.BlockSpec(memory_space=pl.ANY)
        big = 60 * 1024 * 1024

        pos, gates, probs, stats = pl.pallas_call(
            functools.partial(route_kernel, per_expert),
            out_shape=(
                jax.ShapeDtypeStruct((2, rows), jnp.int32),
                jax.ShapeDtypeStruct((8, rows), F32),
                jax.ShapeDtypeStruct((n_experts, rows), F32),
                jax.ShapeDtypeStruct((8, 2 * n_experts), F32),
            ),
            in_specs=[vmem] * 3,
            out_specs=(vmem,) * 4,
            cost_estimate=pl.CostEstimate(flops=5_000_000_000, bytes_accessed=4_000_000, transcendentals=0),
            name="route",
        )(hidden, wr_t, ids_t)

        block = min(512, rows)
        steps = rows // block
        pos = pos.reshape(2, rows // GROUP, GROUP).transpose(1, 0, 2)
        tile = n_slots * per_expert
        tiles = all_slots // tile
        send = pl.pallas_call(
            functools.partial(scatter_kernel, steps),
            out_shape=jax.ShapeDtypeStruct((all_slots, 2 * d), BF16),
            grid=(steps + tiles,),
            in_specs=[
                smem,
                pl.BlockSpec((8, block), lambda i: (0, jnp.minimum(i, steps - 1))),
                pl.BlockSpec((block, d), lambda i: (jnp.minimum(i, steps - 1), 0)),
                pl.BlockSpec((block, d), lambda i: (jnp.minimum(i, steps - 1), 0)),
            ],
            out_specs=pl.BlockSpec((tile, 2 * d), lambda i: (jnp.maximum(i - steps, 0), 0)),
            scratch_shapes=[pltpu.VMEM((block // 8, 8, 2 * d), F32)] * 2 + [pltpu.VMEM((all_slots, 2 * d), F32)],
            compiler_params=pltpu.CompilerParams(vmem_limit_bytes=big),
            cost_estimate=pl.CostEstimate(flops=50_000_000_000, bytes_accessed=20_000_000, transcendentals=0),
            name="scatter",
        )(pos, gates, hidden, d_out)
        send = send.reshape(n_experts, per_expert, 2 * d)

        dma = pltpu.SemaphoreType.DMA
        assert part == d
        slots = 2 * per
        sources = n_dev // 2
        ring = 3
        results = (jax.ShapeDtypeStruct((local_experts, d, part), F32),) * 3
        back, *rest = pl.pallas_call(
            functools.partial(expert_kernel, ep_size, etp_size, float(capacity)),
            out_shape=(
                jax.ShapeDtypeStruct((n_experts, per_expert, 2 * d), BF16),
                *(jax.ShapeDtypeStruct((per, d, part), F32),) * 6,
                *(jax.ShapeDtypeStruct((2 * per, d, part), F32),) * 2,
                *(jax.ShapeDtypeStruct((per, d, part), F32),) * 2,
                jax.ShapeDtypeStruct((n_dev, 8, 2 * n_experts), F32),
            ),
            in_specs=[anywhere, vmem] + [anywhere] * 15,
            out_specs=(anywhere,) * 11 + (vmem,),
            scratch_shapes=[
                pltpu.VMEM((slots, sources, per_expert, 2 * d), BF16),
                pltpu.VMEM((slots, d, 2 * ff), BF16),
                pltpu.VMEM((slots, ff, d), BF16),
                pltpu.VMEM((ring, d, 2 * ff), F32),
                pltpu.VMEM((ring, ff, d), F32),
                pltpu.VMEM((d, ff), F32),
                pltpu.VMEM((slots, 6, d, part), F32),
                pltpu.VMEM((2 * per_expert, 2 * d), BF16),
                pltpu.VMEM((2 * per_expert, ff), BF16),
                pltpu.VMEM((2 * per_expert, 2 * ff), BF16),
                pltpu.VMEM((n_dev, 8, 2 * n_experts), F32),
                dma, dma, dma((18,)), dma((6,)), dma((6,)), dma, dma((slots,)), dma, dma, dma, dma((ring,)), dma((slots,)),
            ],
            cost_estimate=pl.CostEstimate(flops=300_000_000_000, bytes_accessed=60_000_000, transcendentals=0),
            compiler_params=pltpu.CompilerParams(collective_id=0, has_side_effects=True, vmem_limit_bytes=big),
            name="experts",
        )(send, stats, *weights, *near[0], *near[1], *twin[0], *twin[1])
        table = rest[-1]
        mine = rest[0:6]
        came_in = [lax.ppermute(part_in, "etp", swap) for part_in, swap in zip(rest[6:8], (swap_z, swap_y))]
        came_out = [lax.ppermute(part_out, "etp", swap) for part_out, swap in zip(rest[8:10], (swap_z, swap_y))]

        cols = lambda n: pl.BlockSpec((n, block), lambda i: (0, i))
        tok = pl.BlockSpec((block, d), lambda i: (i, 0))
        output, d_hidden, dwr_part, aux_loss = pl.pallas_call(
            functools.partial(combine_kernel, n_tokens, tile),
            out_shape=(
                jax.ShapeDtypeStruct((rows, d), BF16),
                jax.ShapeDtypeStruct((rows, d), BF16),
                jax.ShapeDtypeStruct((n_experts, d), F32),
                jax.ShapeDtypeStruct((1, 1), F32),
            ),
            grid=(steps,),
            in_specs=[smem, anywhere, vmem, vmem, tok, tok, cols(2), cols(8), cols(n_experts)],
            out_specs=(tok, tok, pl.BlockSpec((n_experts, d), lambda i: (0, 0)), smem),
            scratch_shapes=[
                pltpu.VMEM((all_slots, 2 * d), F32),
                pltpu.VMEM((2, tile, 2 * d), BF16),
                pltpu.VMEM((block // 8, 8, 2 * d), F32),
                pltpu.VMEM((block // 8, 8, 2 * d), F32),
                dma((2,)),
            ],
            compiler_params=pltpu.CompilerParams(vmem_limit_bytes=big),
            cost_estimate=pl.CostEstimate(flops=60_000_000_000, bytes_accessed=30_000_000, transcendentals=0),
            name="combine",
        )(pos, back.reshape(all_slots, 2 * d), table, wr_t, hidden, d_out, ids_t, gates, probs)

        plan = [(kind * 3 + w, 0, w, kind, 0) for w in (2, 0, 1) for kind in range(2)]
        plan += [(6 + kind, w * per, w, kind, 1) for w in range(2) for kind in range(2)]
        half = pl.pallas_call(
            functools.partial(place_kernel, per, plan),
            out_shape=results,
            in_specs=[anywhere] * 8,
            out_specs=(anywhere,) * 3,
            scratch_shapes=[pltpu.VMEM((len(plan), per, d, part), F32), dma((len(plan),)), dma((len(plan),))],
            cost_estimate=pl.CostEstimate(flops=10_000_000_000, bytes_accessed=20_000_000, transcendentals=0),
            compiler_params=pltpu.CompilerParams(vmem_limit_bytes=big),
            name="place",
        )(*mine, *came_in)
        dwr_part, *half = lax.optimization_barrier((dwr_part, *half))
        dwr = pl.pallas_call(
            functools.partial(sum_kernel, ep_size, etp_size),
            out_shape=jax.ShapeDtypeStruct((n_experts, d), F32),
            in_specs=[vmem],
            out_specs=vmem,
            scratch_shapes=[
                pltpu.VMEM((n_dev, 8, 128), F32), pltpu.VMEM((8, 128), F32), pltpu.VMEM((n_dev, 8, 128), F32),
                dma, dma, dma, dma,
            ],
            compiler_params=pltpu.CompilerParams(collective_id=1, has_side_effects=True),
            cost_estimate=pl.CostEstimate(flops=10_000_000_000, bytes_accessed=100_000, transcendentals=0),
            name="sum_router",
        )(dwr_part)
        g_gate, g_up = half[0:2]
        g_down = pl.pallas_call(
            functools.partial(place_last_kernel, per),
            out_shape=results[2],
            in_specs=[vmem, vmem, anywhere],
            out_specs=anywhere,
            input_output_aliases={2: 0},
            scratch_shapes=[dma((2,))],
            compiler_params=pltpu.CompilerParams(vmem_limit_bytes=8 * 1024 * 1024),
            name="place_last",
        )(*came_out, half[2])
        return output, d_hidden, dwr.T, aux_loss.reshape(()), g_gate, g_up, g_down

    return jax.shard_map(layer, mesh=mesh, in_specs=(tok_spec, P(), tok_spec, tok_spec, gate_spec, gate_spec, down_spec), out_specs=(tok_spec, tok_spec, P(), P(), gate_spec, gate_spec, down_spec), check_vma=False)
```

```python
import functools
import jax
import jax.numpy as jnp
from jax import lax
from jax.experimental import pallas as pl
from jax.experimental.pallas import tpu as pltpu
from jax.sharding import PartitionSpec as P


AUX_COEF = 0.01
OUT_SCALE = 2.0
GROUP = 128
F32 = jnp.float32
BF16 = jnp.bfloat16
HI = lax.Precision.HIGHEST
MESH = pl.DeviceIdType.MESH
NT = (((1,), (1,)), ((), ()))
TN = (((0,), (0,)), ((), ()))


def dot(a, b, dims=(((1,), (0,)), ((), ())), precision=None):
    return lax.dot_general(a, b, dims, precision=precision, preferred_element_type=F32)


def flip(index, mask, bits):
    total = 0
    for bit in range(bits):
        total = total + ((index // 2**bit + mask // 2**bit) % 2) * 2**bit
    return total


def route_kernel(per_expert, hidden_ref, wr_ref, ids_ref, pos_ref, gate_ref, prob_ref, stat_ref):
    n_experts = wr_ref.shape[0]
    rows = hidden_ref.shape[0]
    block = min(512, rows)
    iota_e = lax.broadcasted_iota(jnp.int32, (n_experts, block), 0)
    upper = (lax.broadcasted_iota(jnp.int32, (block, block), 0) < lax.broadcasted_iota(jnp.int32, (block, block), 1)).astype(BF16)
    ones = jnp.ones((8, block), BF16)
    ones_f = jnp.ones((8, block), F32)
    wr = wr_ref[...]
    wr_hi = wr.astype(BF16)
    rest = wr - wr_hi.astype(F32)
    wr_mid = rest.astype(BF16)
    wr_lo = (rest - wr_mid.astype(F32)).astype(BF16)
    gate_ref[...] = jnp.zeros_like(gate_ref)
    carry = jnp.zeros((n_experts, 1), F32)
    counts = jnp.zeros((8, n_experts), F32)
    probs = jnp.zeros((8, n_experts), F32)
    for i in range(rows // block):
        cols = pl.ds(i * block, block)
        h = hidden_ref[cols, :]
        z = dot(wr_lo, h, NT) + dot(wr_mid, h, NT) + dot(wr_hi, h, NT)
        e = jnp.exp(z - jnp.max(z, axis=0, keepdims=True))
        p = e / jnp.sum(e, axis=0, keepdims=True)
        prob_ref[:, cols] = p
        id0 = ids_ref[0:1, cols]
        id1 = ids_ref[1:2, cols]
        hit0 = iota_e == id0
        hit1 = iota_e == id1
        p0 = jnp.sum(jnp.where(hit0, p, 0.0), axis=0, keepdims=True)
        p1 = jnp.sum(jnp.where(hit1, p, 0.0), axis=0, keepdims=True)
        den = p0 + p1
        gate_ref[0:1, cols] = p0 / den
        gate_ref[1:2, cols] = p1 / den
        hits = jnp.where(hit0 | hit1, 1.0, 0.0).astype(F32)
        hits_b = hits.astype(BF16)
        rank = dot(hits_b, upper) + carry
        r0 = jnp.sum(jnp.where(hit0, rank, 0.0), axis=0, keepdims=True)
        r1 = jnp.sum(jnp.where(hit1, rank, 0.0), axis=0, keepdims=True)
        pos_ref[0:1, cols] = id0 * per_expert + r0.astype(jnp.int32)
        pos_ref[1:2, cols] = id1 * per_expert + r1.astype(jnp.int32)
        carry = carry + jnp.sum(hits, axis=1, keepdims=True)
        counts = counts + dot(ones, hits_b, NT)
        probs = probs + dot(ones_f, p, NT, HI)
    stat_ref[:, 0:n_experts] = counts
    stat_ref[:, n_experts:2 * n_experts] = probs


def scatter_kernel(steps, pos_ref, gate_ref, hidden_ref, dout_ref, send_ref, first_ref, second_ref, slots_ref):
    step = pl.program_id(0)
    block, d = hidden_ref.shape
    tile = send_ref.shape[0]

    @pl.when(step < steps)
    def _():
        x = hidden_ref[...].astype(F32)
        m = OUT_SCALE * dout_ref[...].astype(F32)
        g = gate_ref[...].T
        x = x.reshape(block // 8, 8, d)
        first_ref[:, :, 0:d] = x
        first_ref[:, :, d:2 * d] = (g[:, 0:1] * m).reshape(block // 8, 8, d)
        second_ref[:, :, 0:d] = x
        second_ref[:, :, d:2 * d] = (g[:, 1:2] * m).reshape(block // 8, 8, d)

        def group(c, _):
            for i in range(GROUP):
                for k, ref in enumerate((first_ref, second_ref)):
                    q = pos_ref[step * (block // GROUP) + c, k, i]
                    slots_ref[pl.ds(q, 1), :] = ref[c * (GROUP // 8) + i // 8, i % 8:i % 8 + 1, :]
            return 0

        lax.fori_loop(0, block // GROUP, group, 0)

    @pl.when(step >= steps)
    def _():
        start = pl.multiple_of((step - steps) * tile, tile)
        send_ref[...] = slots_ref[pl.ds(start, tile), :].astype(BF16)


def expert_kernel(
    ep, etp, capacity, send_ref, stat_ref, *refs,
):
    own, near, twin, refs = refs[0:3], (refs[3:6], refs[6:9]), (refs[9:12], refs[12:15]), refs[15:]
    back_ref = refs[0]
    mine, onward_in, onward_out = (refs[1:4], refs[4:7]), refs[7:9], refs[9:11]
    tab_out_ref, x_ref, w13_ref, w2f_ref, ga13_ref, ga2_ref, ga2t_ref, twin_ref, xm_ref, u_ref, dab_ref, tab_ref = refs[11:23]
    stat_send, stat_recv, w_recv, relay_send, relay_recv, x_send, x_recv, back_send, back_recv, g_done, g_send, g_recv = refs[23:]
    n_dev = ep * etp
    n_slots, n_src, rows, _ = x_ref.shape
    per = n_slots // 2
    ring = ga13_ref.shape[0]
    d = w2f_ref.shape[2]
    ff = w2f_ref.shape[1]
    part = ff // etp
    bits = n_dev.bit_length() - 1
    src_bits = n_src.bit_length() - 1
    me_o = lax.axis_index("ep")
    me_t = lax.axis_index("etp")
    me = me_o * etp + me_t
    z = me_t // 2
    y = me_t % 2
    t_y = flip(me_t, 1, 2)
    t_z = flip(me_t, 2, 2)
    t_yz = flip(me_t, 3, 2)

    def pick(kind, first, second):
        return first + kind * (second - first)

    def place(kind, w):
        return pick(kind, w * 2 + y, z * 2 + w)

    def remote(src, dst, send, recv, o, t):
        pltpu.make_async_remote_copy(src_ref=src, dst_ref=dst, send_sem=send, recv_sem=recv, device_id={"ep": o, "etp": t}, device_id_type=MESH).start()

    def wait_bytes(ref, sem):
        pltpu.make_async_copy(ref, ref, sem).wait()

    barrier = pltpu.get_barrier_semaphore()

    def hello(i, _):
        peer = (me + i) % n_dev
        pl.semaphore_signal(barrier, inc=1, device_id={"ep": peer // etp, "etp": peer % etp}, device_id_type=MESH)
        return 0

    lax.fori_loop(1, n_dev, hello, 0)
    pl.semaphore_wait(barrier, n_dev - 1)

    def lanes(offset, t):
        return pl.ds(pl.multiple_of(offset + t * part, part), part)

    def places(kind, t):
        group = slice(kind * per, (kind + 1) * per)
        return w13_ref.at[group, :, lanes(0, t)], w13_ref.at[group, :, lanes(ff, t)], w2f_ref.at[group, lanes(0, t), :]

    relays, loads = [], []
    for kind in range(2):
        beside, across = (t_z, t_y) if kind == 0 else (t_y, t_z)
        start = pick(kind, z * per, (2 + y) * per)
        for w in range(3):
            n = kind * 3 + w
            relays.append(pltpu.make_async_remote_copy(
                src_ref=near[kind][w], dst_ref=places(kind, beside)[w], send_sem=relay_send.at[n], recv_sem=relay_recv.at[n],
                device_id={"ep": me_o, "etp": across}, device_id_type=MESH,
            ))
            for ref, t in ((own[w].at[pl.ds(start, per)], me_t), (near[kind][w], beside), (twin[kind][w], across)):
                loads.append(pltpu.make_async_copy(ref, places(kind, t)[w], w_recv.at[len(loads)]))
    for copy in relays + loads:
        copy.start()

    def send_stats(i, _):
        peer = flip(me, (i * 11) % n_dev, bits)
        remote(stat_ref, tab_ref.at[me], stat_send, stat_recv, peer // etp, peer % etp)
        return 0

    lax.fori_loop(1, n_dev, send_stats, 0)
    tab_ref[me] = stat_ref[...]

    def expert_of(o, kind, w, k):
        return o * (4 * per) + kind * (2 * per) + w * per + k

    def send_slot(i, _):
        kind, k = i % 2, i // 2
        here = me_o * 2 + pick(kind, z, y)
        pltpu.make_async_copy(send_ref.at[expert_of(me_o, kind, pick(kind, z, y), k)], x_ref.at[i, here], x_recv.at[i]).start()

        def tokens(m, _):
            there = flip(here, (m * 5) % n_src, src_bits)
            o, w = there // 2, there % 2
            remote(send_ref.at[expert_of(o, kind, w, k)], x_ref.at[i, here], x_send, x_recv.at[i], o, place(kind, w))
            return 0

        lax.fori_loop(1, n_src, tokens, 0)
        return 0

    lax.fori_loop(0, n_slots, send_slot, 0)

    wait_bytes(tab_ref.at[0:n_dev - 1], stat_recv)
    tab_out_ref[...] = tab_ref[...]
    table = tab_ref[:, 0, :]
    shape = table.shape
    below = (lax.broadcasted_iota(jnp.int32, (n_dev, n_dev), 1) < lax.broadcasted_iota(jnp.int32, (n_dev, n_dev), 0)).astype(F32)
    keep = jnp.minimum(table, capacity - dot(below, table, precision=HI))
    src_iota = lax.broadcasted_iota(jnp.int32, shape, 0)
    lane_iota = lax.broadcasted_iota(jnp.int32, shape, 1)
    row_iota = lax.broadcasted_iota(jnp.int32, (rows, 2 * d), 0).astype(F32)

    for copy in loads:
        copy.wait()
    for copy in relays:
        copy.wait_recv()

    def do_slot(i, _):
        kind, k = i % 2, i // 2
        at = kind * per + k
        r = i % ring
        v = pick(kind, z, y)
        expert = expert_of(me_o, kind, v, k)

        @pl.when(i >= ring)
        def _():
            wait_bytes(twin_ref.at[0], g_send.at[r])

        wait_bytes(x_ref.at[i], x_recv.at[i])
        ga13_ref[r] = jnp.zeros((d, 2 * ff), F32)
        ga2t_ref[...] = jnp.zeros((d, ff), F32)

        def give_back(b):
            o = flip(me_o, b, 2)
            for w in range(2):
                away = (o - me_o) * (o - me_o) + (w - v) * (w - v)

                @pl.when(away == 0)
                def _():
                    pltpu.make_async_copy(x_ref.at[i, o * 2 + w], back_ref.at[expert], back_recv).start()

                @pl.when(away != 0)
                def _():
                    remote(x_ref.at[i, o * 2 + w], back_ref.at[expert], back_send, back_recv, o, place(kind, w))

        def do_block(b, _):
            o = flip(me_o, b, 2)
            for w in range(2):
                limit = jnp.sum(jnp.where((src_iota == o * etp + place(kind, w)) & (lane_iota == expert), keep, 0.0), keepdims=True)
                full = x_ref[i, o * 2 + w].astype(F32)
                xm_ref[w * rows:(w + 1) * rows, :] = jnp.where(row_iota < limit, full, 0.0).astype(BF16)
            x = xm_ref[:, 0:d]
            c = xm_ref[:, d:2 * d]
            for q in range(etp):
                here = slice(q * part, (q + 1) * part)
                there = slice(ff + q * part, ff + (q + 1) * part)
                a = dot(x, w13_ref[at, :, here])
                up = dot(x, w13_ref[at, :, there])
                du = dot(c, w2f_ref[at, here, :], NT)
                sig = jax.nn.sigmoid(a)
                silu = a * sig
                u_ref[:, here] = (silu * up).astype(BF16)
                dab_ref[:, here] = (du * up * sig * (1.0 + a * (1.0 - sig))).astype(BF16)
                dab_ref[:, there] = (du * silu).astype(BF16)
            out = dot(u_ref[...], w2f_ref[at]).astype(BF16)
            dx = dot(dab_ref[...], w13_ref[at], NT).astype(BF16)
            for w in range(2):
                x_ref[i, o * 2 + w, :, 0:d] = out[w * rows:(w + 1) * rows]
                x_ref[i, o * 2 + w, :, d:2 * d] = dx[w * rows:(w + 1) * rows]
            ga13_ref[r] += dot(x, dab_ref[...], TN)
            ga2t_ref[...] += dot(c, u_ref[...], TN)

            @pl.when(b > 0)
            def _():
                give_back(b - 1)

            return 0

        lax.fori_loop(0, ep, do_block, 0)
        ga2_ref[r] = ga2t_ref[...].T
        give_back(ep - 1)

        for one in range(2):
            @pl.when(kind == one)
            def _():
                across = t_y if one == 0 else t_z
                for w in range(3):
                    remote(parts(r, across)[w], twin_ref.at[i, w], g_send.at[r], g_recv.at[i], me_o, across)
                    remote(parts(r, t_yz)[w], twin_ref.at[i, 3 + w], g_send.at[r], g_recv.at[i], me_o, across)

        @pl.when(i >= 2)
        def _():
            add_twin(i - 2)

        return 0

    def parts(r, t):
        return ga13_ref.at[r, :, lanes(0, t)], ga13_ref.at[r, :, lanes(ff, t)], ga2_ref.at[r, lanes(0, t), :]

    def add_twin(i):
        kind, k = i % 2, i // 2
        r = i % ring
        wait_bytes(twin_ref.at[i], g_recv.at[i])
        for one in range(2):
            @pl.when(kind == one)
            def _():
                beside = t_z if one == 0 else t_y
                for w in range(3):
                    twin_ref[i, w] += parts(r, me_t)[w][...]
                    twin_ref[i, 3 + w] += parts(r, beside)[w][...]
                for w in range(3):
                    pltpu.make_async_copy(twin_ref.at[i, w], mine[one][w].at[k], g_done).start()
                    onward = onward_in[one].at[w * per + k] if w < 2 else onward_out[one].at[k]
                    pltpu.make_async_copy(twin_ref.at[i, 3 + w], onward, g_done).start()

    lax.fori_loop(0, n_slots, do_slot, 0)
    lax.fori_loop(n_slots - 2, n_slots, lambda i, _: (add_twin(i), 0)[1], 0)

    others = (n_src - 1) * n_slots
    wait_bytes(tab_ref.at[0:n_dev - 1], stat_send)
    for copy in relays:
        copy.wait_send()
    wait_bytes(send_ref.at[0:others], x_send)
    wait_bytes(send_ref.at[0:others], back_send)
    for r in range(ring):
        wait_bytes(twin_ref.at[0], g_send.at[r])
    wait_bytes(back_ref, back_recv)
    wait_bytes(twin_ref, g_done)


def combine_kernel(
    n_tokens, chunk,
    pos_ref, back_ref, tab_ref, wr_ref, hidden_ref, dout_ref, ids_ref, gate_ref, prob_ref,
    out_ref, dh_ref, dwr_ref, aux_ref,
    rows_ref, stage_ref, first_ref, second_ref, sem,
):
    step = pl.program_id(0)
    block, d = hidden_ref.shape
    n_experts = wr_ref.shape[0]
    n_chunks = rows_ref.shape[0] // chunk

    totals = jnp.sum(tab_ref[:, 0:1, :], axis=0)
    frac = totals[:, 0:n_experts] / (2 * n_tokens)

    def fetch(i, slot):
        start = pl.multiple_of(i * chunk, chunk)
        return pltpu.make_async_copy(back_ref.at[pl.ds(start, chunk), :], stage_ref.at[slot], sem.at[slot])

    @pl.when(step == 0)
    def _():
        fetch(0, 0).start()

        def body(i, _):
            slot = i % 2

            @pl.when(i + 1 < n_chunks)
            def _():
                fetch(i + 1, 1 - slot).start()

            fetch(i, slot).wait()
            rows_ref[pl.ds(pl.multiple_of(i * chunk, chunk), chunk), :] = stage_ref[slot].astype(F32)
            return 0

        lax.fori_loop(0, n_chunks, body, 0)
        dwr_ref[...] = jnp.zeros_like(dwr_ref)
        mean_prob = totals[:, n_experts:2 * n_experts] / n_tokens
        aux_ref[0, 0] = AUX_COEF * n_experts * jnp.sum(frac * mean_prob)

    def group(c, _):
        for i in range(GROUP):
            for k, ref in enumerate((first_ref, second_ref)):
                q = pos_ref[step * (block // GROUP) + c, k, i]
                ref[c * (GROUP // 8) + i // 8, i % 8:i % 8 + 1, :] = rows_ref[pl.ds(q, 1), :]
        return 0

    lax.fori_loop(0, block // GROUP, group, 0)

    h = hidden_ref[...].astype(F32)
    dy = dout_ref[...].astype(F32)
    m = OUT_SCALE * dy
    y0 = first_ref[:, :, 0:d].reshape(block, d)
    y1 = second_ref[:, :, 0:d].reshape(block, d)
    dx = (first_ref[:, :, d:2 * d] + second_ref[:, :, d:2 * d]).reshape(block, d)
    g = gate_ref[...].T
    out_ref[...] = (h + OUT_SCALE * (g[:, 0:1] * y0 + g[:, 1:2] * y1)).astype(BF16)

    ones = jnp.ones((8, d), F32)
    dg0 = dot(ones, m * y0, NT, HI)[0:1]
    dg1 = dot(ones, m * y1, NT, HI)[0:1]
    p = prob_ref[...]
    iota_e = lax.broadcasted_iota(jnp.int32, p.shape, 0)
    hit0 = iota_e == ids_ref[0:1, :]
    hit1 = iota_e == ids_ref[1:2, :]
    den = jnp.sum(jnp.where(hit0 | hit1, p, 0.0), axis=0, keepdims=True)
    mean = gate_ref[0:1, :] * dg0 + gate_ref[1:2, :] * dg1
    eye = lax.broadcasted_iota(jnp.int32, (n_experts, n_experts), 0) == lax.broadcasted_iota(jnp.int32, (n_experts, n_experts), 1)
    ct = (AUX_COEF * n_experts / n_tokens) * jnp.sum(jnp.where(eye, frac, 0.0), axis=1, keepdims=True)
    dp = jnp.where(hit0, (dg0 - mean) / den, 0.0) + jnp.where(hit1, (dg1 - mean) / den, 0.0) + ct
    dz = p * (dp - jnp.sum(p * dp, axis=0, keepdims=True))
    dwr_ref[...] += dot(dz, h, precision=HI)
    dh_ref[...] = (dy + dx + dot(dz, wr_ref[...], TN, HI)).astype(BF16)


def sum_kernel(ep, etp, part_ref, out_ref, box_ref, mine_ref, all_ref, send1, recv1, send2, recv2):
    n_dev = ep * etp
    across = part_ref.shape[1] // 128
    me = lax.axis_index("ep") * etp + lax.axis_index("etp")

    def where_is(peer):
        return {"ep": peer // etp, "etp": peer % etp}

    def tile(ref, i):
        return ref.at[pl.ds(pl.multiple_of((i // across) * 8, 8), 8), pl.ds(pl.multiple_of((i % across) * 128, 128), 128)]

    def wait_bytes(ref, sem):
        pltpu.make_async_copy(ref, ref, sem).wait()

    barrier = pltpu.get_barrier_semaphore()

    def hello(i, _):
        pl.semaphore_signal(barrier, inc=1, device_id=where_is((me + i) % n_dev), device_id_type=MESH)
        return 0

    lax.fori_loop(1, n_dev, hello, 0)
    pl.semaphore_wait(barrier, n_dev - 1)

    def first(i, _):
        peer = (me + i) % n_dev
        pltpu.make_async_remote_copy(tile(part_ref, peer), box_ref.at[me], send1, recv1, device_id=where_is(peer), device_id_type=MESH).start()
        return 0

    lax.fori_loop(1, n_dev, first, 0)
    pltpu.make_async_copy(tile(part_ref, me), box_ref.at[me], recv1).start()
    wait_bytes(box_ref, recv1)
    mine_ref[...] = jnp.sum(box_ref[...], axis=0)

    def second(i, _):
        peer = (me + i) % n_dev
        pltpu.make_async_remote_copy(mine_ref, all_ref.at[me], send2, recv2, device_id=where_is(peer), device_id_type=MESH).start()
        return 0

    lax.fori_loop(1, n_dev, second, 0)
    all_ref[me] = mine_ref[...]
    wait_bytes(all_ref.at[0:n_dev - 1], recv2)
    for i in range(n_dev):
        out_ref[(i // across) * 8:(i // across) * 8 + 8, (i % across) * 128:(i % across) * 128 + 128] = all_ref[i]
    wait_bytes(box_ref.at[0:n_dev - 1], send1)
    wait_bytes(all_ref.at[0:n_dev - 1], send2)


def starts_of(per):
    me_t = lax.axis_index("etp")
    z, y = me_t // 2, me_t % 2
    return (z * per, (2 + y) * per), ((1 - z) * per, (3 - y) * per)


def place_kernel(per, plan, *refs):
    parts, outs = refs[:-6], refs[-6:-3]
    stage_ref, in_sem, out_sem = refs[-3:]
    starts = starts_of(per)
    loads, stores = [], []
    for i, (ref, row, out, kind, came) in enumerate(plan):
        loads.append(pltpu.make_async_copy(parts[ref].at[row:row + per], stage_ref.at[i], in_sem.at[i]))
        stores.append(pltpu.make_async_copy(stage_ref.at[i], outs[out].at[pl.ds(starts[came][kind], per)], out_sem.at[i]))
    for load in loads:
        load.start()
    for load, store in zip(loads, stores):
        load.wait()
        store.start()
    for store in stores:
        store.wait()


def place_last_kernel(per, first_ref, second_ref, _, out_ref, sem):
    starts = starts_of(per)[1]
    copies = [pltpu.make_async_copy(ref, out_ref.at[pl.ds(starts[i], per)], sem.at[i]) for i, ref in enumerate((first_ref, second_ref))]
    for copy in copies:
        copy.start()
    for copy in copies:
        copy.wait()


def solution(mesh):
    ep_size = mesh.shape["ep"]
    etp_size = mesh.shape["etp"]
    n_dev = ep_size * etp_size
    all_axes = ("ep", "etp")
    tok_spec = P(all_axes, None)
    gate_spec = P("ep", None, "etp")
    down_spec = P("ep", "etp", None)

    def layer(hidden, w_router, expert_ids, d_out, w_gate, w_up, w_down):
        rows, d = hidden.shape
        n_experts = w_router.shape[1]
        n_tokens = rows * n_dev
        capacity = (5 * n_tokens + 2 * n_experts - 1) // (2 * n_experts)
        per_expert = 7 * rows // (2 * n_experts)
        n_slots = n_experts // n_dev
        local_experts, _, part = w_gate.shape
        ff = part * etp_size
        all_slots = n_experts * per_expert
        assert etp_size == 4 and ep_size == 4
        me_t = lax.axis_index("etp")
        z, y = me_t // 2, me_t % 2
        per = n_experts // ep_size // 4
        swap_y = [(t, t ^ 1) for t in range(4)]
        swap_z = [(t, t ^ 2) for t in range(4)]

        weights = w_gate, w_up, w_down

        def parts_at(w, start):
            return lax.dynamic_slice_in_dim(w, start, per)

        near, twin = ([], []), ([], [])
        for w in weights:
            first = [parts_at(w, (1 - z) * per), parts_at(w, (3 - y) * per)]
            if w is w_gate:
                *first, w = lax.optimization_barrier((*first, w))
            near[0].append(lax.ppermute(first[0], "etp", swap_z))
            near[1].append(lax.ppermute(first[1], "etp", swap_y))
            twin[0].append(lax.ppermute(parts_at(w, z * per), "etp", swap_y))
            twin[1].append(lax.ppermute(parts_at(w, (2 + y) * per), "etp", swap_z))
        ids_t = expert_ids.T
        wr_t = w_router.T

        vmem = pl.BlockSpec(memory_space=pltpu.VMEM)
        smem = pl.BlockSpec(memory_space=pltpu.SMEM)
        anywhere = pl.BlockSpec(memory_space=pl.ANY)
        big = 60 * 1024 * 1024

        pos, gates, probs, stats = pl.pallas_call(
            functools.partial(route_kernel, per_expert),
            out_shape=(
                jax.ShapeDtypeStruct((2, rows), jnp.int32),
                jax.ShapeDtypeStruct((8, rows), F32),
                jax.ShapeDtypeStruct((n_experts, rows), F32),
                jax.ShapeDtypeStruct((8, 2 * n_experts), F32),
            ),
            in_specs=[vmem] * 3,
            out_specs=(vmem,) * 4,
            cost_estimate=pl.CostEstimate(flops=5_000_000_000, bytes_accessed=4_000_000, transcendentals=0),
            name="route",
        )(hidden, wr_t, ids_t)

        block = min(512, rows)
        steps = rows // block
        pos = pos.reshape(2, rows // GROUP, GROUP).transpose(1, 0, 2)
        tile = n_slots * per_expert
        tiles = all_slots // tile
        send = pl.pallas_call(
            functools.partial(scatter_kernel, steps),
            out_shape=jax.ShapeDtypeStruct((all_slots, 2 * d), BF16),
            grid=(steps + tiles,),
            in_specs=[
                smem,
                pl.BlockSpec((8, block), lambda i: (0, jnp.minimum(i, steps - 1))),
                pl.BlockSpec((block, d), lambda i: (jnp.minimum(i, steps - 1), 0)),
                pl.BlockSpec((block, d), lambda i: (jnp.minimum(i, steps - 1), 0)),
            ],
            out_specs=pl.BlockSpec((tile, 2 * d), lambda i: (jnp.maximum(i - steps, 0), 0)),
            scratch_shapes=[pltpu.VMEM((block // 8, 8, 2 * d), F32)] * 2 + [pltpu.VMEM((all_slots, 2 * d), F32)],
            compiler_params=pltpu.CompilerParams(vmem_limit_bytes=big),
            cost_estimate=pl.CostEstimate(flops=50_000_000_000, bytes_accessed=20_000_000, transcendentals=0),
            name="scatter",
        )(pos, gates, hidden, d_out)
        send = send.reshape(n_experts, per_expert, 2 * d)

        dma = pltpu.SemaphoreType.DMA
        assert part == d
        slots = 2 * per
        sources = n_dev // 2
        ring = 3
        results = (jax.ShapeDtypeStruct((local_experts, d, part), F32),) * 3
        back, *rest = pl.pallas_call(
            functools.partial(expert_kernel, ep_size, etp_size, float(capacity)),
            out_shape=(
                jax.ShapeDtypeStruct((n_experts, per_expert, 2 * d), BF16),
                *(jax.ShapeDtypeStruct((per, d, part), F32),) * 6,
                *(jax.ShapeDtypeStruct((2 * per, d, part), F32),) * 2,
                *(jax.ShapeDtypeStruct((per, d, part), F32),) * 2,
                jax.ShapeDtypeStruct((n_dev, 8, 2 * n_experts), F32),
            ),
            in_specs=[anywhere, vmem] + [anywhere] * 15,
            out_specs=(anywhere,) * 11 + (vmem,),
            scratch_shapes=[
                pltpu.VMEM((slots, sources, per_expert, 2 * d), BF16),
                pltpu.VMEM((slots, d, 2 * ff), BF16),
                pltpu.VMEM((slots, ff, d), BF16),
                pltpu.VMEM((ring, d, 2 * ff), F32),
                pltpu.VMEM((ring, ff, d), F32),
                pltpu.VMEM((d, ff), F32),
                pltpu.VMEM((slots, 6, d, part), F32),
                pltpu.VMEM((2 * per_expert, 2 * d), BF16),
                pltpu.VMEM((2 * per_expert, ff), BF16),
                pltpu.VMEM((2 * per_expert, 2 * ff), BF16),
                pltpu.VMEM((n_dev, 8, 2 * n_experts), F32),
                dma, dma, dma((18,)), dma((6,)), dma((6,)), dma, dma((slots,)), dma, dma, dma, dma((ring,)), dma((slots,)),
            ],
            cost_estimate=pl.CostEstimate(flops=300_000_000_000, bytes_accessed=60_000_000, transcendentals=0),
            compiler_params=pltpu.CompilerParams(collective_id=0, has_side_effects=True, vmem_limit_bytes=big),
            name="experts",
        )(send, stats, *weights, *near[0], *near[1], *twin[0], *twin[1])
        table = rest[-1]
        mine = rest[0:6]
        came_in = [lax.ppermute(part_in, "etp", swap) for part_in, swap in zip(rest[6:8], (swap_z, swap_y))]
        came_out = [lax.ppermute(part_out, "etp", swap) for part_out, swap in zip(rest[8:10], (swap_z, swap_y))]

        cols = lambda n: pl.BlockSpec((n, block), lambda i: (0, i))
        tok = pl.BlockSpec((block, d), lambda i: (i, 0))
        output, d_hidden, dwr_part, aux_loss = pl.pallas_call(
            functools.partial(combine_kernel, n_tokens, tile),
            out_shape=(
                jax.ShapeDtypeStruct((rows, d), BF16),
                jax.ShapeDtypeStruct((rows, d), BF16),
                jax.ShapeDtypeStruct((n_experts, d), F32),
                jax.ShapeDtypeStruct((1, 1), F32),
            ),
            grid=(steps,),
            in_specs=[smem, anywhere, vmem, vmem, tok, tok, cols(2), cols(8), cols(n_experts)],
            out_specs=(tok, tok, pl.BlockSpec((n_experts, d), lambda i: (0, 0)), smem),
            scratch_shapes=[
                pltpu.VMEM((all_slots, 2 * d), F32),
                pltpu.VMEM((2, tile, 2 * d), BF16),
                pltpu.VMEM((block // 8, 8, 2 * d), F32),
                pltpu.VMEM((block // 8, 8, 2 * d), F32),
                dma((2,)),
            ],
            compiler_params=pltpu.CompilerParams(vmem_limit_bytes=big),
            cost_estimate=pl.CostEstimate(flops=60_000_000_000, bytes_accessed=30_000_000, transcendentals=0),
            name="combine",
        )(pos, back.reshape(all_slots, 2 * d), table, wr_t, hidden, d_out, ids_t, gates, probs)

        plan = [(kind * 3 + w, 0, w, kind, 0) for w in (2, 0, 1) for kind in range(2)]
        plan += [(6 + kind, w * per, w, kind, 1) for w in range(2) for kind in range(2)]
        half = pl.pallas_call(
            functools.partial(place_kernel, per, plan),
            out_shape=results,
            in_specs=[anywhere] * 8,
            out_specs=(anywhere,) * 3,
            scratch_shapes=[pltpu.VMEM((len(plan), per, d, part), F32), dma((len(plan),)), dma((len(plan),))],
            cost_estimate=pl.CostEstimate(flops=10_000_000_000, bytes_accessed=20_000_000, transcendentals=0),
            compiler_params=pltpu.CompilerParams(vmem_limit_bytes=big),
            name="place",
        )(*mine, *came_in)
        dwr_part, *half = lax.optimization_barrier((dwr_part, *half))
        dwr = pl.pallas_call(
            functools.partial(sum_kernel, ep_size, etp_size),
            out_shape=jax.ShapeDtypeStruct((n_experts, d), F32),
            in_specs=[vmem],
            out_specs=vmem,
            scratch_shapes=[
                pltpu.VMEM((n_dev, 8, 128), F32), pltpu.VMEM((8, 128), F32), pltpu.VMEM((n_dev, 8, 128), F32),
                dma, dma, dma, dma,
            ],
            compiler_params=pltpu.CompilerParams(collective_id=1, has_side_effects=True),
            cost_estimate=pl.CostEstimate(flops=10_000_000_000, bytes_accessed=100_000, transcendentals=0),
            name="sum_router",
        )(dwr_part)
        g_gate, g_up = half[0:2]
        g_down = pl.pallas_call(
            functools.partial(place_last_kernel, per),
            out_shape=results[2],
            in_specs=[vmem, vmem, anywhere],
            out_specs=anywhere,
            input_output_aliases={2: 0},
            scratch_shapes=[dma((2,))],
            compiler_params=pltpu.CompilerParams(vmem_limit_bytes=8 * 1024 * 1024),
            name="place_last",
        )(*came_out, half[2])
        return output, d_hidden, dwr.T, aux_loss.reshape(()), g_gate, g_up, g_down

    return jax.shard_map(layer, mesh=mesh, in_specs=(tok_spec, P(), tok_spec, tok_spec, gate_spec, gate_spec, down_spec), out_specs=(tok_spec, tok_spec, P(), P(), gate_spec, gate_spec, down_spec), check_vma=False)
```
